32 devices in a mesh: dp: 4 (over z), ctx: 4 (over x, core), fsdp: 2 (over y).
Axes of the slice: x: 2, y: 2, z: 4, core: 2. Of those that a mesh axis runs over, the one named last changes fastest.
Arguments:
- tokens: bfloat16 [16, 1024, 768], P(('dp', 'fsdp'), 'ctx'), may hold values from -12 to 12
- cotangent: bfloat16 [16, 1024, 768], P(('dp', 'fsdp'), 'ctx'), may hold values from -6 to 6
- lengths: int32 [16], P(('dp', 'fsdp')), may hold values from 256 to 1024, as said below
- w_qkv: bfloat16 [768, 2304], P('fsdp'), may hold values from -0.21875 to 0.21875
- bias_q: bfloat16 [768], P('fsdp'), may hold values from -3 to 3
- bias_v: bfloat16 [768], P('fsdp'), may hold values from -0.29882812 to 0.29882812
- w_out: bfloat16 [768, 768], P('fsdp'), may hold values from -6 to 6
- bias_out: bfloat16 [768], P('fsdp'), may hold values from -3 to 3
- gain_one: bfloat16 [768], P('fsdp'), may hold values from 0.5 to 1.5
- shift_one: bfloat16 [768], P('fsdp'), may hold values from -3 to 3
- w_up: bfloat16 [768, 3072], P('fsdp'), may hold values from -0.21875 to 0.21875
- bias_up: bfloat16 [3072], P('fsdp'), may hold values from -3 to 3
- w_down: bfloat16 [3072, 768], P('fsdp'), may hold values from -0.109375 to 0.109375
- bias_down: bfloat16 [768], P('fsdp'), may hold values from -3 to 3
- gain_two: bfloat16 [768], P('fsdp'), may hold values from 0.5 to 1.5
- shift_two: bfloat16 [768], P('fsdp'), may hold values from -3 to 3
Outputs:
- output: bfloat16 [16, 1024, 768], P(('dp', 'fsdp'), 'ctx')
- input_grad: bfloat16 [16, 1024, 768], P(('dp', 'fsdp'), 'ctx')
- grad_w_qkv: float32 [768, 2304], P('fsdp')
- grad_bias_q: float32 [768], P('fsdp')
- grad_bias_v: float32 [768], P('fsdp')
- grad_w_out: float32 [768, 768], P('fsdp')
- grad_bias_out: float32 [768], P('fsdp')
- grad_gain_one: float32 [768], P('fsdp')
- grad_shift_one: float32 [768], P('fsdp')
- grad_w_up: float32 [768, 3072], P('fsdp')
- grad_bias_up: float32 [3072], P('fsdp')
- grad_w_down: float32 [3072, 768], P('fsdp')
- grad_bias_down: float32 [768], P('fsdp')
- grad_gain_two: float32 [768], P('fsdp')
- grad_shift_two: float32 [768], P('fsdp')
The draws below stay inside these ranges and needn't reach their ends.
Inputs may be any that keep to these rules, and one draw needn't show every extreme that they name: `lengths`: count of real tokens of each sequence; keys at later positions are padding that no query attends to; some sequence is full in every draw.
All inputs are finite; a program needn't handle non-finite values.
Results may differ from the reference program's by a relative error of at most 0.02.
The reference program's roundings to bfloat16 on the way count: a program that leaves them out, or rounds other values in their place, can miss the bound.
Values may be sent and summed in bfloat16 or wider, within the bound.
A program may use at most 192 MiB of HBM per device.

```python
import math
import jax
import jax.numpy as jnp
from jax import lax

D = 768
HEADS = 12
FF = 3072
SEQ_LEN = 1024
SEQS = 16


def draw_tokens(key, part):
    values = jax.random.normal(key, (SEQS, SEQ_LEN, D), jnp.float32)
    return jnp.clip(values, -12.0, 12.0).astype(jnp.bfloat16)


def draw_lengths(key, part):
    first_key, second_key = jax.random.split(jax.random.fold_in(key, 3))
    drawn = jax.random.randint(first_key, (SEQS,), SEQ_LEN // 4, SEQ_LEN + 1)
    chosen = jax.random.randint(second_key, (), 0, SEQS)
    return jnp.where(jnp.arange(SEQS) == chosen, SEQ_LEN, drawn).astype(jnp.int32)


def shard_levels(own_key, shape, cuts, low, largest):
    def one(position, blocks):
        heights = jax.random.uniform(jax.random.fold_in(jax.random.fold_in(own_key, 6), position), (blocks,), jnp.float32, low / len(cuts), largest / len(cuts))
        return jnp.repeat(jnp.exp(heights), shape[position] // blocks).reshape((-1,) + (1,) * (len(shape) - position - 1))

    factor_of = one(*cuts[0])
    for cut in cuts[1:]:
        factor_of = factor_of * one(*cut)
    return factor_of


def gaussian(stream_key, extent, width, limit, cuts=(), held_as=jnp.bfloat16):
    array = width * jax.random.normal(stream_key, extent, jnp.float32)
    if cuts:
        array = array * shard_levels(stream_key, extent, cuts, -0.22, 0.18)
    return jnp.clip(array, -limit, limit).astype(held_as)


def setup_inputs(seed: int = 0) -> dict:
    keys = jax.random.split(jax.random.key(seed), 17)
    tokens = draw_tokens(jax.random.fold_in(keys[16], 71), 0)
    cotangent = gaussian(keys[1], (SEQS, SEQ_LEN, D), 1.0, 6.0, ((0, 8), (1, 4)))
    lengths = draw_lengths(jax.random.fold_in(keys[16], 71), 0)
    w_qkv = gaussian(keys[3], (D, 3 * D), D ** -0.5, 0.21875, ((0, 2),))
    bias_q = gaussian(keys[4], (D,), 0.5, 3.0, ((0, 2),))
    bias_v = gaussian(keys[5], (D,), 0.05, 0.29882812, ((0, 2),))
    w_out = gaussian(keys[6], (D, D), (max(1, 2 * D // SEQ_LEN)) ** -0.5, 6.0, ((0, 2),))
    bias_out = gaussian(keys[7], (D,), 0.5, 3.0, ((0, 2),))
    gain_one = jnp.clip(1.0 + 0.1 * jax.random.normal(keys[8], (D,), jnp.float32), 0.5, 1.5).astype(jnp.bfloat16)
    shift_one = gaussian(keys[9], (D,), 0.5, 3.0, ((0, 2),))
    w_up = gaussian(keys[10], (D, FF), D ** -0.5, 0.21875, ((0, 2),))
    bias_up = gaussian(keys[11], (FF,), 0.5, 3.0, ((0, 2),))
    w_down = gaussian(keys[12], (FF, D), FF ** -0.5, 0.109375, ((0, 2),))
    bias_down = gaussian(keys[13], (D,), 0.5, 3.0, ((0, 2),))
    gain_two = jnp.clip(1.0 + 0.1 * jax.random.normal(keys[14], (D,), jnp.float32), 0.5, 1.5).astype(jnp.bfloat16)
    shift_two = gaussian(keys[15], (D,), 0.5, 3.0, ((0, 2),))
    return {"tokens": tokens, "cotangent": cotangent, "lengths": lengths, "w_qkv": w_qkv, "bias_q": bias_q, "bias_v": bias_v, "w_out": w_out, "bias_out": bias_out, "gain_one": gain_one, "shift_one": shift_one, "w_up": w_up, "bias_up": bias_up, "w_down": w_down, "bias_down": bias_down, "gain_two": gain_two, "shift_two": shift_two}


@jax.custom_vjp
def low(v):
    return lax.optimization_barrier(v.astype(jnp.bfloat16)).astype(jnp.float32)

@jax.custom_vjp
def low_back(v):
    return v

def low_keep(v):
    return (low(v), None)

def low_pass(kept, grad):
    return (grad,)

def back_keep(v):
    return (v, None)

def back_low(kept, grad):
    return (low(grad),)
low.defvjp(low_keep, low_pass)
low_back.defvjp(back_keep, back_low)
EPSILON = 1e-12
MASKED = -1e+30
HIGHEST = lax.Precision.HIGHEST

def normalize(values, norm_gain, norm_shift):
    row_mean = lax.optimization_barrier(jnp.mean(values, -1, keepdims=True))
    centred = values - row_mean
    spread = lax.optimization_barrier(jnp.mean(centred * centred, -1, keepdims=True))
    return centred * lax.rsqrt(spread + EPSILON) * norm_gain + norm_shift

def product(left_op, right_op):
    return jnp.dot(left_op, right_op, precision=HIGHEST)

def attend(queries, key_rows, value_rows, length):
    positions = queries.shape[0]
    head_count = HEADS
    head_dim = queries.shape[1] // head_count
    score_scale = head_dim ** (-0.5)
    query_rows = math.gcd(positions, 512)
    key_heads = key_rows.reshape(positions, head_count, head_dim)
    value_heads = value_rows.reshape(positions, head_count, head_dim)
    key_live = (jnp.arange(positions) < length)[None, None, :]

    def one_block(query_block):
        query_heads = query_block.reshape(query_rows, head_count, head_dim)
        scores = low_back(jnp.einsum('qhe,khe->hqk', query_heads, key_heads, precision=HIGHEST) * score_scale)
        scores = jnp.where(key_live, scores, MASKED)
        highest = lax.optimization_barrier(jnp.max(scores, -1, keepdims=True))
        weights = jnp.where(key_live, jnp.exp(scores - highest), 0.0)
        chances = weights / lax.optimization_barrier(jnp.sum(weights, -1, keepdims=True))
        attended = jnp.einsum('hqk,khe->qhe', low(chances), value_heads, precision=HIGHEST)
        return attended.reshape(query_rows, head_count * head_dim)
    outcome = lax.map(jax.checkpoint(one_block), queries.reshape(positions // query_rows, query_rows, queries.shape[1]))
    return outcome.reshape(positions, queries.shape[1])

def forward(tokens_row, length, w_qkv, bias_q, bias_v, w_out, bias_out, gain_one, shift_one, w_up, bias_up, w_down, bias_down, gain_two, shift_two):
    model_width = tokens_row.shape[1]
    projected = product(tokens_row, w_qkv)
    queries = low(low_back(projected[:, :model_width] + bias_q))
    key_rows = low(low_back(projected[:, model_width:2 * model_width]))
    value_rows = low(low_back(projected[:, 2 * model_width:] + bias_v))
    attended = low(low_back(attend(queries, key_rows, value_rows, length)))
    branch_one = low_back(product(attended, w_out) + bias_out)
    normed = normalize(tokens_row + branch_one, gain_one, shift_one)
    hidden_pre = low_back(product(low(normed), w_up) + bias_up)
    hidden_act = low(jax.nn.gelu(hidden_pre, approximate=False))
    branch_two = low_back(product(hidden_act, w_down) + bias_down)
    return normalize(normed + branch_two, gain_two, shift_two)

def reference(tokens, cotangent, lengths, w_qkv, bias_q, bias_v, w_out, bias_out, gain_one, shift_one, w_up, bias_up, w_down, bias_down, gain_two, shift_two):
    weights = tuple((weight_arg.astype(jnp.float32) for weight_arg in (w_qkv, bias_q, bias_v, w_out, bias_out, gain_one, shift_one, w_up, bias_up, w_down, bias_down, gain_two, shift_two)))

    def per_sequence(partial_value, inputs):
        seq_tokens, seq_cotangent, length = inputs

        def run_layer(tokens_row, *params):
            return forward(tokens_row, length, *params)
        result, pullback = jax.vjp(run_layer, seq_tokens.astype(jnp.float32), *weights)
        gradients = pullback(seq_cotangent.astype(jnp.float32))
        summed = tuple((before + update for before, update in zip(partial_value, gradients[1:])))
        return (summed, (result.astype(jnp.bfloat16), gradients[0].astype(jnp.bfloat16)))
    initial = tuple((jnp.zeros(weight_arg.shape, jnp.float32) for weight_arg in weights))
    totals, (outputs, input_grads) = lax.scan(per_sequence, initial, (tokens, cotangent, lengths))
    return (outputs, input_grads, totals[0], totals[1], totals[2], totals[3], totals[4], totals[5], totals[6], totals[7], totals[8], totals[9], totals[10], totals[11], totals[12])
```

```python
import functools
import math

import jax
import jax.numpy as jnp
from jax import lax
from jax.experimental import pallas as pl
from jax.experimental.pallas import tpu as pltpu
from jax.sharding import PartitionSpec as P

MESH = pl.DeviceIdType.MESH
F32, BF16 = jnp.float32, jnp.bfloat16
U = 384
VR = 24


def places():
    c = lax.axis_index("ctx")
    return lax.rem(c, 2), c // 2, lax.axis_index("fsdp"), lax.axis_index("dp")


def grad_kernel(nx, nd, grp, wd, wu, wo, wq, vec, od, ou, oo, oq, ov,
                L, R1, R2, R3, R4, AX, AC, ST, V0, VX, VZ,
                s0, s1s, s1r, s2s, s2r, s3s, s3r, s4s, s4r, s5s, s5r, s6s, s6r, s7s, s7r, so, vs, vr):
    core, x, f, z = places()
    nch = 12 // grp
    CH, CX, PZ = U * grp, U * grp // nx, U * grp // nx // nd
    sib = {"ctx": x * 2 + 1 - core}
    yp = {"fsdp": 1 - f}
    xps = [{"ctx": lax.rem(x + j, nx) * 2 + core} for j in range(1, nx)]
    zps = [{"dp": lax.rem(z + j, nd)} for j in range(1, nd)]
    peers = [sib, yp] + xps + zps
    bar = pltpu.get_barrier_semaphore()
    for p in peers:
        pl.semaphore_signal(bar, inc=1, device_id=p, device_id_type=MESH)

    def rect(i, ff, cc):
        if i < 4:
            return wd, ff * 1536 + i * U, cc * U
        if i < 8:
            return wu, ff * U, cc * 1536 + (i - 4) * U
        if i < 9:
            return wo, ff * U, cc * U
        return wq, ff * U, cc * 1152 + (i - 9) * U

    def orect(i, cc):
        if i < 4:
            return od, i * U, cc * U
        if i < 8:
            return ou, 0, cc * 1536 + (i - 4) * U
        if i < 9:
            return oo, 0, cc * U
        return oq, 0, cc * 1152 + (i - 9) * U

    def sl(ref, r, c):
        return ref.at[pl.ds(pl.multiple_of(r, U), U), pl.ds(pl.multiple_of(c, 128), U)]

    def local(i, k):
        ff = (1 - f) if k == 0 else f
        return pltpu.make_async_copy(sl(*rect(i, ff, core)), L.at[i // grp, ff, pl.ds(i % grp * U, U)], s0.at[i, k])

    def remote(src, dst, ss, rs, dev):
        return pltpu.make_async_remote_copy(src_ref=src, dst_ref=dst, send_sem=ss, recv_sem=rs, device_id=dev, device_id_type=MESH)

    def c1(i, k):
        ff = (1 - f) if k == 0 else f
        return remote(sl(*rect(i, ff, 1 - core)), R1.at[i // grp, ff, pl.ds(i % grp * U, U)], s1s.at[i, k], s1r.at[i, k], sib)

    def c2(c):
        return remote(L.at[c, 1 - f], R2.at[c], s2s.at[c], s2r.at[c], yp)

    def c3(c, j):
        xt = lax.rem(x + j, nx)
        return remote(L.at[c, f, pl.ds(pl.multiple_of(xt * CX, CX), CX)], R3.at[c, j - 1], s3s.at[c, j - 1], s3r.at[c, j - 1], xps[j - 1])

    def mine(c, zz):
        return pl.ds(pl.multiple_of(x * CX + zz * PZ, PZ), PZ)

    def c4(c, j):
        zt = lax.rem(z + j, nd)
        return remote(L.at[c, f, mine(c, zt)], R4.at[c, j - 1], s4s.at[c, j - 1], s4r.at[c, j - 1], zps[j - 1])

    def c5(c, j):
        return remote(AX.at[c, mine(c, z)], AX.at[c, mine(c, z)], s5s.at[c, j - 1], s5r.at[c, j - 1], zps[j - 1])

    def c6(c, j):
        rows = pl.ds(pl.multiple_of(x * CX, CX), CX)
        return remote(AX.at[c, rows], AX.at[c, rows], s6s.at[c, j - 1], s6r.at[c, j - 1], xps[j - 1])

    def c7(c):
        return remote(AX.at[c], AC.at[c], s7s.at[c], s7r.at[c], sib)

    B = 48

    def rows_loop(n, fn):
        def bodyf(i, _):
            fn(pl.multiple_of(i * B, B))
            return 0
        lax.fori_loop(0, n // B, bodyf, 0)

    def up(v):
        return v.astype(F32)

    def st2(c):
        for k in range(grp):
            local(c * grp + k, 0).wait()
            c1(c * grp + k, 0).wait_recv()

        def fn(r):
            s = pl.ds(r, B)
            L[c, 1 - f, s, :] = (up(L[c, 1 - f, s, :]) + up(R1[c, 1 - f, s, :])).astype(BF16)
        rows_loop(CH, fn)
        c2(c).start()

    def st3(c):
        for k in range(grp):
            local(c * grp + k, 1).wait()
            c1(c * grp + k, 1).wait_recv()
        c2(c).wait_recv()
        for j in range(1, nx):
            xt = lax.rem(x + j, nx)

            def fn(r):
                s = pl.ds(pl.multiple_of(xt * CX + r, B), B)
                L[c, f, s, :] = (up(L[c, f, s, :]) + up(R1[c, f, s, :]) + up(R2[c, s, :])).astype(BF16)
            rows_loop(CX, fn)
            c3(c, j).start()

    def st4(c):
        for j in range(1, nx):
            c3(c, j).wait_recv()

        def fn(r):
            s = pl.ds(pl.multiple_of(x * CX + r, B), B)
            t = up(L[c, f, s, :]) + up(R1[c, f, s, :]) + up(R2[c, s, :])
            for j in range(1, nx):
                t = t + up(R3[c, j - 1, pl.ds(r, B), :])
            L[c, f, s, :] = t.astype(BF16)
        rows_loop(CX, fn)
        for j in range(1, nd):
            c4(c, j).start()

    def st5(c):
        for j in range(1, nd):
            c4(c, j).wait_recv()
        t = up(L[c, f, mine(c, z), :])
        for j in range(1, nd):
            t = t + up(R4[c, j - 1])
        AX[c, mine(c, z), :] = t.astype(BF16)
        for j in range(1, nd):
            c5(c, j).start()

    def st6(c):
        for j in range(1, nd):
            c5(c, j).wait_recv()
        for j in range(1, nx):
            c6(c, j).start()

    def outc(i, k, slot):
        cc = core if k == 0 else 1 - core
        return pltpu.make_async_copy(ST.at[slot], sl(*orect(i, cc)), so.at[slot])

    def emit(i, k, src):
        slot = emit.n % 4
        if emit.n >= 4:
            outc(*emit.log[emit.n - 4], slot).wait()
        off = i % grp * U

        def fn(r):
            ST[slot, pl.ds(r, B), :] = up(src[i // grp, pl.ds(pl.multiple_of(off + r, B), B), :])
        rows_loop(U, fn)
        outc(i, k, slot).start()
        emit.log.append((i, k))
        emit.n += 1
    emit.n = 0
    emit.log = []

    def st7(c):
        for j in range(1, nx):
            c6(c, j).wait_recv()
        c7(c).start()
        for k in range(grp):
            emit(c * grp + k, 0, AX)

    def st8(c):
        c7(c).wait_recv()
        for k in range(grp):
            emit(c * grp + k, 1, AC)

    def v_core():
        return remote(vec, V0.at[0], vs.at[0], vr.at[0], sib)

    def v_y():
        return remote(V0.at[1], V0.at[2], vs.at[1], vr.at[1], yp)

    def v_x(j):
        return remote(VX.at[x], VX.at[x], vs.at[1 + j], vr.at[1 + j], xps[j - 1])

    def v_z(j):
        return remote(VZ.at[z], VZ.at[z], vs.at[nx + j], vr.at[nx + j], zps[j - 1])

    def vst(k):
        if k == 0:
            v_core().start()
        elif k == 1:
            v_core().wait_recv()
            V0[1] = vec[...] + V0[0]
            v_y().start()
        elif k == 2:
            v_y().wait_recv()
            VX[x] = V0[1] + V0[2]
            for j in range(1, nx):
                v_x(j).start()
        elif k == 3:
            for j in range(1, nx):
                v_x(j).wait_recv()
            t = VX[0]
            for j in range(1, nx):
                t = t + VX[j]
            VZ[z] = t
            for j in range(1, nd):
                v_z(j).start()
        elif k == 4:
            for j in range(1, nd):
                v_z(j).wait_recv()
            t = VZ[0]
            for j in range(1, nd):
                t = t + VZ[j]
            ov[...] = t

    for i in range(12):
        local(i, 0).start()
    pl.semaphore_wait(bar, len(peers))
    for i in range(12):
        c1(i, 0).start()
    vst(0)
    for i in range(12):
        local(i, 1).start()
        c1(i, 1).start()
    stages = [(8, st8), (7, st7), (6, st6), (5, st5), (4, st4), (3, st3)]
    for t in range(nch + 8):
        if t < nch:
            st2(t)
        if 1 <= t <= 4:
            vst(t)
        for k, fn in stages:
            c = t - (k - 1)
            if 0 <= c < nch:
                fn(c)
    n = emit.n
    for q in range(max(0, n - 4), n):
        outc(*emit.log[q], q % 4).wait()
    for i in range(12):
        for k in range(2):
            c1(i, k).wait_send()
    for c in range(nch):
        c2(c).wait_send()
        c7(c).wait_send()
        for j in range(1, nx):
            c3(c, j).wait_send()
            c6(c, j).wait_send()
        for j in range(1, nd):
            c4(c, j).wait_send()
            c5(c, j).wait_send()
    v_core().wait_send()
    v_y().wait_send()
    for j in range(1, nx):
        v_x(j).wait_send()
    for j in range(1, nd):
        v_z(j).wait_send()


def grad_reduce(wd, wu, wo, wq, vec, nx, nd, cid):
    grp = nx * nd // 8
    nch = 12 // grp
    CH, CX, PZ = U * grp, U * grp // nx, U * grp // nx // nd
    anyspec = pl.BlockSpec(memory_space=pl.ANY)
    vspec = pl.BlockSpec(memory_space=pltpu.VMEM)
    D = pltpu.SemaphoreType.DMA
    V = pltpu.VMEM
    sems = [D((12, 2)), D((12, 2)), D((12, 2)), D((nch,)), D((nch,)), D((nch, nx - 1)), D((nch, nx - 1)),
            D((nch, nd - 1)), D((nch, nd - 1)), D((nch, nd - 1)), D((nch, nd - 1)), D((nch, nx - 1)), D((nch, nx - 1)),
            D((nch,)), D((nch,)), D((4,)), D((nx + nd,)), D((nx + nd,))]
    return pl.pallas_call(
        functools.partial(grad_kernel, nx, nd, grp),
        out_shape=(jax.ShapeDtypeStruct((1536, 768), F32), jax.ShapeDtypeStruct((U, 3072), F32),
                   jax.ShapeDtypeStruct((U, 768), F32), jax.ShapeDtypeStruct((U, 2304), F32),
                   jax.ShapeDtypeStruct((VR, U), F32)),
        in_specs=[anyspec] * 4 + [vspec],
        out_specs=(anyspec,) * 4 + (vspec,),
        scratch_shapes=[V((nch, 2, CH, U), BF16), V((nch, 2, CH, U), BF16), V((nch, CH, U), BF16),
                        V((nch, nx - 1, CX, U), BF16), V((nch, nd - 1, PZ, U), BF16),
                        V((nch, CH, U), BF16), V((nch, CH, U), BF16), V((4, U, U), F32),
                        V((3, VR, U), F32), V((nx, VR, U), F32), V((nd, VR, U), F32)] + sems,
        compiler_params=pltpu.CompilerParams(collective_id=cid, has_side_effects=True, vmem_limit_bytes=60 << 20),
        name="grad_reduce",
    )(wd, wu, wo, wq, vec)


HEADS = 12


EPSILON = 1e-12
MASKED = -1e30


def shifted(value, axis, steps):
    count = lax.axis_size(axis)
    pairs = [(source, (source + steps) % count) for source in range(count)]
    return lax.ppermute(value, axis, pairs)


def normalize(values, norm_gain, norm_shift):
    row_mean = jnp.mean(values, -1, keepdims=True)
    centred = values - row_mean
    spread = jnp.mean(centred * centred, -1, keepdims=True)
    return centred * lax.rsqrt(spread + EPSILON) * norm_gain + norm_shift


def gelu_exact(values):
    return jax.nn.gelu(values, approximate=False)


def row_dot(left_op, right_op):
    return jnp.dot(left_op, right_op, preferred_element_type=jnp.float32)


def left_dot(left_op, right_op):
    return lax.dot_general(
        left_op, right_op, (((0,), (0,)), ((), ())), preferred_element_type=jnp.float32
    )


def right_dot(left_op, right_op):
    return lax.dot_general(
        left_op, right_op, (((1,), (1,)), ((), ())), preferred_element_type=jnp.float32
    )


def body(
    tokens,
    cotangent,
    lengths,
    w_qkv,
    bias_q,
    bias_v,
    w_out,
    bias_out,
    gain_one,
    shift_one,
    w_up,
    bias_up,
    w_down,
    bias_down,
    gain_two,
    shift_two,
):
    seq_count, block_rows, model_width = tokens.shape
    head_count = HEADS
    head_dim = model_width // head_count
    all_rows = seq_count * block_rows
    score_scale = head_dim ** (-0.5)
    cycle_size = lax.axis_size("ctx")
    cycle_index = lax.axis_index("ctx")
    gathered = (
        lax.all_gather(w_qkv, "fsdp", axis=0, tiled=True),
        lax.all_gather(bias_q, "fsdp", axis=0, tiled=True),
        lax.all_gather(bias_v, "fsdp", axis=0, tiled=True),
        lax.all_gather(w_out, "fsdp", axis=0, tiled=True),
        lax.all_gather(bias_out, "fsdp", axis=0, tiled=True),
        lax.all_gather(gain_one, "fsdp", axis=0, tiled=True),
        lax.all_gather(shift_one, "fsdp", axis=0, tiled=True),
        lax.all_gather(w_up, "fsdp", axis=0, tiled=True),
        lax.all_gather(bias_up, "fsdp", axis=0, tiled=True),
        lax.all_gather(w_down, "fsdp", axis=0, tiled=True),
        lax.all_gather(bias_down, "fsdp", axis=0, tiled=True),
        lax.all_gather(gain_two, "fsdp", axis=0, tiled=True),
        lax.all_gather(shift_two, "fsdp", axis=0, tiled=True),
    )
    full_qkv, full_out, full_up, full_down = (gathered[0], gathered[3], gathered[7], gathered[9])
    add_q, add_v, add_out, scale_one, move_one, add_up, add_down, scale_two, move_two = [
        gathered[place].astype(jnp.float32) for place in (1, 2, 4, 5, 6, 8, 10, 11, 12)
    ]
    flat_tokens = tokens.reshape(all_rows, model_width)
    projected = row_dot(flat_tokens, full_qkv)
    queries = (
        (projected[:, :model_width] + add_q)
        .astype(jnp.bfloat16)
        .reshape(seq_count, block_rows, head_count, head_dim)
    )
    key_rows = (
        projected[:, model_width : 2 * model_width]
        .astype(jnp.bfloat16)
        .reshape(seq_count, block_rows, model_width)
    )
    value_rows = (
        (projected[:, 2 * model_width :] + add_v)
        .astype(jnp.bfloat16)
        .reshape(seq_count, block_rows, model_width)
    )
    start_state = (
        jnp.full((seq_count, block_rows, head_count), MASKED, jnp.float32),
        jnp.zeros((seq_count, block_rows, head_count), jnp.float32),
        jnp.zeros((seq_count, block_rows, head_count, head_dim), jnp.float32),
    )
    key_part = lax.all_gather(key_rows, "ctx", axis=1, tiled=True)
    value_part = lax.all_gather(value_rows, "ctx", axis=1, tiled=True)
    key_count = key_part.shape[1]
    sub_rows = math.gcd(key_count, 512)

    def visit(block_index, carried):
        first_key = block_index * sub_rows
        key_block = lax.dynamic_slice_in_dim(key_part, block_index * sub_rows, sub_rows, 1).reshape(
            seq_count, sub_rows, head_count, head_dim
        )
        value_block = lax.dynamic_slice_in_dim(
            value_part, block_index * sub_rows, sub_rows, 1
        ).reshape(seq_count, sub_rows, head_count, head_dim)
        peak, weight_sum, weighted = carried
        key_live = (
            (first_key + jnp.arange(sub_rows, dtype=jnp.int32))[None, :] < lengths[:, None]
        )[:, None, None, :]
        scores = (
            jnp.einsum("sqhe,skhe->sqhk", queries, key_block, preferred_element_type=jnp.float32)
            * score_scale
        )
        scores = jnp.where(key_live, scores, MASKED)
        new_peak = jnp.maximum(peak, jnp.max(scores, -1))
        factor = jnp.exp(peak - new_peak)
        weights = jnp.where(key_live, jnp.exp(scores - new_peak[..., None]), 0.0)
        mixed_values = jnp.einsum(
            "sqhk,skhe->sqhe",
            weights.astype(jnp.bfloat16),
            value_block,
            preferred_element_type=jnp.float32,
        )
        return (
            new_peak,
            weight_sum * factor + jnp.sum(weights, -1),
            weighted * factor[..., None] + mixed_values,
        )

    peak, weight_sum, weighted = lax.fori_loop(0, key_count // sub_rows, visit, start_state)
    log_total = peak + jnp.log(weight_sum)
    attended = weighted / weight_sum[..., None]
    attended_low = attended.astype(jnp.bfloat16).reshape(all_rows, model_width)
    first_sum = flat_tokens.astype(jnp.float32) + row_dot(attended_low, full_out) + add_out
    normed, norm_pull = jax.vjp(normalize, first_sum, scale_one, move_one)
    normed_low = normed.astype(jnp.bfloat16)
    hidden_pre = row_dot(normed_low, full_up) + add_up
    hidden_act, gelu_pull = jax.vjp(gelu_exact, hidden_pre)
    hidden_low = hidden_act.astype(jnp.bfloat16)
    second_sum = normed + row_dot(hidden_low, full_down) + add_down
    result, result_pull = jax.vjp(normalize, second_sum, scale_two, move_two)
    grad_second, grad_gain_two, grad_shift_two = result_pull(
        cotangent.reshape(all_rows, model_width).astype(jnp.float32)
    )
    down_low = grad_second.astype(jnp.bfloat16)
    grad_w_down = left_dot(hidden_low, down_low)
    grad_bias_down = jnp.sum(down_low.astype(jnp.float32), 0)
    (grad_pre,) = gelu_pull(right_dot(down_low, full_down))
    up_low = grad_pre.astype(jnp.bfloat16)
    grad_w_up = left_dot(normed_low, up_low)
    grad_bias_up = jnp.sum(up_low.astype(jnp.float32), 0)
    grad_first, grad_gain_one, grad_shift_one = norm_pull(grad_second + right_dot(up_low, full_up))
    branch_low = grad_first.astype(jnp.bfloat16)
    grad_w_out = left_dot(attended_low, branch_low)
    grad_bias_out = jnp.sum(branch_low.astype(jnp.float32), 0)
    grad_att = (
        right_dot(branch_low, full_out)
        .astype(jnp.bfloat16)
        .reshape(seq_count, block_rows, head_count, head_dim)
    )
    delta_rows = jnp.sum(grad_att.astype(jnp.float32) * attended, -1)

    def block_grads(query_part, grad_part, lse_part, delta_part, key_block, value_block, first_key):
        key_count = key_block.shape[1]
        key_heads = key_block.reshape(seq_count, key_count, head_count, head_dim)
        value_heads = value_block.reshape(seq_count, key_count, head_count, head_dim)
        key_live = (
            (first_key + jnp.arange(key_count, dtype=jnp.int32))[None, :] < lengths[:, None]
        )[:, None, None, :]
        scores = (
            jnp.einsum("sqhe,skhe->sqhk", query_part, key_heads, preferred_element_type=jnp.float32)
            * score_scale
        )
        chances = jnp.where(key_live, jnp.exp(scores - lse_part[..., None]), 0.0)
        grad_value = jnp.einsum(
            "sqhk,sqhe->skhe",
            chances.astype(jnp.bfloat16),
            grad_part,
            preferred_element_type=jnp.float32,
        )
        grad_chance = jnp.einsum(
            "sqhe,skhe->sqhk", grad_part, value_heads, preferred_element_type=jnp.float32
        )
        grad_score = (chances * (grad_chance - delta_part[..., None])).astype(jnp.bfloat16)
        grad_query = (
            jnp.einsum("sqhk,skhe->sqhe", grad_score, key_heads, preferred_element_type=jnp.float32)
            * score_scale
        )
        grad_key = (
            jnp.einsum(
                "sqhk,sqhe->skhe", grad_score, query_part, preferred_element_type=jnp.float32
            )
            * score_scale
        )
        return (
            grad_query,
            grad_key.reshape(seq_count, key_count, model_width),
            grad_value.reshape(seq_count, key_count, model_width),
        )

    query_start = jnp.zeros((seq_count, block_rows, head_count, head_dim), jnp.float32)

    def key_terms(key_block, value_block, first_key):
        return block_grads(
            queries, grad_att, log_total, delta_rows, key_block, value_block, first_key
        )

    def block_terms(key_block, value_block, first_key):
        return key_terms(key_block, value_block, first_key)

    def turn(step_index, carried):
        key_now, value_now, key_grads, query_acc = carried
        first_key = (cycle_index - step_index) % cycle_size * block_rows
        add_query, add_key, add_value = block_terms(key_now, value_now, first_key)
        key_now, value_now = shifted((key_now, value_now), "ctx", 1)
        key_grads = (
            shifted((key_grads[0] + add_key).astype(jnp.bfloat16), "ctx", 1).astype(jnp.float32),
            shifted((key_grads[1] + add_value).astype(jnp.bfloat16), "ctx", 1).astype(jnp.float32),
        )
        return (key_now, value_now, key_grads, query_acc + add_query)

    grad_start = (
        jnp.zeros((seq_count, block_rows, model_width), jnp.float32),
        jnp.zeros((seq_count, block_rows, model_width), jnp.float32),
    )
    key_final, value_final, key_grads, query_grad = lax.fori_loop(
        0, cycle_size, turn, (key_rows, value_rows, grad_start, query_start)
    )
    grad_key, grad_value = key_grads
    qkv_grad = jnp.concatenate(
        [
            query_grad.astype(jnp.bfloat16).reshape(all_rows, model_width),
            grad_key.astype(jnp.bfloat16).reshape(all_rows, model_width),
            grad_value.astype(jnp.bfloat16).reshape(all_rows, model_width),
        ],
        1,
    )
    grad_w_qkv = left_dot(flat_tokens, qkv_grad)
    grad_bias_q = jnp.sum(qkv_grad[:, :model_width].astype(jnp.float32), 0)
    grad_bias_v = jnp.sum(qkv_grad[:, 2 * model_width :].astype(jnp.float32), 0)
    grad_input = grad_first + right_dot(qkv_grad, full_qkv)
    vectors = (
        grad_bias_q,
        grad_bias_v,
        grad_bias_out,
        grad_gain_one,
        grad_shift_one,
        grad_bias_up,
        grad_bias_down,
        grad_gain_two,
        grad_shift_two,
    )
    packed = jnp.concatenate(vectors).reshape(VR, U)
    t_down, t_up, t_out, t_qkv, t_vec = grad_reduce(
        grad_w_down.astype(BF16),
        grad_w_up.astype(BF16),
        grad_w_out.astype(BF16),
        grad_w_qkv.astype(BF16),
        packed,
        cycle_size // 2,
        lax.axis_size("dp"),
        1,
    )
    flat = t_vec.reshape(-1)
    own = lax.axis_index("fsdp")
    parts, start = [], 0
    for vector in vectors:
        half = vector.shape[0] // 2
        parts.append(lax.dynamic_slice_in_dim(flat, start + own * half, half, 0))
        start += 2 * half
    totals = (
        t_qkv, parts[0], parts[1], t_out, parts[2], parts[3], parts[4],
        t_up, parts[5], t_down, parts[6], parts[7], parts[8],
    )
    output_rows = result.astype(jnp.bfloat16).reshape(seq_count, block_rows, model_width)
    input_rows = grad_input.astype(jnp.bfloat16).reshape(seq_count, block_rows, model_width)
    return (
        output_rows,
        input_rows,
        totals[0],
        totals[1],
        totals[2],
        totals[3],
        totals[4],
        totals[5],
        totals[6],
        totals[7],
        totals[8],
        totals[9],
        totals[10],
        totals[11],
        totals[12],
    )


def solution(mesh):
    return jax.shard_map(
        body,
        mesh=mesh,
        in_specs=(
            P(("dp", "fsdp"), "ctx", None),
            P(("dp", "fsdp"), "ctx", None),
            P(("dp", "fsdp")),
            P("fsdp", None),
            P("fsdp"),
            P("fsdp"),
            P("fsdp", None),
            P("fsdp"),
            P("fsdp"),
            P("fsdp"),
            P("fsdp", None),
            P("fsdp"),
            P("fsdp", None),
            P("fsdp"),
            P("fsdp"),
            P("fsdp"),
        ),
        out_specs=(
            P(("dp", "fsdp"), "ctx", None),
            P(("dp", "fsdp"), "ctx", None),
            P("fsdp", None),
            P("fsdp"),
            P("fsdp"),
            P("fsdp", None),
            P("fsdp"),
            P("fsdp"),
            P("fsdp"),
            P("fsdp", None),
            P("fsdp"),
            P("fsdp", None),
            P("fsdp"),
            P("fsdp"),
            P("fsdp"),
        ),
        check_vma=False,
    )
```

```python
import functools
import math

import jax
import jax.numpy as jnp
from jax import lax
from jax.experimental import pallas as pl
from jax.experimental.pallas import tpu as pltpu
from jax.sharding import PartitionSpec as P

MESH = pl.DeviceIdType.MESH
F32, BF16 = jnp.float32, jnp.bfloat16
U = 384
VR = 24


def places():
    c = lax.axis_index("ctx")
    return lax.rem(c, 2), c // 2, lax.axis_index("fsdp"), lax.axis_index("dp")


def grad_kernel(nx, nd, grp, wd, wu, wo, wq, vec, od, ou, oo, oq, ov,
                L, R1, R2, R3, R4, AX, AC, ST, V0, VX, VZ,
                s0, s1s, s1r, s2s, s2r, s3s, s3r, s4s, s4r, s5s, s5r, s6s, s6r, s7s, s7r, so, vs, vr):
    core, x, f, z = places()
    nch = 12 // grp
    CH, CX, PZ = U * grp, U * grp // nx, U * grp // nx // nd
    sib = {"ctx": x * 2 + 1 - core}
    yp = {"fsdp": 1 - f}
    xps = [{"ctx": lax.rem(x + j, nx) * 2 + core} for j in range(1, nx)]
    zps = [{"dp": lax.rem(z + j, nd)} for j in range(1, nd)]
    peers = [sib, yp] + xps + zps
    bar = pltpu.get_barrier_semaphore()
    for p in peers:
        pl.semaphore_signal(bar, inc=1, device_id=p, device_id_type=MESH)

    def rect(i, ff, cc):
        if i < 4:
            return wd, ff * 1536 + i * U, cc * U
        if i < 8:
            return wu, ff * U, cc * 1536 + (i - 4) * U
        if i < 9:
            return wo, ff * U, cc * U
        return wq, ff * U, cc * 1152 + (i - 9) * U

    def orect(i, cc):
        if i < 4:
            return od, i * U, cc * U
        if i < 8:
            return ou, 0, cc * 1536 + (i - 4) * U
        if i < 9:
            return oo, 0, cc * U
        return oq, 0, cc * 1152 + (i - 9) * U

    def sl(ref, r, c):
        return ref.at[pl.ds(pl.multiple_of(r, U), U), pl.ds(pl.multiple_of(c, 128), U)]

    def local(i, k):
        ff = (1 - f) if k == 0 else f
        return pltpu.make_async_copy(sl(*rect(i, ff, core)), L.at[i // grp, ff, pl.ds(i % grp * U, U)], s0.at[i, k])

    def remote(src, dst, ss, rs, dev):
        return pltpu.make_async_remote_copy(src_ref=src, dst_ref=dst, send_sem=ss, recv_sem=rs, device_id=dev, device_id_type=MESH)

    def c1(i, k):
        ff = (1 - f) if k == 0 else f
        return remote(sl(*rect(i, ff, 1 - core)), R1.at[i // grp, ff, pl.ds(i % grp * U, U)], s1s.at[i, k], s1r.at[i, k], sib)

    def c2(c):
        return remote(L.at[c, 1 - f], R2.at[c], s2s.at[c], s2r.at[c], yp)

    def c3(c, j):
        xt = lax.rem(x + j, nx)
        return remote(L.at[c, f, pl.ds(pl.multiple_of(xt * CX, CX), CX)], R3.at[c, j - 1], s3s.at[c, j - 1], s3r.at[c, j - 1], xps[j - 1])

    def mine(c, zz):
        return pl.ds(pl.multiple_of(x * CX + zz * PZ, PZ), PZ)

    def c4(c, j):
        zt = lax.rem(z + j, nd)
        return remote(L.at[c, f, mine(c, zt)], R4.at[c, j - 1], s4s.at[c, j - 1], s4r.at[c, j - 1], zps[j - 1])

    def c5(c, j):
        return remote(AX.at[c, mine(c, z)], AX.at[c, mine(c, z)], s5s.at[c, j - 1], s5r.at[c, j - 1], zps[j - 1])

    def c6(c, j):
        rows = pl.ds(pl.multiple_of(x * CX, CX), CX)
        return remote(AX.at[c, rows], AX.at[c, rows], s6s.at[c, j - 1], s6r.at[c, j - 1], xps[j - 1])

    def c7(c):
        return remote(AX.at[c], AC.at[c], s7s.at[c], s7r.at[c], sib)

    B = 48

    def rows_loop(n, fn):
        def bodyf(i, _):
            fn(pl.multiple_of(i * B, B))
            return 0
        lax.fori_loop(0, n // B, bodyf, 0)

    def up(v):
        return v.astype(F32)

    def st2(c):
        for k in range(grp):
            local(c * grp + k, 0).wait()
            c1(c * grp + k, 0).wait_recv()

        def fn(r):
            s = pl.ds(r, B)
            L[c, 1 - f, s, :] = (up(L[c, 1 - f, s, :]) + up(R1[c, 1 - f, s, :])).astype(BF16)
        rows_loop(CH, fn)
        c2(c).start()

    def st3(c):
        for k in range(grp):
            local(c * grp + k, 1).wait()
            c1(c * grp + k, 1).wait_recv()
        c2(c).wait_recv()
        for j in range(1, nx):
            xt = lax.rem(x + j, nx)

            def fn(r):
                s = pl.ds(pl.multiple_of(xt * CX + r, B), B)
                L[c, f, s, :] = (up(L[c, f, s, :]) + up(R1[c, f, s, :]) + up(R2[c, s, :])).astype(BF16)
            rows_loop(CX, fn)
            c3(c, j).start()

    def st4(c):
        for j in range(1, nx):
            c3(c, j).wait_recv()

        def fn(r):
            s = pl.ds(pl.multiple_of(x * CX + r, B), B)
            t = up(L[c, f, s, :]) + up(R1[c, f, s, :]) + up(R2[c, s, :])
            for j in range(1, nx):
                t = t + up(R3[c, j - 1, pl.ds(r, B), :])
            L[c, f, s, :] = t.astype(BF16)
        rows_loop(CX, fn)
        for j in range(1, nd):
            c4(c, j).start()

    def st5(c):
        for j in range(1, nd):
            c4(c, j).wait_recv()
        t = up(L[c, f, mine(c, z), :])
        for j in range(1, nd):
            t = t + up(R4[c, j - 1])
        AX[c, mine(c, z), :] = t.astype(BF16)
        for j in range(1, nd):
            c5(c, j).start()

    def st6(c):
        for j in range(1, nd):
            c5(c, j).wait_recv()
        for j in range(1, nx):
            c6(c, j).start()

    def outc(i, k, slot):
        cc = core if k == 0 else 1 - core
        return pltpu.make_async_copy(ST.at[slot], sl(*orect(i, cc)), so.at[slot])

    def emit(i, k, src):
        slot = emit.n % 4
        if emit.n >= 4:
            outc(*emit.log[emit.n - 4], slot).wait()
        off = i % grp * U

        def fn(r):
            ST[slot, pl.ds(r, B), :] = up(src[i // grp, pl.ds(pl.multiple_of(off + r, B), B), :])
        rows_loop(U, fn)
        outc(i, k, slot).start()
        emit.log.append((i, k))
        emit.n += 1
    emit.n = 0
    emit.log = []

    def st7(c):
        for j in range(1, nx):
            c6(c, j).wait_recv()
        c7(c).start()
        for k in range(grp):
            emit(c * grp + k, 0, AX)

    def st8(c):
        c7(c).wait_recv()
        for k in range(grp):
            emit(c * grp + k, 1, AC)

    def v_core():
        return remote(vec, V0.at[0], vs.at[0], vr.at[0], sib)

    def v_y():
        return remote(V0.at[1], V0.at[2], vs.at[1], vr.at[1], yp)

    def v_x(j):
        return remote(VX.at[x], VX.at[x], vs.at[1 + j], vr.at[1 + j], xps[j - 1])

    def v_z(j):
        return remote(VZ.at[z], VZ.at[z], vs.at[nx + j], vr.at[nx + j], zps[j - 1])

    def vst(k):
        if k == 0:
            v_core().start()
        elif k == 1:
            v_core().wait_recv()
            V0[1] = vec[...] + V0[0]
            v_y().start()
        elif k == 2:
            v_y().wait_recv()
            VX[x] = V0[1] + V0[2]
            for j in range(1, nx):
                v_x(j).start()
        elif k == 3:
            for j in range(1, nx):
                v_x(j).wait_recv()
            t = VX[0]
            for j in range(1, nx):
                t = t + VX[j]
            VZ[z] = t
            for j in range(1, nd):
                v_z(j).start()
        elif k == 4:
            for j in range(1, nd):
                v_z(j).wait_recv()
            t = VZ[0]
            for j in range(1, nd):
                t = t + VZ[j]
            ov[...] = t

    for i in range(12):
        local(i, 0).start()
    pl.semaphore_wait(bar, len(peers))
    for i in range(12):
        c1(i, 0).start()
    vst(0)
    for i in range(12):
        local(i, 1).start()
        c1(i, 1).start()
    stages = [(8, st8), (7, st7), (6, st6), (5, st5), (4, st4), (3, st3)]
    for t in range(nch + 8):
        if t < nch:
            st2(t)
        if 1 <= t <= 4:
            vst(t)
        for k, fn in stages:
            c = t - (k - 1)
            if 0 <= c < nch:
                fn(c)
    n = emit.n
    for q in range(max(0, n - 4), n):
        outc(*emit.log[q], q % 4).wait()
    for i in range(12):
        for k in range(2):
            c1(i, k).wait_send()
    for c in range(nch):
        c2(c).wait_send()
        c7(c).wait_send()
        for j in range(1, nx):
            c3(c, j).wait_send()
            c6(c, j).wait_send()
        for j in range(1, nd):
            c4(c, j).wait_send()
            c5(c, j).wait_send()
    v_core().wait_send()
    v_y().wait_send()
    for j in range(1, nx):
        v_x(j).wait_send()
    for j in range(1, nd):
        v_z(j).wait_send()


def grad_reduce(wd, wu, wo, wq, vec, nx, nd, cid):
    grp = nx * nd // 8
    nch = 12 // grp
    CH, CX, PZ = U * grp, U * grp // nx, U * grp // nx // nd
    anyspec = pl.BlockSpec(memory_space=pl.ANY)
    vspec = pl.BlockSpec(memory_space=pltpu.VMEM)
    D = pltpu.SemaphoreType.DMA
    V = pltpu.VMEM
    sems = [D((12, 2)), D((12, 2)), D((12, 2)), D((nch,)), D((nch,)), D((nch, nx - 1)), D((nch, nx - 1)),
            D((nch, nd - 1)), D((nch, nd - 1)), D((nch, nd - 1)), D((nch, nd - 1)), D((nch, nx - 1)), D((nch, nx - 1)),
            D((nch,)), D((nch,)), D((4,)), D((nx + nd,)), D((nx + nd,))]
    return pl.pallas_call(
        functools.partial(grad_kernel, nx, nd, grp),
        out_shape=(jax.ShapeDtypeStruct((1536, 768), F32), jax.ShapeDtypeStruct((U, 3072), F32),
                   jax.ShapeDtypeStruct((U, 768), F32), jax.ShapeDtypeStruct((U, 2304), F32),
                   jax.ShapeDtypeStruct((VR, U), F32)),
        in_specs=[anyspec] * 4 + [vspec],
        out_specs=(anyspec,) * 4 + (vspec,),
        scratch_shapes=[V((nch, 2, CH, U), BF16), V((nch, 2, CH, U), BF16), V((nch, CH, U), BF16),
                        V((nch, nx - 1, CX, U), BF16), V((nch, nd - 1, PZ, U), BF16),
                        V((nch, CH, U), BF16), V((nch, CH, U), BF16), V((4, U, U), F32),
                        V((3, VR, U), F32), V((nx, VR, U), F32), V((nd, VR, U), F32)] + sems,
        compiler_params=pltpu.CompilerParams(collective_id=cid, has_side_effects=True, vmem_limit_bytes=60 << 20),
        name="grad_reduce",
    )(wd, wu, wo, wq, vec)


HW = 64
QT = 256
MASKED = -1e30


def remote(src, dst, ss, rs, dev):
    return pltpu.make_async_remote_copy(src_ref=src, dst_ref=dst, send_sem=ss, recv_sem=rs, device_id=dev, device_id_type=MESH)


def nt(a, b):
    return lax.dot_general(a, b, (((1,), (1,)), ((), ())), preferred_element_type=F32)


def mm(a, b):
    return jnp.dot(a, b, preferred_element_type=F32)


def head_masks(rows):
    lane = lax.broadcasted_iota(jnp.int32, (rows, 2 * HW), 1)
    return lane < HW


def fwd_kernel(nx, seqs, seq_rows, lens, tok, sq, so_, su, sd, vec,
               qkv_o, att_o, lse_o, wq_o, wo_o, wu_o, wd_o, vec_o,
               XT, WB, QKV,
               ls, ys, yr, zs, zr, as_, ar, bs, br, t0s, t0r, t1s, t1r, t2s, t2r, vs, vr, lts, outs):
    core, x, f, z = places()
    me = x * 2 + core
    nblk = 2 * nx
    rows = seqs * seq_rows
    sib = {"ctx": x * 2 + 1 - core}
    yp = {"fsdp": 1 - f}
    zp = {"dp": z + 1 - 2 * lax.rem(z, 2)}
    zb = lax.rem(z, 2)
    xts = [lax.rem(x + j, nx) for j in range(1, nx)]
    xps = [{"ctx": t * 2 + core} for t in xts]
    xsrc = [lax.rem(x + nx - j, nx) * 2 + core for j in range(1, nx)]
    peers = [sib, yp, zp] + xps
    bar = pltpu.get_barrier_semaphore()
    for p in peers:
        pl.semaphore_signal(bar, inc=1, device_id=p, device_id_type=MESH)
    order = (1, 2, 0)
    PR = U // 4
    piece = pl.multiple_of((zb * 2 + core) * PR, PR)
    zpiece = pl.multiple_of(((1 - zb) * 2 + core) * PR, PR)
    H = rows // 2

    def shard(b, r0, n):
        r = pl.ds(r0, n)
        if b < 3:
            return sq.at[r, pl.ds(b * 768, 768)]
        if b == 3:
            return so_.at[r, :]
        if b < 8:
            return su.at[r, pl.ds((b - 4) * 768, 768)]
        return sd.at[pl.ds((b - 8) * U + r0, n), :]

    def loc(b):
        return pltpu.make_async_copy(shard(b, 0, U), WB.at[b, f], ls.at[b])

    def ycp(b):
        if not isinstance(b, int):
            src = WB.at[b, f, pl.ds(piece, PR)]
        else:
            src = shard(b, piece, PR)
        return remote(src, WB.at[b, f, pl.ds(piece, PR)], ys.at[b], yr.at[b], yp)

    def zcp(b):
        w = WB.at[b, 1 - f, pl.ds(piece, PR)]
        return remote(w, w, zs.at[b], zr.at[b], zp)

    def acp(b):
        w = WB.at[b, 1 - f, pl.ds(piece, PR)]
        return remote(w, w, as_.at[b], ar.at[b], sib)

    def bcp(b):
        w = WB.at[b, 1 - f, pl.ds(zpiece, PR)]
        return remote(w, w, bs.at[b], br.at[b], sib)

    def A(b):
        ycp(b).wait_recv()
        zcp(b).start()
        acp(b).start()

    def B(b):
        zcp(b).wait_recv()
        bcp(b).start()

    def C(b):
        acp(b).wait_recv()
        bcp(b).wait_recv()

    def tsl(h):
        return pl.ds(h * H, H)

    def t_sib(h):
        return remote(tok.at[tsl(h)], XT.at[me, tsl(h)], t0s.at[h], t0r.at[h], sib)

    def t_x(j, h):
        return remote(tok.at[tsl(h)], XT.at[me, tsl(h)], t1s.at[j - 1, h], t1r.at[j - 1, h], xps[j - 1])

    def t_f(j, h):
        w = XT.at[xsrc[j - 1], tsl(h)]
        return remote(w, w, t2s.at[j - 1, h], t2r.at[j - 1, h], sib)

    vcp = remote(vec, vec_o.at[f], vs.at[0], vr.at[0], yp)
    tl = pltpu.make_async_copy(tok, XT.at[me], lts.at[0])
    tl.start()
    for b in order:
        loc(b).start()
    vec_o[f] = vec[...]
    pl.semaphore_wait(bar, len(peers))
    vcp.start()
    for b in order:
        ycp(b).start()
    for h in range(2):
        for j in range(1, nx):
            t_x(j, h).start()
        t_sib(h).start()
    for b in range(3, 12):
        ycp(b).start()
    for b in range(3, 12):
        loc(b).start()
    tl.wait()

    def qkv(b, blk):
        fac = 0.125 if b == 0 else 1.0

        def one(t, _):
            c = pl.ds(pl.multiple_of(t * 256, 256), 256)
            w = WB[b, :, :, c].reshape(768, 256)
            QKV[b, blk, :, c] = mm(XT[blk], w).astype(BF16)
            return 0
        if b == 1:
            lax.fori_loop(0, 3, one, 0)
        else:
            row = 0 if b == 0 else 1
            for t in range(3):
                w = WB[b, :, :, t * 256:(t + 1) * 256].reshape(768, 256)
                if t == 0:
                    bias = vec_o[0, row:row + 1, 0:256]
                elif t == 1:
                    bias = jnp.concatenate([vec_o[0, row:row + 1, 256:384], vec_o[1, row:row + 1, 0:128]], 1)
                else:
                    bias = vec_o[1, row:row + 1, 128:384]
                r = (mm(XT[blk], w) + bias).astype(BF16)
                if b == 0:
                    r = r * jnp.asarray(fac, BF16)
                QKV[b, blk, :, t * 256:(t + 1) * 256] = r

    seq = list(order)
    A(seq[0])
    A(seq[1])
    B(seq[0])
    for h in range(2):
        t_sib(h).wait_recv()
    A(seq[2])
    B(seq[1])
    vcp.wait_recv()
    for n, b in enumerate(seq):
        loc(b).wait()
        C(b)

        def both(i, _):
            qkv(b, x * 2 + i)
            return 0
        lax.fori_loop(0, 2, both, 0)
        if n == 0:
            B(seq[2])
            A(3)
        if n == 1:
            B(3)
            A(4)
    for j in range(1, nx):
        for h in range(2):
            t_x(j, h).wait_recv()
            t_f(j, h).start()
    B(4)
    A(5)
    for j in range(1, nx):
        for h in range(2):
            t_f(j, h).wait_recv()
        base = lax.rem(x + nx - j, nx) * 2

        def pair(i, _):
            for b in seq:
                qkv(b, base + i)
            return 0
        lax.fori_loop(0, 2, pair, 0)
    B(5)
    qo = pltpu.make_async_copy(QKV, qkv_o, outs.at[0])
    qo.start()

    low_half = head_masks(QT)
    lane128 = lax.broadcasted_iota(jnp.int32, (QT, 128), 1)
    kpos = lax.broadcasted_iota(jnp.int32, (QT, QT), 1)
    nr = seq_rows // QT

    def attend(tile, j):
        s0 = tile // nr
        qr = pl.ds(pl.multiple_of(tile * QT, QT), QT)
        cols = pl.ds(pl.multiple_of(j * 128, 128), 128)
        q = QKV[0, me, qr, cols]
        length = lens[s0]
        outs_ = []
        tot = lse_o[qr, :]
        for h in range(2):
            qh = jnp.where(low_half == (h == 0), q, jnp.zeros_like(q))
            sc = []
            mx = None
            for blk in range(nblk):
                for r in range(nr):
                    kr = pl.ds(pl.multiple_of(s0 * seq_rows + r * QT, QT), QT)
                    v = nt(qh, QKV[1, blk, kr, cols])
                    v = jnp.where(kpos < length - (blk * seq_rows + r * QT), v, MASKED)
                    sc.append(v)
                    mx = v if mx is None else jnp.maximum(mx, v)
            m = jnp.max(mx, 1, keepdims=True)
            acc = None
            lsum = None
            i = 0
            for blk in range(nblk):
                for r in range(nr):
                    kr = pl.ds(pl.multiple_of(s0 * seq_rows + r * QT, QT), QT)
                    p = jnp.exp(sc[i] - m)
                    i += 1
                    lsum = p if lsum is None else lsum + p
                    o = mm(p.astype(BF16), QKV[2, blk, kr, cols])
                    acc = o if acc is None else acc + o
            den = jnp.sum(lsum, 1, keepdims=True)
            outs_.append(acc / den)
            tot = jnp.where(lane128 == 2 * j + h, m + jnp.log(den), tot)
        att_o[qr, cols] = jnp.where(low_half, outs_[0], outs_[1])
        lse_o[qr, :] = tot

    ntile = rows // QT
    per = ntile * 6 // 4

    def group(g, _):
        A(6 + g)

        def one(i, _):
            it = g * per + i
            attend(it // 6, lax.rem(it, 6))
            return 0
        lax.fori_loop(0, per, one, 0)
        B(6 + g)
        return 0
    lax.fori_loop(0, 4, group, 0)
    A(10)
    A(11)

    def full(b):
        res = []
        for ff in range(2):
            src = WB.at[b, ff]
            if b < 3:
                dst = wq_o.at[pl.ds(ff * U, U), pl.ds(b * 768, 768)]
            elif b == 3:
                dst = wo_o.at[pl.ds(ff * U, U), :]
            elif b < 8:
                dst = wu_o.at[pl.ds(ff * U, U), pl.ds((b - 4) * 768, 768)]
            else:
                dst = wd_o.at[pl.ds(ff * 1536 + (b - 8) * U, U), :]
            res.append(pltpu.make_async_copy(src, dst, outs.at[1 + 2 * b + ff]))
        return res

    for b in range(3):
        for cp in full(b):
            cp.start()
    for b in range(3, 10):
        loc(b).wait()
        C(b)
        for cp in full(b):
            cp.start()
    for b in range(10, 12):
        B(b)
    for b in range(10, 12):
        loc(b).wait()
        C(b)
        for cp in full(b):
            cp.start()
    vcp.wait_send()
    qo.wait()
    for b in range(12):
        ycp(b).wait_send()
        zcp(b).wait_send()
        acp(b).wait_send()
        bcp(b).wait_send()
        for cp in full(b):
            cp.wait()
    for h in range(2):
        t_sib(h).wait_send()
        for j in range(1, nx):
            t_x(j, h).wait_send()
            t_f(j, h).wait_send()


def forward_gather(lens, tok, sq, so_, su, sd, vec, nx, cid):
    seqs, seq_rows, d = tok.shape
    rows = seqs * seq_rows
    nblk = 2 * nx
    anyspec = pl.BlockSpec(memory_space=pl.ANY)
    vspec = pl.BlockSpec(memory_space=pltpu.VMEM)
    sspec = pl.BlockSpec(memory_space=pltpu.SMEM)
    D = pltpu.SemaphoreType.DMA
    V = pltpu.VMEM
    S = jax.ShapeDtypeStruct
    sems = [D((12,))] * 9 + [D((2,)), D((2,))] + [D((nx - 1, 2))] * 4 + [D((1,)), D((1,)), D((1,)), D((25,))]
    return pl.pallas_call(
        functools.partial(fwd_kernel, nx, seqs, seq_rows),
        out_shape=(S((3, nblk, rows, d), BF16), S((rows, d), F32), S((rows, 128), F32),
                   S((768, 2304), BF16), S((768, 768), BF16), S((768, 3072), BF16), S((3072, 768), BF16),
                   S((2, 12, U), F32)),
        in_specs=[sspec, anyspec, anyspec, anyspec, anyspec, anyspec, vspec],
        out_specs=(anyspec, vspec, vspec, anyspec, anyspec, anyspec, anyspec, vspec),
        scratch_shapes=[V((nblk, rows, d), BF16), V((12, 2, U, 768), BF16), V((3, nblk, rows, d), BF16)] + sems,
        compiler_params=pltpu.CompilerParams(collective_id=cid, has_side_effects=True, vmem_limit_bytes=60 << 20),
        name="forward_gather",
    )(lens, tok.reshape(rows, d), sq, so_, su, sd, vec)


HEADS = 12


EPSILON = 1e-12
MASKED = -1e30


def shifted(value, axis, steps):
    count = lax.axis_size(axis)
    pairs = [(source, (source + steps) % count) for source in range(count)]
    return lax.ppermute(value, axis, pairs)


def normalize(values, norm_gain, norm_shift):
    row_mean = jnp.mean(values, -1, keepdims=True)
    centred = values - row_mean
    spread = jnp.mean(centred * centred, -1, keepdims=True)
    return centred * lax.rsqrt(spread + EPSILON) * norm_gain + norm_shift


def gelu_exact(values):
    return jax.nn.gelu(values, approximate=False)


def row_dot(left_op, right_op):
    return jnp.dot(left_op, right_op, preferred_element_type=jnp.float32)


def left_dot(left_op, right_op):
    return lax.dot_general(
        left_op, right_op, (((0,), (0,)), ((), ())), preferred_element_type=jnp.float32
    )


def right_dot(left_op, right_op):
    return lax.dot_general(
        left_op, right_op, (((1,), (1,)), ((), ())), preferred_element_type=jnp.float32
    )


def general_body(
    tokens,
    cotangent,
    lengths,
    w_qkv,
    bias_q,
    bias_v,
    w_out,
    bias_out,
    gain_one,
    shift_one,
    w_up,
    bias_up,
    w_down,
    bias_down,
    gain_two,
    shift_two,
):
    seq_count, block_rows, model_width = tokens.shape
    head_count = HEADS
    head_dim = model_width // head_count
    all_rows = seq_count * block_rows
    score_scale = head_dim ** (-0.5)
    cycle_size = lax.axis_size("ctx")
    cycle_index = lax.axis_index("ctx")
    gathered = (
        lax.all_gather(w_qkv, "fsdp", axis=0, tiled=True),
        lax.all_gather(bias_q, "fsdp", axis=0, tiled=True),
        lax.all_gather(bias_v, "fsdp", axis=0, tiled=True),
        lax.all_gather(w_out, "fsdp", axis=0, tiled=True),
        lax.all_gather(bias_out, "fsdp", axis=0, tiled=True),
        lax.all_gather(gain_one, "fsdp", axis=0, tiled=True),
        lax.all_gather(shift_one, "fsdp", axis=0, tiled=True),
        lax.all_gather(w_up, "fsdp", axis=0, tiled=True),
        lax.all_gather(bias_up, "fsdp", axis=0, tiled=True),
        lax.all_gather(w_down, "fsdp", axis=0, tiled=True),
        lax.all_gather(bias_down, "fsdp", axis=0, tiled=True),
        lax.all_gather(gain_two, "fsdp", axis=0, tiled=True),
        lax.all_gather(shift_two, "fsdp", axis=0, tiled=True),
    )
    full_qkv, full_out, full_up, full_down = (gathered[0], gathered[3], gathered[7], gathered[9])
    add_q, add_v, add_out, scale_one, move_one, add_up, add_down, scale_two, move_two = [
        gathered[place].astype(jnp.float32) for place in (1, 2, 4, 5, 6, 8, 10, 11, 12)
    ]
    flat_tokens = tokens.reshape(all_rows, model_width)
    projected = row_dot(flat_tokens, full_qkv)
    queries = (
        (projected[:, :model_width] + add_q)
        .astype(jnp.bfloat16)
        .reshape(seq_count, block_rows, head_count, head_dim)
    )
    key_rows = (
        projected[:, model_width : 2 * model_width]
        .astype(jnp.bfloat16)
        .reshape(seq_count, block_rows, model_width)
    )
    value_rows = (
        (projected[:, 2 * model_width :] + add_v)
        .astype(jnp.bfloat16)
        .reshape(seq_count, block_rows, model_width)
    )
    start_state = (
        jnp.full((seq_count, block_rows, head_count), MASKED, jnp.float32),
        jnp.zeros((seq_count, block_rows, head_count), jnp.float32),
        jnp.zeros((seq_count, block_rows, head_count, head_dim), jnp.float32),
    )
    key_part = lax.all_gather(key_rows, "ctx", axis=1, tiled=True)
    value_part = lax.all_gather(value_rows, "ctx", axis=1, tiled=True)
    key_count = key_part.shape[1]
    sub_rows = math.gcd(key_count, 512)

    def visit(block_index, carried):
        first_key = block_index * sub_rows
        key_block = lax.dynamic_slice_in_dim(key_part, block_index * sub_rows, sub_rows, 1).reshape(
            seq_count, sub_rows, head_count, head_dim
        )
        value_block = lax.dynamic_slice_in_dim(
            value_part, block_index * sub_rows, sub_rows, 1
        ).reshape(seq_count, sub_rows, head_count, head_dim)
        peak, weight_sum, weighted = carried
        key_live = (
            (first_key + jnp.arange(sub_rows, dtype=jnp.int32))[None, :] < lengths[:, None]
        )[:, None, None, :]
        scores = (
            jnp.einsum("sqhe,skhe->sqhk", queries, key_block, preferred_element_type=jnp.float32)
            * score_scale
        )
        scores = jnp.where(key_live, scores, MASKED)
        new_peak = jnp.maximum(peak, jnp.max(scores, -1))
        factor = jnp.exp(peak - new_peak)
        weights = jnp.where(key_live, jnp.exp(scores - new_peak[..., None]), 0.0)
        mixed_values = jnp.einsum(
            "sqhk,skhe->sqhe",
            weights.astype(jnp.bfloat16),
            value_block,
            preferred_element_type=jnp.float32,
        )
        return (
            new_peak,
            weight_sum * factor + jnp.sum(weights, -1),
            weighted * factor[..., None] + mixed_values,
        )

    peak, weight_sum, weighted = lax.fori_loop(0, key_count // sub_rows, visit, start_state)
    log_total = peak + jnp.log(weight_sum)
    attended = weighted / weight_sum[..., None]
    attended_low = attended.astype(jnp.bfloat16).reshape(all_rows, model_width)
    first_sum = flat_tokens.astype(jnp.float32) + row_dot(attended_low, full_out) + add_out
    normed, norm_pull = jax.vjp(normalize, first_sum, scale_one, move_one)
    normed_low = normed.astype(jnp.bfloat16)
    hidden_pre = row_dot(normed_low, full_up) + add_up
    hidden_act, gelu_pull = jax.vjp(gelu_exact, hidden_pre)
    hidden_low = hidden_act.astype(jnp.bfloat16)
    second_sum = normed + row_dot(hidden_low, full_down) + add_down
    result, result_pull = jax.vjp(normalize, second_sum, scale_two, move_two)
    grad_second, grad_gain_two, grad_shift_two = result_pull(
        cotangent.reshape(all_rows, model_width).astype(jnp.float32)
    )
    down_low = grad_second.astype(jnp.bfloat16)
    grad_w_down = left_dot(hidden_low, down_low)
    grad_bias_down = jnp.sum(down_low.astype(jnp.float32), 0)
    (grad_pre,) = gelu_pull(right_dot(down_low, full_down))
    up_low = grad_pre.astype(jnp.bfloat16)
    grad_w_up = left_dot(normed_low, up_low)
    grad_bias_up = jnp.sum(up_low.astype(jnp.float32), 0)
    grad_first, grad_gain_one, grad_shift_one = norm_pull(grad_second + right_dot(up_low, full_up))
    branch_low = grad_first.astype(jnp.bfloat16)
    grad_w_out = left_dot(attended_low, branch_low)
    grad_bias_out = jnp.sum(branch_low.astype(jnp.float32), 0)
    grad_att = (
        right_dot(branch_low, full_out)
        .astype(jnp.bfloat16)
        .reshape(seq_count, block_rows, head_count, head_dim)
    )
    delta_rows = jnp.sum(grad_att.astype(jnp.float32) * attended, -1)

    def block_grads(query_part, grad_part, lse_part, delta_part, key_block, value_block, first_key):
        key_count = key_block.shape[1]
        key_heads = key_block.reshape(seq_count, key_count, head_count, head_dim)
        value_heads = value_block.reshape(seq_count, key_count, head_count, head_dim)
        key_live = (
            (first_key + jnp.arange(key_count, dtype=jnp.int32))[None, :] < lengths[:, None]
        )[:, None, None, :]
        scores = (
            jnp.einsum("sqhe,skhe->sqhk", query_part, key_heads, preferred_element_type=jnp.float32)
            * score_scale
        )
        chances = jnp.where(key_live, jnp.exp(scores - lse_part[..., None]), 0.0)
        grad_value = jnp.einsum(
            "sqhk,sqhe->skhe",
            chances.astype(jnp.bfloat16),
            grad_part,
            preferred_element_type=jnp.float32,
        )
        grad_chance = jnp.einsum(
            "sqhe,skhe->sqhk", grad_part, value_heads, preferred_element_type=jnp.float32
        )
        grad_score = (chances * (grad_chance - delta_part[..., None])).astype(jnp.bfloat16)
        grad_query = (
            jnp.einsum("sqhk,skhe->sqhe", grad_score, key_heads, preferred_element_type=jnp.float32)
            * score_scale
        )
        grad_key = (
            jnp.einsum(
                "sqhk,sqhe->skhe", grad_score, query_part, preferred_element_type=jnp.float32
            )
            * score_scale
        )
        return (
            grad_query,
            grad_key.reshape(seq_count, key_count, model_width),
            grad_value.reshape(seq_count, key_count, model_width),
        )

    query_start = jnp.zeros((seq_count, block_rows, head_count, head_dim), jnp.float32)

    def key_terms(key_block, value_block, first_key):
        return block_grads(
            queries, grad_att, log_total, delta_rows, key_block, value_block, first_key
        )

    def block_terms(key_block, value_block, first_key):
        return key_terms(key_block, value_block, first_key)

    def turn(step_index, carried):
        key_now, value_now, key_grads, query_acc = carried
        first_key = (cycle_index - step_index) % cycle_size * block_rows
        add_query, add_key, add_value = block_terms(key_now, value_now, first_key)
        key_now, value_now = shifted((key_now, value_now), "ctx", 1)
        key_grads = (
            shifted((key_grads[0] + add_key).astype(jnp.bfloat16), "ctx", 1).astype(jnp.float32),
            shifted((key_grads[1] + add_value).astype(jnp.bfloat16), "ctx", 1).astype(jnp.float32),
        )
        return (key_now, value_now, key_grads, query_acc + add_query)

    grad_start = (
        jnp.zeros((seq_count, block_rows, model_width), jnp.float32),
        jnp.zeros((seq_count, block_rows, model_width), jnp.float32),
    )
    key_final, value_final, key_grads, query_grad = lax.fori_loop(
        0, cycle_size, turn, (key_rows, value_rows, grad_start, query_start)
    )
    grad_key, grad_value = key_grads
    qkv_grad = jnp.concatenate(
        [
            query_grad.astype(jnp.bfloat16).reshape(all_rows, model_width),
            grad_key.astype(jnp.bfloat16).reshape(all_rows, model_width),
            grad_value.astype(jnp.bfloat16).reshape(all_rows, model_width),
        ],
        1,
    )
    grad_w_qkv = left_dot(flat_tokens, qkv_grad)
    grad_bias_q = jnp.sum(qkv_grad[:, :model_width].astype(jnp.float32), 0)
    grad_bias_v = jnp.sum(qkv_grad[:, 2 * model_width :].astype(jnp.float32), 0)
    grad_input = grad_first + right_dot(qkv_grad, full_qkv)
    vectors = (
        grad_bias_q,
        grad_bias_v,
        grad_bias_out,
        grad_gain_one,
        grad_shift_one,
        grad_bias_up,
        grad_bias_down,
        grad_gain_two,
        grad_shift_two,
    )
    packed = jnp.concatenate(vectors).reshape(VR, U)
    t_down, t_up, t_out, t_qkv, t_vec = grad_reduce(
        grad_w_down.astype(BF16),
        grad_w_up.astype(BF16),
        grad_w_out.astype(BF16),
        grad_w_qkv.astype(BF16),
        packed,
        cycle_size // 2,
        lax.axis_size("dp"),
        1,
    )
    flat = t_vec.reshape(-1)
    own = lax.axis_index("fsdp")
    parts, start = [], 0
    for vector in vectors:
        half = vector.shape[0] // 2
        parts.append(lax.dynamic_slice_in_dim(flat, start + own * half, half, 0))
        start += 2 * half
    totals = (
        t_qkv, parts[0], parts[1], t_out, parts[2], parts[3], parts[4],
        t_up, parts[5], t_down, parts[6], parts[7], parts[8],
    )
    output_rows = result.astype(jnp.bfloat16).reshape(seq_count, block_rows, model_width)
    input_rows = grad_input.astype(jnp.bfloat16).reshape(seq_count, block_rows, model_width)
    return (
        output_rows,
        input_rows,
        totals[0],
        totals[1],
        totals[2],
        totals[3],
        totals[4],
        totals[5],
        totals[6],
        totals[7],
        totals[8],
        totals[9],
        totals[10],
        totals[11],
        totals[12],
    )


def fast_body(
    tokens,
    cotangent,
    lengths,
    w_qkv,
    bias_q,
    bias_v,
    w_out,
    bias_out,
    gain_one,
    shift_one,
    w_up,
    bias_up,
    w_down,
    bias_down,
    gain_two,
    shift_two,
):
    seq_count, block_rows, model_width = tokens.shape
    head_count = HEADS
    head_dim = model_width // head_count
    all_rows = seq_count * block_rows
    score_scale = head_dim ** (-0.5)
    cycle_size = lax.axis_size("ctx")
    cycle_index = lax.axis_index("ctx")
    packed_in = jnp.concatenate(
        [bias_q, bias_v, bias_out, gain_one, shift_one, bias_up, bias_down, gain_two, shift_two]
    ).astype(jnp.float32).reshape(VR // 2, U)
    flat_tokens = tokens.reshape(all_rows, model_width)
    qkv_all, attended, lse_pad, full_qkv, full_out, full_up, full_down, vec_all = forward_gather(
        lengths, tokens, w_qkv, w_out, w_up, w_down, packed_in, cycle_size // 2, 2
    )

    def vector(first, count):
        return vec_all[:, first : first + count].reshape(-1)

    add_out, scale_one, move_one = vector(2, 1), vector(3, 1), vector(4, 1)
    add_up, add_down, scale_two, move_two = vector(5, 4), vector(9, 1), vector(10, 1), vector(11, 1)
    mine = lax.dynamic_index_in_dim(qkv_all, cycle_index, 1, False)
    shape4 = (seq_count, block_rows, head_count, head_dim)
    queries = (mine[0] * jnp.asarray(8.0, jnp.bfloat16)).reshape(shape4)
    key_rows = mine[1].reshape(seq_count, block_rows, model_width)
    value_rows = mine[2].reshape(seq_count, block_rows, model_width)
    attended = attended.reshape(shape4)
    log_total = lse_pad[:, :head_count].reshape(seq_count, block_rows, head_count)
    attended_low = attended.astype(jnp.bfloat16).reshape(all_rows, model_width)
    first_sum = flat_tokens.astype(jnp.float32) + row_dot(attended_low, full_out) + add_out
    normed, norm_pull = jax.vjp(normalize, first_sum, scale_one, move_one)
    normed_low = normed.astype(jnp.bfloat16)
    hidden_pre = row_dot(normed_low, full_up) + add_up
    hidden_act, gelu_pull = jax.vjp(gelu_exact, hidden_pre)
    hidden_low = hidden_act.astype(jnp.bfloat16)
    second_sum = normed + row_dot(hidden_low, full_down) + add_down
    result, result_pull = jax.vjp(normalize, second_sum, scale_two, move_two)
    grad_second, grad_gain_two, grad_shift_two = result_pull(
        cotangent.reshape(all_rows, model_width).astype(jnp.float32)
    )
    down_low = grad_second.astype(jnp.bfloat16)
    grad_w_down = left_dot(hidden_low, down_low)
    grad_bias_down = jnp.sum(down_low.astype(jnp.float32), 0)
    (grad_pre,) = gelu_pull(right_dot(down_low, full_down))
    up_low = grad_pre.astype(jnp.bfloat16)
    grad_w_up = left_dot(normed_low, up_low)
    grad_bias_up = jnp.sum(up_low.astype(jnp.float32), 0)
    grad_first, grad_gain_one, grad_shift_one = norm_pull(grad_second + right_dot(up_low, full_up))
    branch_low = grad_first.astype(jnp.bfloat16)
    grad_w_out = left_dot(attended_low, branch_low)
    grad_bias_out = jnp.sum(branch_low.astype(jnp.float32), 0)
    grad_att = (
        right_dot(branch_low, full_out)
        .astype(jnp.bfloat16)
        .reshape(seq_count, block_rows, head_count, head_dim)
    )
    delta_rows = jnp.sum(grad_att.astype(jnp.float32) * attended, -1)

    def block_grads(query_part, grad_part, lse_part, delta_part, key_block, value_block, first_key):
        key_count = key_block.shape[1]
        key_heads = key_block.reshape(seq_count, key_count, head_count, head_dim)
        value_heads = value_block.reshape(seq_count, key_count, head_count, head_dim)
        key_live = (
            (first_key + jnp.arange(key_count, dtype=jnp.int32))[None, :] < lengths[:, None]
        )[:, None, None, :]
        scores = (
            jnp.einsum("sqhe,skhe->sqhk", query_part, key_heads, preferred_element_type=jnp.float32)
            * score_scale
        )
        chances = jnp.where(key_live, jnp.exp(scores - lse_part[..., None]), 0.0)
        grad_value = jnp.einsum(
            "sqhk,sqhe->skhe",
            chances.astype(jnp.bfloat16),
            grad_part,
            preferred_element_type=jnp.float32,
        )
        grad_chance = jnp.einsum(
            "sqhe,skhe->sqhk", grad_part, value_heads, preferred_element_type=jnp.float32
        )
        grad_score = (chances * (grad_chance - delta_part[..., None])).astype(jnp.bfloat16)
        grad_query = (
            jnp.einsum("sqhk,skhe->sqhe", grad_score, key_heads, preferred_element_type=jnp.float32)
            * score_scale
        )
        grad_key = (
            jnp.einsum(
                "sqhk,sqhe->skhe", grad_score, query_part, preferred_element_type=jnp.float32
            )
            * score_scale
        )
        return (
            grad_query,
            grad_key.reshape(seq_count, key_count, model_width),
            grad_value.reshape(seq_count, key_count, model_width),
        )

    query_start = jnp.zeros((seq_count, block_rows, head_count, head_dim), jnp.float32)

    def key_terms(key_block, value_block, first_key):
        return block_grads(
            queries, grad_att, log_total, delta_rows, key_block, value_block, first_key
        )

    def block_terms(key_block, value_block, first_key):
        return key_terms(key_block, value_block, first_key)

    def turn(step_index, carried):
        key_now, value_now, key_grads, query_acc = carried
        first_key = (cycle_index - step_index) % cycle_size * block_rows
        add_query, add_key, add_value = block_terms(key_now, value_now, first_key)
        key_now, value_now = shifted((key_now, value_now), "ctx", 1)
        key_grads = (
            shifted((key_grads[0] + add_key).astype(jnp.bfloat16), "ctx", 1).astype(jnp.float32),
            shifted((key_grads[1] + add_value).astype(jnp.bfloat16), "ctx", 1).astype(jnp.float32),
        )
        return (key_now, value_now, key_grads, query_acc + add_query)

    grad_start = (
        jnp.zeros((seq_count, block_rows, model_width), jnp.float32),
        jnp.zeros((seq_count, block_rows, model_width), jnp.float32),
    )
    key_final, value_final, key_grads, query_grad = lax.fori_loop(
        0, cycle_size, turn, (key_rows, value_rows, grad_start, query_start)
    )
    grad_key, grad_value = key_grads
    qkv_grad = jnp.concatenate(
        [
            query_grad.astype(jnp.bfloat16).reshape(all_rows, model_width),
            grad_key.astype(jnp.bfloat16).reshape(all_rows, model_width),
            grad_value.astype(jnp.bfloat16).reshape(all_rows, model_width),
        ],
        1,
    )
    grad_w_qkv = left_dot(flat_tokens, qkv_grad)
    grad_bias_q = jnp.sum(qkv_grad[:, :model_width].astype(jnp.float32), 0)
    grad_bias_v = jnp.sum(qkv_grad[:, 2 * model_width :].astype(jnp.float32), 0)
    grad_input = grad_first + right_dot(qkv_grad, full_qkv)
    vectors = (
        grad_bias_q,
        grad_bias_v,
        grad_bias_out,
        grad_gain_one,
        grad_shift_one,
        grad_bias_up,
        grad_bias_down,
        grad_gain_two,
        grad_shift_two,
    )
    packed = jnp.concatenate(vectors).reshape(VR, U)
    t_down, t_up, t_out, t_qkv, t_vec = grad_reduce(
        grad_w_down.astype(BF16),
        grad_w_up.astype(BF16),
        grad_w_out.astype(BF16),
        grad_w_qkv.astype(BF16),
        packed,
        cycle_size // 2,
        lax.axis_size("dp"),
        1,
    )
    flat = t_vec.reshape(-1)
    own = lax.axis_index("fsdp")
    parts, start = [], 0
    for vector in vectors:
        half = vector.shape[0] // 2
        parts.append(lax.dynamic_slice_in_dim(flat, start + own * half, half, 0))
        start += 2 * half
    totals = (
        t_qkv, parts[0], parts[1], t_out, parts[2], parts[3], parts[4],
        t_up, parts[5], t_down, parts[6], parts[7], parts[8],
    )
    output_rows = result.astype(jnp.bfloat16).reshape(seq_count, block_rows, model_width)
    input_rows = grad_input.astype(jnp.bfloat16).reshape(seq_count, block_rows, model_width)
    return (
        output_rows,
        input_rows,
        totals[0],
        totals[1],
        totals[2],
        totals[3],
        totals[4],
        totals[5],
        totals[6],
        totals[7],
        totals[8],
        totals[9],
        totals[10],
        totals[11],
        totals[12],
    )


def solution(mesh):
    return jax.shard_map(
        fast_body if mesh.shape["ctx"] <= 4 else general_body,
        mesh=mesh,
        in_specs=(
            P(("dp", "fsdp"), "ctx", None),
            P(("dp", "fsdp"), "ctx", None),
            P(("dp", "fsdp")),
            P("fsdp", None),
            P("fsdp"),
            P("fsdp"),
            P("fsdp", None),
            P("fsdp"),
            P("fsdp"),
            P("fsdp"),
            P("fsdp", None),
            P("fsdp"),
            P("fsdp", None),
            P("fsdp"),
            P("fsdp"),
            P("fsdp"),
        ),
        out_specs=(
            P(("dp", "fsdp"), "ctx", None),
            P(("dp", "fsdp"), "ctx", None),
            P("fsdp", None),
            P("fsdp"),
            P("fsdp"),
            P("fsdp", None),
            P("fsdp"),
            P("fsdp"),
            P("fsdp"),
            P("fsdp", None),
            P("fsdp"),
            P("fsdp", None),
            P("fsdp"),
            P("fsdp"),
            P("fsdp"),
        ),
        check_vma=False,
    )
```

```python
import functools
import math

import jax
import jax.numpy as jnp
from jax import lax
from jax.experimental import pallas as pl
from jax.experimental.pallas import tpu as pltpu
from jax.sharding import PartitionSpec as P

MESH = pl.DeviceIdType.MESH
F32, BF16 = jnp.float32, jnp.bfloat16
U = 384
VR = 24


def places():
    c = lax.axis_index("ctx")
    return lax.rem(c, 2), c // 2, lax.axis_index("fsdp"), lax.axis_index("dp")


def grad_kernel(nx, nd, grp, wd, wu, wo, wq, vec, od, ou, oo, oq, ov,
                L, R1, R2, R3, R4, AX, AC, ST, V0, VX, VZ,
                s0, s1s, s1r, s2s, s2r, s3s, s3r, s4s, s4r, s5s, s5r, s6s, s6r, s7s, s7r, so, vs, vr):
    core, x, f, z = places()
    nch = 12 // grp
    CH, CX, PZ = U * grp, U * grp // nx, U * grp // nx // nd
    sib = {"ctx": x * 2 + 1 - core}
    yp = {"fsdp": 1 - f}
    xps = [{"ctx": lax.rem(x + j, nx) * 2 + core} for j in range(1, nx)]
    zps = [{"dp": lax.rem(z + j, nd)} for j in range(1, nd)]
    peers = [sib, yp] + xps + zps
    bar = pltpu.get_barrier_semaphore()
    for p in peers:
        pl.semaphore_signal(bar, inc=1, device_id=p, device_id_type=MESH)

    def rect(i, ff, cc):
        if i < 4:
            return wd, ff * 1536 + i * U, cc * U
        if i < 8:
            return wu, ff * U, cc * 1536 + (i - 4) * U
        if i < 9:
            return wo, ff * U, cc * U
        return wq, ff * U, cc * 1152 + (i - 9) * U

    def orect(i, cc):
        if i < 4:
            return od, i * U, cc * U
        if i < 8:
            return ou, 0, cc * 1536 + (i - 4) * U
        if i < 9:
            return oo, 0, cc * U
        return oq, 0, cc * 1152 + (i - 9) * U

    def sl(ref, r, c):
        return ref.at[pl.ds(pl.multiple_of(r, U), U), pl.ds(pl.multiple_of(c, 128), U)]

    def local(i, k):
        ff = (1 - f) if k == 0 else f
        return pltpu.make_async_copy(sl(*rect(i, ff, core)), L.at[i // grp, ff, pl.ds(i % grp * U, U)], s0.at[i, k])

    def remote(src, dst, ss, rs, dev):
        return pltpu.make_async_remote_copy(src_ref=src, dst_ref=dst, send_sem=ss, recv_sem=rs, device_id=dev, device_id_type=MESH)

    def c1(i, k):
        ff = (1 - f) if k == 0 else f
        return remote(sl(*rect(i, ff, 1 - core)), R1.at[i // grp, ff, pl.ds(i % grp * U, U)], s1s.at[i, k], s1r.at[i, k], sib)

    def c2(c):
        return remote(L.at[c, 1 - f], R2.at[c], s2s.at[c], s2r.at[c], yp)

    def c3(c, j):
        xt = lax.rem(x + j, nx)
        return remote(L.at[c, f, pl.ds(pl.multiple_of(xt * CX, CX), CX)], R3.at[c, j - 1], s3s.at[c, j - 1], s3r.at[c, j - 1], xps[j - 1])

    def mine(c, zz):
        return pl.ds(pl.multiple_of(x * CX + zz * PZ, PZ), PZ)

    def c4(c, j):
        zt = lax.rem(z + j, nd)
        return remote(L.at[c, f, mine(c, zt)], R4.at[c, j - 1], s4s.at[c, j - 1], s4r.at[c, j - 1], zps[j - 1])

    def c5(c, j):
        return remote(AX.at[c, mine(c, z)], AX.at[c, mine(c, z)], s5s.at[c, j - 1], s5r.at[c, j - 1], zps[j - 1])

    def c6(c, j):
        rows = pl.ds(pl.multiple_of(x * CX, CX), CX)
        return remote(AX.at[c, rows], AX.at[c, rows], s6s.at[c, j - 1], s6r.at[c, j - 1], xps[j - 1])

    def c7(c):
        return remote(AX.at[c], AC.at[c], s7s.at[c], s7r.at[c], sib)

    B = 48

    def rows_loop(n, fn):
        def bodyf(i, _):
            fn(pl.multiple_of(i * B, B))
            return 0
        lax.fori_loop(0, n // B, bodyf, 0)

    def up(v):
        return v.astype(F32)

    def st2(c):
        for k in range(grp):
            local(c * grp + k, 0).wait()
            c1(c * grp + k, 0).wait_recv()

        def fn(r):
            s = pl.ds(r, B)
            L[c, 1 - f, s, :] = (up(L[c, 1 - f, s, :]) + up(R1[c, 1 - f, s, :])).astype(BF16)
        rows_loop(CH, fn)
        c2(c).start()

    def st3(c):
        for k in range(grp):
            local(c * grp + k, 1).wait()
            c1(c * grp + k, 1).wait_recv()
        c2(c).wait_recv()
        for j in range(1, nx):
            xt = lax.rem(x + j, nx)

            def fn(r):
                s = pl.ds(pl.multiple_of(xt * CX + r, B), B)
                L[c, f, s, :] = (up(L[c, f, s, :]) + up(R1[c, f, s, :]) + up(R2[c, s, :])).astype(BF16)
            rows_loop(CX, fn)
            c3(c, j).start()

    def st4(c):
        for j in range(1, nx):
            c3(c, j).wait_recv()

        def fn(r):
            s = pl.ds(pl.multiple_of(x * CX + r, B), B)
            t = up(L[c, f, s, :]) + up(R1[c, f, s, :]) + up(R2[c, s, :])
            for j in range(1, nx):
                t = t + up(R3[c, j - 1, pl.ds(r, B), :])
            L[c, f, s, :] = t.astype(BF16)
        rows_loop(CX, fn)
        for j in range(1, nd):
            c4(c, j).start()

    def st5(c):
        for j in range(1, nd):
            c4(c, j).wait_recv()
        t = up(L[c, f, mine(c, z), :])
        for j in range(1, nd):
            t = t + up(R4[c, j - 1])
        AX[c, mine(c, z), :] = t.astype(BF16)
        for j in range(1, nd):
            c5(c, j).start()

    def st6(c):
        for j in range(1, nd):
            c5(c, j).wait_recv()
        for j in range(1, nx):
            c6(c, j).start()

    def outc(i, k, slot):
        cc = core if k == 0 else 1 - core
        return pltpu.make_async_copy(ST.at[slot], sl(*orect(i, cc)), so.at[slot])

    def emit(i, k, src):
        slot = emit.n % 4
        if emit.n >= 4:
            outc(*emit.log[emit.n - 4], slot).wait()
        off = i % grp * U

        def fn(r):
            ST[slot, pl.ds(r, B), :] = up(src[i // grp, pl.ds(pl.multiple_of(off + r, B), B), :])
        rows_loop(U, fn)
        outc(i, k, slot).start()
        emit.log.append((i, k))
        emit.n += 1
    emit.n = 0
    emit.log = []

    def st7(c):
        for j in range(1, nx):
            c6(c, j).wait_recv()
        c7(c).start()
        for k in range(grp):
            emit(c * grp + k, 0, AX)

    def st8(c):
        c7(c).wait_recv()
        for k in range(grp):
            emit(c * grp + k, 1, AC)

    def v_core():
        return remote(vec, V0.at[0], vs.at[0], vr.at[0], sib)

    def v_y():
        return remote(V0.at[1], V0.at[2], vs.at[1], vr.at[1], yp)

    def v_x(j):
        return remote(VX.at[x], VX.at[x], vs.at[1 + j], vr.at[1 + j], xps[j - 1])

    def v_z(j):
        return remote(VZ.at[z], VZ.at[z], vs.at[nx + j], vr.at[nx + j], zps[j - 1])

    def vst(k):
        if k == 0:
            v_core().start()
        elif k == 1:
            v_core().wait_recv()
            V0[1] = vec[...] + V0[0]
            v_y().start()
        elif k == 2:
            v_y().wait_recv()
            VX[x] = V0[1] + V0[2]
            for j in range(1, nx):
                v_x(j).start()
        elif k == 3:
            for j in range(1, nx):
                v_x(j).wait_recv()
            t = VX[0]
            for j in range(1, nx):
                t = t + VX[j]
            VZ[z] = t
            for j in range(1, nd):
                v_z(j).start()
        elif k == 4:
            for j in range(1, nd):
                v_z(j).wait_recv()
            t = VZ[0]
            for j in range(1, nd):
                t = t + VZ[j]
            ov[...] = t

    for i in range(12):
        local(i, 0).start()
    pl.semaphore_wait(bar, len(peers))
    for i in range(12):
        c1(i, 0).start()
    vst(0)
    for i in range(12):
        local(i, 1).start()
        c1(i, 1).start()
    stages = [(8, st8), (7, st7), (6, st6), (5, st5), (4, st4), (3, st3)]
    for t in range(nch + 8):
        if t < nch:
            st2(t)
        if 1 <= t <= 4:
            vst(t)
        for k, fn in stages:
            c = t - (k - 1)
            if 0 <= c < nch:
                fn(c)
    n = emit.n
    for q in range(max(0, n - 4), n):
        outc(*emit.log[q], q % 4).wait()
    for i in range(12):
        for k in range(2):
            c1(i, k).wait_send()
    for c in range(nch):
        c2(c).wait_send()
        c7(c).wait_send()
        for j in range(1, nx):
            c3(c, j).wait_send()
            c6(c, j).wait_send()
        for j in range(1, nd):
            c4(c, j).wait_send()
            c5(c, j).wait_send()
    v_core().wait_send()
    v_y().wait_send()
    for j in range(1, nx):
        v_x(j).wait_send()
    for j in range(1, nd):
        v_z(j).wait_send()


def grad_reduce(wd, wu, wo, wq, vec, nx, nd, cid):
    grp = nx * nd // 8
    nch = 12 // grp
    CH, CX, PZ = U * grp, U * grp // nx, U * grp // nx // nd
    anyspec = pl.BlockSpec(memory_space=pl.ANY)
    vspec = pl.BlockSpec(memory_space=pltpu.VMEM)
    D = pltpu.SemaphoreType.DMA
    V = pltpu.VMEM
    sems = [D((12, 2)), D((12, 2)), D((12, 2)), D((nch,)), D((nch,)), D((nch, nx - 1)), D((nch, nx - 1)),
            D((nch, nd - 1)), D((nch, nd - 1)), D((nch, nd - 1)), D((nch, nd - 1)), D((nch, nx - 1)), D((nch, nx - 1)),
            D((nch,)), D((nch,)), D((4,)), D((nx + nd,)), D((nx + nd,))]
    return pl.pallas_call(
        functools.partial(grad_kernel, nx, nd, grp),
        out_shape=(jax.ShapeDtypeStruct((1536, 768), F32), jax.ShapeDtypeStruct((U, 3072), F32),
                   jax.ShapeDtypeStruct((U, 768), F32), jax.ShapeDtypeStruct((U, 2304), F32),
                   jax.ShapeDtypeStruct((VR, U), F32)),
        in_specs=[anyspec] * 4 + [vspec],
        out_specs=(anyspec,) * 4 + (vspec,),
        scratch_shapes=[V((nch, 2, CH, U), BF16), V((nch, 2, CH, U), BF16), V((nch, CH, U), BF16),
                        V((nch, nx - 1, CX, U), BF16), V((nch, nd - 1, PZ, U), BF16),
                        V((nch, CH, U), BF16), V((nch, CH, U), BF16), V((4, U, U), F32),
                        V((3, VR, U), F32), V((nx, VR, U), F32), V((nd, VR, U), F32)] + sems,
        compiler_params=pltpu.CompilerParams(collective_id=cid, has_side_effects=True, vmem_limit_bytes=60 << 20),
        name="grad_reduce",
    )(wd, wu, wo, wq, vec)


HEADS = 12


EPSILON = 1e-12
MASKED = -1e30


def shifted(value, axis, steps):
    count = lax.axis_size(axis)
    pairs = [(source, (source + steps) % count) for source in range(count)]
    return lax.ppermute(value, axis, pairs)


def normalize(values, norm_gain, norm_shift):
    row_mean = jnp.mean(values, -1, keepdims=True)
    centred = values - row_mean
    spread = jnp.mean(centred * centred, -1, keepdims=True)
    return centred * lax.rsqrt(spread + EPSILON) * norm_gain + norm_shift


def gelu_exact(values):
    return jax.nn.gelu(values, approximate=False)


def row_dot(left_op, right_op):
    return jnp.dot(left_op, right_op, preferred_element_type=jnp.float32)


def left_dot(left_op, right_op):
    return lax.dot_general(
        left_op, right_op, (((0,), (0,)), ((), ())), preferred_element_type=jnp.float32
    )


def right_dot(left_op, right_op):
    return lax.dot_general(
        left_op, right_op, (((1,), (1,)), ((), ())), preferred_element_type=jnp.float32
    )


def general_body(
    tokens,
    cotangent,
    lengths,
    w_qkv,
    bias_q,
    bias_v,
    w_out,
    bias_out,
    gain_one,
    shift_one,
    w_up,
    bias_up,
    w_down,
    bias_down,
    gain_two,
    shift_two,
):
    seq_count, block_rows, model_width = tokens.shape
    head_count = HEADS
    head_dim = model_width // head_count
    all_rows = seq_count * block_rows
    score_scale = head_dim ** (-0.5)
    cycle_size = lax.axis_size("ctx")
    cycle_index = lax.axis_index("ctx")
    gathered = (
        lax.all_gather(w_qkv, "fsdp", axis=0, tiled=True),
        lax.all_gather(bias_q, "fsdp", axis=0, tiled=True),
        lax.all_gather(bias_v, "fsdp", axis=0, tiled=True),
        lax.all_gather(w_out, "fsdp", axis=0, tiled=True),
        lax.all_gather(bias_out, "fsdp", axis=0, tiled=True),
        lax.all_gather(gain_one, "fsdp", axis=0, tiled=True),
        lax.all_gather(shift_one, "fsdp", axis=0, tiled=True),
        lax.all_gather(w_up, "fsdp", axis=0, tiled=True),
        lax.all_gather(bias_up, "fsdp", axis=0, tiled=True),
        lax.all_gather(w_down, "fsdp", axis=0, tiled=True),
        lax.all_gather(bias_down, "fsdp", axis=0, tiled=True),
        lax.all_gather(gain_two, "fsdp", axis=0, tiled=True),
        lax.all_gather(shift_two, "fsdp", axis=0, tiled=True),
    )
    full_qkv, full_out, full_up, full_down = (gathered[0], gathered[3], gathered[7], gathered[9])
    add_q, add_v, add_out, scale_one, move_one, add_up, add_down, scale_two, move_two = [
        gathered[place].astype(jnp.float32) for place in (1, 2, 4, 5, 6, 8, 10, 11, 12)
    ]
    flat_tokens = tokens.reshape(all_rows, model_width)
    projected = row_dot(flat_tokens, full_qkv)
    queries = (
        (projected[:, :model_width] + add_q)
        .astype(jnp.bfloat16)
        .reshape(seq_count, block_rows, head_count, head_dim)
    )
    key_rows = (
        projected[:, model_width : 2 * model_width]
        .astype(jnp.bfloat16)
        .reshape(seq_count, block_rows, model_width)
    )
    value_rows = (
        (projected[:, 2 * model_width :] + add_v)
        .astype(jnp.bfloat16)
        .reshape(seq_count, block_rows, model_width)
    )
    start_state = (
        jnp.full((seq_count, block_rows, head_count), MASKED, jnp.float32),
        jnp.zeros((seq_count, block_rows, head_count), jnp.float32),
        jnp.zeros((seq_count, block_rows, head_count, head_dim), jnp.float32),
    )
    key_part = lax.all_gather(key_rows, "ctx", axis=1, tiled=True)
    value_part = lax.all_gather(value_rows, "ctx", axis=1, tiled=True)
    key_count = key_part.shape[1]
    sub_rows = math.gcd(key_count, 512)

    def visit(block_index, carried):
        first_key = block_index * sub_rows
        key_block = lax.dynamic_slice_in_dim(key_part, block_index * sub_rows, sub_rows, 1).reshape(
            seq_count, sub_rows, head_count, head_dim
        )
        value_block = lax.dynamic_slice_in_dim(
            value_part, block_index * sub_rows, sub_rows, 1
        ).reshape(seq_count, sub_rows, head_count, head_dim)
        peak, weight_sum, weighted = carried
        key_live = (
            (first_key + jnp.arange(sub_rows, dtype=jnp.int32))[None, :] < lengths[:, None]
        )[:, None, None, :]
        scores = (
            jnp.einsum("sqhe,skhe->sqhk", queries, key_block, preferred_element_type=jnp.float32)
            * score_scale
        )
        scores = jnp.where(key_live, scores, MASKED)
        new_peak = jnp.maximum(peak, jnp.max(scores, -1))
        factor = jnp.exp(peak - new_peak)
        weights = jnp.where(key_live, jnp.exp(scores - new_peak[..., None]), 0.0)
        mixed_values = jnp.einsum(
            "sqhk,skhe->sqhe",
            weights.astype(jnp.bfloat16),
            value_block,
            preferred_element_type=jnp.float32,
        )
        return (
            new_peak,
            weight_sum * factor + jnp.sum(weights, -1),
            weighted * factor[..., None] + mixed_values,
        )

    peak, weight_sum, weighted = lax.fori_loop(0, key_count // sub_rows, visit, start_state)
    log_total = peak + jnp.log(weight_sum)
    attended = weighted / weight_sum[..., None]
    attended_low = attended.astype(jnp.bfloat16).reshape(all_rows, model_width)
    first_sum = flat_tokens.astype(jnp.float32) + row_dot(attended_low, full_out) + add_out
    normed, norm_pull = jax.vjp(normalize, first_sum, scale_one, move_one)
    normed_low = normed.astype(jnp.bfloat16)
    hidden_pre = row_dot(normed_low, full_up) + add_up
    hidden_act, gelu_pull = jax.vjp(gelu_exact, hidden_pre)
    hidden_low = hidden_act.astype(jnp.bfloat16)
    second_sum = normed + row_dot(hidden_low, full_down) + add_down
    result, result_pull = jax.vjp(normalize, second_sum, scale_two, move_two)
    grad_second, grad_gain_two, grad_shift_two = result_pull(
        cotangent.reshape(all_rows, model_width).astype(jnp.float32)
    )
    down_low = grad_second.astype(jnp.bfloat16)
    grad_w_down = left_dot(hidden_low, down_low)
    grad_bias_down = jnp.sum(down_low.astype(jnp.float32), 0)
    (grad_pre,) = gelu_pull(right_dot(down_low, full_down))
    up_low = grad_pre.astype(jnp.bfloat16)
    grad_w_up = left_dot(normed_low, up_low)
    grad_bias_up = jnp.sum(up_low.astype(jnp.float32), 0)
    grad_first, grad_gain_one, grad_shift_one = norm_pull(grad_second + right_dot(up_low, full_up))
    branch_low = grad_first.astype(jnp.bfloat16)
    grad_w_out = left_dot(attended_low, branch_low)
    grad_bias_out = jnp.sum(branch_low.astype(jnp.float32), 0)
    grad_att = (
        right_dot(branch_low, full_out)
        .astype(jnp.bfloat16)
        .reshape(seq_count, block_rows, head_count, head_dim)
    )
    delta_rows = jnp.sum(grad_att.astype(jnp.float32) * attended, -1)

    def block_grads(query_part, grad_part, lse_part, delta_part, key_block, value_block, first_key):
        key_count = key_block.shape[1]
        key_heads = key_block.reshape(seq_count, key_count, head_count, head_dim)
        value_heads = value_block.reshape(seq_count, key_count, head_count, head_dim)
        key_live = (
            (first_key + jnp.arange(key_count, dtype=jnp.int32))[None, :] < lengths[:, None]
        )[:, None, None, :]
        scores = (
            jnp.einsum("sqhe,skhe->sqhk", query_part, key_heads, preferred_element_type=jnp.float32)
            * score_scale
        )
        chances = jnp.where(key_live, jnp.exp(scores - lse_part[..., None]), 0.0)
        grad_value = jnp.einsum(
            "sqhk,sqhe->skhe",
            chances.astype(jnp.bfloat16),
            grad_part,
            preferred_element_type=jnp.float32,
        )
        grad_chance = jnp.einsum(
            "sqhe,skhe->sqhk", grad_part, value_heads, preferred_element_type=jnp.float32
        )
        grad_score = (chances * (grad_chance - delta_part[..., None])).astype(jnp.bfloat16)
        grad_query = (
            jnp.einsum("sqhk,skhe->sqhe", grad_score, key_heads, preferred_element_type=jnp.float32)
            * score_scale
        )
        grad_key = (
            jnp.einsum(
                "sqhk,sqhe->skhe", grad_score, query_part, preferred_element_type=jnp.float32
            )
            * score_scale
        )
        return (
            grad_query,
            grad_key.reshape(seq_count, key_count, model_width),
            grad_value.reshape(seq_count, key_count, model_width),
        )

    query_start = jnp.zeros((seq_count, block_rows, head_count, head_dim), jnp.float32)

    def key_terms(key_block, value_block, first_key):
        return block_grads(
            queries, grad_att, log_total, delta_rows, key_block, value_block, first_key
        )

    def block_terms(key_block, value_block, first_key):
        return key_terms(key_block, value_block, first_key)

    def turn(step_index, carried):
        key_now, value_now, key_grads, query_acc = carried
        first_key = (cycle_index - step_index) % cycle_size * block_rows
        add_query, add_key, add_value = block_terms(key_now, value_now, first_key)
        key_now, value_now = shifted((key_now, value_now), "ctx", 1)
        key_grads = (
            shifted((key_grads[0] + add_key).astype(jnp.bfloat16), "ctx", 1).astype(jnp.float32),
            shifted((key_grads[1] + add_value).astype(jnp.bfloat16), "ctx", 1).astype(jnp.float32),
        )
        return (key_now, value_now, key_grads, query_acc + add_query)

    grad_start = (
        jnp.zeros((seq_count, block_rows, model_width), jnp.float32),
        jnp.zeros((seq_count, block_rows, model_width), jnp.float32),
    )
    key_final, value_final, key_grads, query_grad = lax.fori_loop(
        0, cycle_size, turn, (key_rows, value_rows, grad_start, query_start)
    )
    grad_key, grad_value = key_grads
    qkv_grad = jnp.concatenate(
        [
            query_grad.astype(jnp.bfloat16).reshape(all_rows, model_width),
            grad_key.astype(jnp.bfloat16).reshape(all_rows, model_width),
            grad_value.astype(jnp.bfloat16).reshape(all_rows, model_width),
        ],
        1,
    )
    grad_w_qkv = left_dot(flat_tokens, qkv_grad)
    grad_bias_q = jnp.sum(qkv_grad[:, :model_width].astype(jnp.float32), 0)
    grad_bias_v = jnp.sum(qkv_grad[:, 2 * model_width :].astype(jnp.float32), 0)
    grad_input = grad_first + right_dot(qkv_grad, full_qkv)
    vectors = (
        grad_bias_q,
        grad_bias_v,
        grad_bias_out,
        grad_gain_one,
        grad_shift_one,
        grad_bias_up,
        grad_bias_down,
        grad_gain_two,
        grad_shift_two,
    )
    packed = jnp.concatenate(vectors).reshape(VR, U)
    t_down, t_up, t_out, t_qkv, t_vec = grad_reduce(
        grad_w_down.astype(BF16),
        grad_w_up.astype(BF16),
        grad_w_out.astype(BF16),
        grad_w_qkv.astype(BF16),
        packed,
        cycle_size // 2,
        lax.axis_size("dp"),
        1,
    )
    flat = t_vec.reshape(-1)
    own = lax.axis_index("fsdp")
    parts, start = [], 0
    for vector in vectors:
        half = vector.shape[0] // 2
        parts.append(lax.dynamic_slice_in_dim(flat, start + own * half, half, 0))
        start += 2 * half
    totals = (
        t_qkv, parts[0], parts[1], t_out, parts[2], parts[3], parts[4],
        t_up, parts[5], t_down, parts[6], parts[7], parts[8],
    )
    output_rows = result.astype(jnp.bfloat16).reshape(seq_count, block_rows, model_width)
    input_rows = grad_input.astype(jnp.bfloat16).reshape(seq_count, block_rows, model_width)
    return (
        output_rows,
        input_rows,
        totals[0],
        totals[1],
        totals[2],
        totals[3],
        totals[4],
        totals[5],
        totals[6],
        totals[7],
        totals[8],
        totals[9],
        totals[10],
        totals[11],
        totals[12],
    )


HW = 64
QT = 256


def remote(src, dst, ss, rs, dev):
    return pltpu.make_async_remote_copy(src_ref=src, dst_ref=dst, send_sem=ss, recv_sem=rs, device_id=dev, device_id_type=MESH)


def nt(a, b):
    return lax.dot_general(a, b, (((1,), (1,)), ((), ())), preferred_element_type=F32)


def mm(a, b):
    return jnp.dot(a, b, preferred_element_type=F32)


def head_masks(rows):
    lane = lax.broadcasted_iota(jnp.int32, (rows, 2 * HW), 1)
    return lane < HW


def normal_parts(v):
    mean = jnp.mean(v, -1, keepdims=True)
    cen = v - mean
    inv = lax.rsqrt(jnp.mean(cen * cen, -1, keepdims=True) + EPSILON)
    return cen * inv, inv


def normal_back(dn, hat, inv, gain):
    d = dn * gain
    return inv * (d - jnp.mean(d, -1, keepdims=True) - hat * jnp.mean(d * hat, -1, keepdims=True))


def gelu_pair(u):
    w = jnp.abs(u)
    t = 1.0 / (1.0 + (0.3275911 * math.sqrt(0.5)) * w)
    e = jnp.exp(-0.5 * u * u)
    poly = t * (0.127414796 + t * (-0.142248368 + t * (0.7107068705 + t * (-0.7265760135 + t * 0.5307027145))))
    tail = poly * e
    phi = jnp.where(u < 0.0, tail, 1.0 - tail)
    return u * phi, phi + u * (e * (1.0 / math.sqrt(2.0 * math.pi)))


def fold8(v):
    return jnp.sum(v.reshape(v.shape[0] // 8, 8, v.shape[1]), 0)


def fwd_kernel(nx, seqs, seq_rows, lens, tok, cot, sq, so_, su, sd, *rest):
    small = rest[:9]
    (qkv_o, att_o, lse_o, wq_o, wo_o, wu_o, wd_o, vec_o, y_o, dh_o, hat_o, act_o, gp_o, vg_o) = rest[9:23]
    (XT, WB, QKV, CT, ATT, LSE, H1, N1, N1B, ACT, GP, YB,
               ls, ys, yr, zs, zr, as_, ar, bs, br, t0s, t0r, t1s, t1r, t2s, t2r, vs, vr, lts, outs) = rest[23:]
    core, x, f, z = places()
    me = x * 2 + core
    nblk = 2 * nx
    rows = seqs * seq_rows
    sib = {"ctx": x * 2 + 1 - core}
    yp = {"fsdp": 1 - f}
    zp = {"dp": z + 1 - 2 * lax.rem(z, 2)}
    zb = lax.rem(z, 2)
    xts = [lax.rem(x + j, nx) for j in range(1, nx)]
    xps = [{"ctx": t * 2 + core} for t in xts]
    xsrc = [lax.rem(x + nx - j, nx) * 2 + core for j in range(1, nx)]
    peers = [sib, yp, zp] + xps
    bar = pltpu.get_barrier_semaphore()
    for p in peers:
        pl.semaphore_signal(bar, inc=1, device_id=p, device_id_type=MESH)
    order = (1, 2, 0)
    PR = U // 4
    piece = pl.multiple_of((zb * 2 + core) * PR, PR)
    zpiece = pl.multiple_of(((1 - zb) * 2 + core) * PR, PR)
    H = rows // 2

    def shard(b, r0, n):
        r = pl.ds(r0, n)
        if b < 3:
            return sq.at[r, pl.ds(b * 768, 768)]
        if b == 3:
            return so_.at[r, :]
        if b < 8:
            return su.at[r, pl.ds((b - 4) * 768, 768)]
        return sd.at[pl.ds((b - 8) * U + r0, n), :]

    def loc(b):
        return pltpu.make_async_copy(shard(b, 0, U), WB.at[b, f], ls.at[b])

    def ycp(b):
        if not isinstance(b, int):
            src = WB.at[b, f, pl.ds(piece, PR)]
        else:
            src = shard(b, piece, PR)
        return remote(src, WB.at[b, f, pl.ds(piece, PR)], ys.at[b], yr.at[b], yp)

    def zcp(b):
        w = WB.at[b, 1 - f, pl.ds(piece, PR)]
        return remote(w, w, zs.at[b], zr.at[b], zp)

    def acp(b):
        w = WB.at[b, 1 - f, pl.ds(piece, PR)]
        return remote(w, w, as_.at[b], ar.at[b], sib)

    def bcp(b):
        w = WB.at[b, 1 - f, pl.ds(zpiece, PR)]
        return remote(w, w, bs.at[b], br.at[b], sib)

    def A(b):
        ycp(b).wait_recv()
        zcp(b).start()
        acp(b).start()

    def B(b):
        zcp(b).wait_recv()
        bcp(b).start()

    def C(b):
        acp(b).wait_recv()
        bcp(b).wait_recv()

    def tsl(h):
        return pl.ds(h * H, H)

    def t_sib(h):
        return remote(tok.at[tsl(h)], XT.at[me, tsl(h)], t0s.at[h], t0r.at[h], sib)

    def t_x(j, h):
        return remote(tok.at[tsl(h)], XT.at[me, tsl(h)], t1s.at[j - 1, h], t1r.at[j - 1, h], xps[j - 1])

    def t_f(j, h):
        w = XT.at[xsrc[j - 1], tsl(h)]
        return remote(w, w, t2s.at[j - 1, h], t2r.at[j - 1, h], sib)

    vcp = remote(vec_o.at[f], vec_o.at[f], vs.at[0], vr.at[0], yp)
    tl = pltpu.make_async_copy(tok, XT.at[me], lts.at[0])
    tl.start()
    for b in order:
        loc(b).start()
    row = 0
    for v in small:
        for i in range(v.shape[1] // U):
            vec_o[f, row:row + 1, :] = v[:, i * U:(i + 1) * U].astype(F32)
            row += 1
    tc = pltpu.make_async_copy(cot, CT, lts.at[1])
    pl.semaphore_wait(bar, len(peers))
    vcp.start()
    for b in order:
        ycp(b).start()
    for h in range(2):
        for j in range(1, nx):
            t_x(j, h).start()
        t_sib(h).start()
    for b in range(3, 12):
        ycp(b).start()
    for b in range(3, 12):
        loc(b).start()
    tc.start()
    tl.wait()

    def qkv(b, blk):
        fac = 0.125 if b == 0 else 1.0

        def one(t, _):
            c = pl.ds(pl.multiple_of(t * 256, 256), 256)
            w = WB[b, :, :, c].reshape(768, 256)
            QKV[b, blk, :, c] = mm(XT[blk], w).astype(BF16)
            return 0
        if b == 1:
            lax.fori_loop(0, 3, one, 0)
        else:
            row = 0 if b == 0 else 1
            for t in range(3):
                w = WB[b, :, :, t * 256:(t + 1) * 256].reshape(768, 256)
                if t == 0:
                    bias = vec_o[0, row:row + 1, 0:256]
                elif t == 1:
                    bias = jnp.concatenate([vec_o[0, row:row + 1, 256:384], vec_o[1, row:row + 1, 0:128]], 1)
                else:
                    bias = vec_o[1, row:row + 1, 128:384]
                r = (mm(XT[blk], w) + bias).astype(BF16)
                if b == 0:
                    r = r * jnp.asarray(fac, BF16)
                QKV[b, blk, :, t * 256:(t + 1) * 256] = r

    seq = list(order)
    A(seq[0])
    A(seq[1])
    B(seq[0])
    for h in range(2):
        t_sib(h).wait_recv()
    A(seq[2])
    B(seq[1])
    vcp.wait_recv()
    for n, b in enumerate(seq):
        loc(b).wait()
        C(b)

        def both(i, _):
            qkv(b, x * 2 + i)
            return 0
        lax.fori_loop(0, 2, both, 0)
        if n == 0:
            B(seq[2])
            A(3)
        if n == 1:
            B(3)
            A(4)
    for j in range(1, nx):
        for h in range(2):
            t_x(j, h).wait_recv()
            t_f(j, h).start()
    B(4)
    A(5)
    for j in range(1, nx):
        for h in range(2):
            t_f(j, h).wait_recv()
        base = lax.rem(x + nx - j, nx) * 2

        def pair(i, _):
            for b in seq:
                qkv(b, base + i)
            return 0
        lax.fori_loop(0, 2, pair, 0)
    B(5)
    qo = pltpu.make_async_copy(QKV, qkv_o, outs.at[0])
    qo.start()

    low_half = head_masks(QT)
    lane128 = lax.broadcasted_iota(jnp.int32, (QT, 128), 1)
    kpos = lax.broadcasted_iota(jnp.int32, (QT, QT), 1)
    nr = seq_rows // QT

    def attend(tile, j):
        s0 = tile // nr
        qr = pl.ds(pl.multiple_of(tile * QT, QT), QT)
        cols = pl.ds(pl.multiple_of(j * 128, 128), 128)
        q = QKV[0, me, qr, cols]
        length = lens[s0]
        outs_ = []
        tot = LSE[qr, 0:128]
        for h in range(2):
            qh = jnp.where(low_half == (h == 0), q, jnp.zeros_like(q))
            sc = []
            mx = None
            for blk in range(nblk):
                for r in range(nr):
                    kr = pl.ds(pl.multiple_of(s0 * seq_rows + r * QT, QT), QT)
                    v = nt(qh, QKV[1, blk, kr, cols])
                    v = jnp.where(kpos < length - (blk * seq_rows + r * QT), v, MASKED)
                    sc.append(v)
                    mx = v if mx is None else jnp.maximum(mx, v)
            m = jnp.max(mx, 1, keepdims=True)
            acc = None
            lsum = None
            i = 0
            for blk in range(nblk):
                for r in range(nr):
                    kr = pl.ds(pl.multiple_of(s0 * seq_rows + r * QT, QT), QT)
                    p = jnp.exp(sc[i] - m)
                    i += 1
                    lsum = p if lsum is None else lsum + p
                    o = mm(p.astype(BF16), QKV[2, blk, kr, cols])
                    acc = o if acc is None else acc + o
            den = jnp.sum(lsum, 1, keepdims=True)
            outs_.append(acc / den)
            tot = jnp.where(lane128 == 2 * j + h, m + jnp.log(den), tot)
        ATT[qr, cols] = jnp.where(low_half, outs_[0], outs_[1])
        LSE[qr, 0:128] = tot

    ntile = rows // QT
    per = ntile * 6 // 4

    def group(g, _):
        A(6 + g)

        def one(i, _):
            it = g * per + i
            attend(it // 6, lax.rem(it, 6))
            return 0
        lax.fori_loop(0, per, one, 0)
        B(6 + g)
        return 0
    lax.fori_loop(0, 4, group, 0)
    A(10)
    extra = []

    def send_out(src, dst):
        cp = pltpu.make_async_copy(src, dst, outs.at[25 + len(extra)])
        cp.start()
        extra.append(cp)

    def full(b):
        res = []
        for ff in range(2):
            src = WB.at[b, ff]
            if b < 3:
                dst = wq_o.at[pl.ds(ff * U, U), pl.ds(b * 768, 768)]
            elif b == 3:
                dst = wo_o.at[pl.ds(ff * U, U), :]
            elif b < 8:
                dst = wu_o.at[pl.ds(ff * U, U), pl.ds((b - 4) * 768, 768)]
            else:
                dst = wd_o.at[pl.ds(ff * 1536 + (b - 8) * U, U), :]
            res.append(pltpu.make_async_copy(src, dst, outs.at[1 + 2 * b + ff]))
        return res

    def ready(b):
        loc(b).wait()
        C(b)
        for cp in full(b):
            cp.start()

    def vector(r):
        return jnp.concatenate([vec_o[0, r:r + 1, :], vec_o[1, r:r + 1, :]], 1)

    for b in range(3):
        for cp in full(b):
            cp.start()
    send_out(ATT, att_o)
    ready(3)
    bo = vector(2)
    for t in range(3):
        cs = slice(t * 256, (t + 1) * 256)
        w = WB[3, :, :, cs].reshape(768, 256)
        H1[:, cs] = XT[me, :, cs].astype(F32) + mm(ATT[...].astype(BF16), w) + bo[:, cs]
    g1, s1 = vector(3), vector(4)
    RB = 64

    def ln1(i, _):
        r = pl.ds(pl.multiple_of(i * RB, RB), RB)
        hat, inv = normal_parts(H1[r, :])
        H1[r, :] = hat
        n = hat * g1 + s1
        N1[r, :] = n
        N1B[r, :] = n.astype(BF16)
        LSE[r, 128:256] = jnp.broadcast_to(inv, (RB, 128))
        return 0
    lax.fori_loop(0, rows // RB, ln1, 0)
    send_out(H1, hat_o)
    send_out(LSE, lse_o)
    A(11)
    B(10)
    for b in range(4, 8):
        ready(b)

    def upblock(b, _):
        bias = jnp.concatenate([vec_o[b // 2, pl.ds(5 + lax.rem(b, 2) * 2, 1), :], vec_o[b // 2, pl.ds(6 + lax.rem(b, 2) * 2, 1), :]], 1)
        for t in range(3):
            w = WB[4 + b, :, :, t * 256:(t + 1) * 256].reshape(768, 256)
            cs = pl.ds(pl.multiple_of(b * 768 + t * 256, 256), 256)
            act, gp = gelu_pair(mm(N1B[...], w) + bias[:, t * 256:(t + 1) * 256])
            ACT[:, cs] = act.astype(BF16)
            GP[:, cs] = gp
        return 0
    lax.fori_loop(0, 2, upblock, 0)
    B(11)
    lax.fori_loop(2, 4, upblock, 0)
    send_out(ACT, act_o)
    send_out(GP, gp_o)
    for b in range(8, 12):
        ready(b)
    bd = vector(9)
    for t in range(3):
        cs = slice(t * 256, (t + 1) * 256)
        acc = N1[:, cs] + bd[:, cs]
        for ff in range(2):
            acc = acc + mm(ACT[:, ff * 1536:(ff + 1) * 1536], WB[8:12, ff, :, cs].reshape(1536, 256))
        N1[:, cs] = acc
    g2, s2 = vector(10), vector(11)
    tc.wait()

    def ln2(i, carry):
        r = pl.ds(pl.multiple_of(i * RB, RB), RB)
        hat, inv = normal_parts(N1[r, :])
        YB[r, :] = (hat * g2 + s2).astype(BF16)
        g = CT[r, :].astype(F32)
        N1[r, :] = normal_back(g, hat, inv, g2)
        return carry[0] + fold8(g * hat), carry[1] + fold8(g)
    zero = jnp.zeros((8, 768), F32)
    a0, a1 = lax.fori_loop(0, rows // RB, ln2, (zero, zero))
    send_out(YB, y_o)
    send_out(N1, dh_o)
    vg_o[0:1, :] = jnp.sum(a0, 0, keepdims=True)
    vg_o[1:2, :] = jnp.sum(a1, 0, keepdims=True)
    vcp.wait_send()
    qo.wait()
    for b in range(12):
        ycp(b).wait_send()
        zcp(b).wait_send()
        acp(b).wait_send()
        bcp(b).wait_send()
        for cp in full(b):
            cp.wait()
    for h in range(2):
        t_sib(h).wait_send()
        for j in range(1, nx):
            t_x(j, h).wait_send()
            t_f(j, h).wait_send()
    for cp in extra:
        cp.wait()


def forward_gather(lens, tok, cot, sq, so_, su, sd, small, nx, cid):
    seqs, seq_rows, d = tok.shape
    rows = seqs * seq_rows
    nblk = 2 * nx
    anyspec = pl.BlockSpec(memory_space=pl.ANY)
    vspec = pl.BlockSpec(memory_space=pltpu.VMEM)
    sspec = pl.BlockSpec(memory_space=pltpu.SMEM)
    D = pltpu.SemaphoreType.DMA
    V = pltpu.VMEM
    S = jax.ShapeDtypeStruct
    sems = [D((12,))] * 9 + [D((2,)), D((2,))] + [D((nx - 1, 2))] * 4 + [D((1,)), D((1,)), D((2,)), D((33,))]
    return pl.pallas_call(
        functools.partial(fwd_kernel, nx, seqs, seq_rows),
        out_shape=(S((3, nblk, rows, d), BF16), S((rows, d), F32), S((rows, 256), F32),
                   S((768, 2304), BF16), S((768, 768), BF16), S((768, 3072), BF16), S((3072, 768), BF16),
                   S((2, 12, U), F32), S((rows, d), BF16), S((rows, d), F32), S((rows, d), F32),
                   S((rows, 3072), BF16), S((rows, 3072), F32), S((2, d), F32)),
        in_specs=[sspec] + [anyspec] * 6 + [vspec] * 9,
        out_specs=(anyspec,) * 7 + (vspec,) + (anyspec,) * 5 + (vspec,),
        scratch_shapes=[V((nblk, rows, d), BF16), V((12, 2, U, 768), BF16), V((3, nblk, rows, d), BF16),
                        V((rows, d), BF16), V((rows, d), F32), V((rows, 256), F32), V((rows, d), F32), V((rows, d), F32),
                        V((rows, d), BF16), V((rows, 3072), BF16), V((rows, 3072), F32), V((rows, d), BF16)] + sems,
        compiler_params=pltpu.CompilerParams(collective_id=cid, has_side_effects=True, vmem_limit_bytes=62 << 20),
        name="forward_gather",
    )(lens, tok.reshape(rows, d), cot.reshape(rows, d), sq, so_, su, sd, *[v.reshape(1, -1) for v in small])


def tn(a, b):
    return lax.dot_general(a, b, (((0,), (0,)), ((), ())), preferred_element_type=F32)


def colsum(v):
    return jnp.sum(fold8(v), 0, keepdims=True)


def bwd_kernel(nx, nd, seqs, seq_rows, lens, vec, vg, qkv_i, att_i, lse_i, wq_i, wo_i, wu_i, wd_i, dh_i, hat_i, act_i, gp_i, tok_i,
               od, ou, oo, oq, ov, gin_o,
               BIG, WO, WQ, GP, ACT, DH, DM, HAT, NB, DO, ROWS, COLS, DQKV, L, SB, R1, R2, R3, R4, AX, VV, V0, VX, VZ,
               lds, d0s, d0r, d1s, d1r, d2s, d2r, s1s, s1r, s2s, s2r, s3s, s3r, s4s, s4r, s5s, s5r, s6s, s6r, s7s, s7r, s8, vs, vr):
    core, x, f, z = places()
    me = x * 2 + core
    nblk = 2 * nx
    rows = seqs * seq_rows
    CX, PZ = U // nx, U // nx // nd
    NCH = 12
    sib = {"ctx": x * 2 + 1 - core}
    yp = {"fsdp": 1 - f}
    xps = [{"ctx": lax.rem(x + j, nx) * 2 + core} for j in range(1, nx)]
    xsrc = [lax.rem(x + nx - j, nx) * 2 + core for j in range(1, nx)]
    zps = [{"dp": lax.rem(z + j, nd)} for j in range(1, nd)]
    peers = [sib, yp] + xps + zps
    bar = pltpu.get_barrier_semaphore()
    for p in peers:
        pl.semaphore_signal(bar, inc=1, device_id=p, device_id_type=MESH)

    loads = {}

    def load(name, src, dst):
        cp = pltpu.make_async_copy(src, dst, lds.at[len(loads)])
        cp.start()
        loads[name] = cp

    load("dh", dh_i, DH)
    load("act", act_i, ACT)
    load("wd", wd_i, BIG.at[pl.ds(0, 3072)])
    load("gp0", gp_i.at[:, pl.ds(0, 768)], GP.at[0])
    load("hat", hat_i, HAT)
    load("gp1", gp_i.at[:, pl.ds(768, 768)], GP.at[1])
    for b in range(4):
        load(("wu", b), wu_i.at[:, pl.ds(b * 768, 768)], BIG.at[pl.ds(3072 + b * 768, 768)])
    load("lse", lse_i, COLS.at[:, pl.ds(0, 256)])
    load("wo", wo_i, WO)
    for b in range(3):
        load(("wq", b), wq_i.at[:, pl.ds(b * 768, 768)], WQ.at[b])

    def vector(r):
        return jnp.concatenate([vec[0, r:r + 1, :], vec[1, r:r + 1, :]], 1)

    def c1(i, ff, k):
        return remote(SB.at[i % 4, ff], R1.at[i, ff], s1s.at[i, k], s1r.at[i, k], sib)

    def c1s(i):
        return [c1(i, 1 - f, 0), c1(i, f, 1)]

    def c2(c):
        return remote(L.at[c, 1 - f], R2.at[c], s2s.at[c], s2r.at[c], yp)

    def c3(c, j):
        xt = lax.rem(x + j, nx)
        return remote(L.at[c, f, pl.ds(pl.multiple_of(xt * CX, CX), CX)], R3.at[c, j - 1], s3s.at[c, j - 1], s3r.at[c, j - 1], xps[j - 1])

    def mine(zz):
        return pl.ds(pl.multiple_of(x * CX + zz * PZ, PZ), PZ)

    def c4(c, j):
        zt = lax.rem(z + j, nd)
        return remote(L.at[c, f, mine(zt)], R4.at[c, j - 1], s4s.at[c, j - 1], s4r.at[c, j - 1], zps[j - 1])

    def c5(c, j):
        w = AX.at[c, mine(z)]
        return remote(w, w, s5s.at[c, j - 1], s5r.at[c, j - 1], zps[j - 1])

    def c6(c, j):
        w = AX.at[c, pl.ds(pl.multiple_of(x * CX, CX), CX)]
        return remote(w, w, s6s.at[c, j - 1], s6r.at[c, j - 1], xps[j - 1])

    def orect(i):
        if i < 4:
            return od.at[pl.ds(pl.multiple_of(core * 768 + i // 2 * U, U), U), pl.ds(i % 2 * U, U)]
        if i < 8:
            return ou.at[:, pl.ds(pl.multiple_of(core * 1536 + (i - 4) * U, 128), U)]
        if i < 9:
            return oo.at[:, pl.ds(pl.multiple_of(core * U, 128), U)]
        return oq.at[:, pl.ds(pl.multiple_of(core * 1152 + (i - 9) * U, 128), U)]

    def c7(c):
        return remote(AX.at[c], orect(c), s7s.at[c], s7r.at[c], sib)

    def c8(c):
        return pltpu.make_async_copy(AX.at[c], orect(c), s8.at[c])

    B = 48

    def rows_loop(n, fn):
        def bodyf(i, _):
            fn(pl.multiple_of(i * B, B))
            return 0
        lax.fori_loop(0, n // B, bodyf, 0)

    def up(v):
        return v.astype(F32)

    def st1(i):
        for cp in c1s(i):
            cp.start()

    def st2(c):
        c1(c, 1 - f, 0).wait_recv()

        def fn(r):
            s = pl.ds(r, B)
            L[c, 1 - f, s, :] = (up(L[c, 1 - f, s, :]) + up(R1[c, 1 - f, s, :])).astype(BF16)
        rows_loop(U, fn)
        c2(c).start()

    def st3(c):
        c1(c, f, 1).wait_recv()
        c2(c).wait_recv()
        for j in range(1, nx):
            xt = lax.rem(x + j, nx)

            def fn(r):
                s = pl.ds(pl.multiple_of(xt * CX + r, B), B)
                L[c, f, s, :] = (up(L[c, f, s, :]) + up(R1[c, f, s, :]) + up(R2[c, s, :])).astype(BF16)
            rows_loop(CX, fn)
            c3(c, j).start()

    def st4(c):
        for j in range(1, nx):
            c3(c, j).wait_recv()

        def fn(r):
            s = pl.ds(pl.multiple_of(x * CX + r, B), B)
            t = up(L[c, f, s, :]) + up(R1[c, f, s, :]) + up(R2[c, s, :])
            for j in range(1, nx):
                t = t + up(R3[c, j - 1, pl.ds(r, B), :])
            L[c, f, s, :] = t.astype(BF16)
        rows_loop(CX, fn)
        for j in range(1, nd):
            c4(c, j).start()

    def st5(c):
        for j in range(1, nd):
            c4(c, j).wait_recv()
        t = up(L[c, f, mine(z), :])
        for j in range(1, nd):
            t = t + up(R4[c, j - 1])
        AX[c, mine(z), :] = t.astype(BF16)
        for j in range(1, nd):
            c5(c, j).start()

    def st6(c):
        for j in range(1, nd):
            c5(c, j).wait_recv()
        for j in range(1, nx):
            c6(c, j).start()

    def st7(c):
        for j in range(1, nx):
            c6(c, j).wait_recv()
        c7(c).start()
        c8(c).start()

    def tick(c):
        stages = ((4, st7), (3, st6), (2, st5), (1, st4), (0, st3))
        if isinstance(c, int):
            for lag, fn in stages:
                if 0 <= c - lag < NCH:
                    fn(c - lag)
        else:
            for lag, fn in stages[1:]:
                if lag == 0:
                    fn(c)
                else:
                    @pl.when(c >= lag)
                    def _():
                        fn(c - lag)

    def v_core():
        return remote(VV, V0.at[0], vs.at[0], vr.at[0], sib)

    def v_y():
        return remote(V0.at[1], V0.at[2], vs.at[1], vr.at[1], yp)

    def v_x(j):
        return remote(VX.at[x], VX.at[x], vs.at[1 + j], vr.at[1 + j], xps[j - 1])

    def v_z(j):
        return remote(VZ.at[z], VZ.at[z], vs.at[nx + j], vr.at[nx + j], zps[j - 1])

    def vst(k):
        if k == 0:
            v_core().start()
        elif k == 1:
            v_core().wait_recv()
            V0[1] = VV[...] + V0[0]
            v_y().start()
        elif k == 2:
            v_y().wait_recv()
            VX[x] = V0[1] + V0[2]
            for j in range(1, nx):
                v_x(j).start()
        elif k == 3:
            for j in range(1, nx):
                v_x(j).wait_recv()
            t = VX[0]
            for j in range(1, nx):
                t = t + VX[j]
            VZ[z] = t
            for j in range(1, nd):
                v_z(j).start()
        elif k == 4:
            for j in range(1, nd):
                v_z(j).wait_recv()
            t = VZ[0]
            for j in range(1, nd):
                t = t + VZ[j]
            VV2 = t
            for r, n, o in ((0, 1, 0), (2, 1, 1), (4, 1, 2), (6, 1, 3), (8, 1, 4), (10, 4, 5), (18, 1, 9), (20, 1, 10), (22, 1, 11)):
                ov[o:o + n, :] = jnp.where(f == 0, VV2[r:r + n, :], VV2[r + n:r + 2 * n, :])

    def put_vec(r, v):
        VV[r:r + 1, :] = v[:, :U]
        VV[r + 1:r + 2, :] = v[:, U:]

    put_vec(20, vg[0:1, :])
    put_vec(22, vg[1:2, :])

    RB = 64
    loads["dh"].wait()

    def to_dm(i, acc):
        r = pl.ds(pl.multiple_of(i * RB, RB), RB)
        v = DH[r, :].astype(BF16)
        DM[r, :] = v
        return acc + fold8(v.astype(F32))
    zero = jnp.zeros((8, 768), F32)
    put_vec(18, jnp.sum(lax.fori_loop(0, rows // RB, to_dm, zero), 0, keepdims=True))
    loads["act"].wait()

    def fill(i0, kk, ff, val, wide):
        v = val.astype(BF16)
        for t in range(wide):
            if kk == 0:
                L[i0 + t, ff] = v[:, t * U:(t + 1) * U]
            else:
                SB[(i0 + t) % 4, ff] = v[:, t * U:(t + 1) * U]

    def each_f(fn):
        def one(k, _):
            fn(jnp.where(k == 0, 1 - f, f))
            return 0
        lax.fori_loop(0, 2, one, 0)

    def ccof(kk):
        return core if kk == 0 else 1 - core

    for ii in range(2):
        for kk in (1, 0):
            def wdown(ff, kk=kk, ii=ii):
                h = pl.multiple_of(ff * 1536 + ccof(kk) * 768 + ii * U, U)
                fill(2 * ii, kk, ff, tn(ACT[:, pl.ds(h, U)], DM[...]), 2)
            each_f(wdown)
            if kk == 1:
                if ii == 0:
                    pl.semaphore_wait(bar, len(peers))
                st1(2 * ii)
                st1(2 * ii + 1)
    st2(0)
    st2(1)
    loads["wd"].wait()
    for b in range(4):
        loads["gp%d" % b].wait()
        for t in range(3):
            h = b * 768 + t * 256
            du = (nt(DM[...], BIG[h:h + 256, :]) * GP[b % 2, :, t * 256:(t + 1) * 256]).astype(BF16)
            ACT[:, h:h + 256] = du
            s = colsum(du.astype(F32))
            for q in range(2):
                o = h + q * 128
                VV[10 + o // U:11 + o // U, o % U:o % U + 128] = s[:, q * 128:(q + 1) * 128]
        if b < 2:
            load("gp%d" % (b + 2), gp_i.at[:, pl.ds((b + 2) * 768, 768)], GP.at[b % 2])
        if b == 1:
            st2(2)
    st2(3)
    loads["hat"].wait()
    g1, s1 = vector(3), vector(4)

    def to_nb(i, _):
        r = pl.ds(pl.multiple_of(i * RB, RB), RB)
        NB[r, :] = (HAT[r, :] * g1 + s1).astype(BF16)
        return 0
    lax.fori_loop(0, rows // RB, to_nb, 0)
    for ii in range(2):
        for kk in (1, 0):
            if kk == 1:
                for i in (2 * ii, 2 * ii + 1):
                    for cp in c1s(i):
                        cp.wait_send()

            def wup(ff, kk=kk, ii=ii):
                h = pl.multiple_of(ccof(kk) * 1536 + ii * 768, 768)
                fill(4 + 2 * ii, kk, ff, tn(NB[:, pl.ds(pl.multiple_of(ff * U, U), U)], ACT[:, pl.ds(h, 768)]), 2)
            each_f(wup)
            if kk == 1:
                st1(4 + 2 * ii)
                st1(5 + 2 * ii)
    load("tok", tok_i, NB)
    for b in range(4):
        loads[("wu", b)].wait()
    for t in range(3):
        cs = slice(t * 256, (t + 1) * 256)
        acc = DH[:, cs]
        for b in range(4):
            acc = acc + nt(ACT[:, b * 768:(b + 1) * 768], BIG[3072 + b * 768 + t * 256:3072 + b * 768 + (t + 1) * 256, :])
        DH[:, cs] = acc
    for k in (1, 2, 0):
        for blk in range(nblk):
            load(("qkv", k, blk), qkv_i.at[k, blk], BIG.at[pl.ds((k * nblk + blk) * rows, rows)])
    st2(4)
    st2(5)
    loads["lse"].wait()

    def ln1(i, carry):
        r = pl.ds(pl.multiple_of(i * RB, RB), RB)
        dn, hat = DH[r, :], HAT[r, :]
        d = normal_back(dn, hat, COLS[r, 128:129], g1)
        DH[r, :] = d
        da = d.astype(BF16)
        DM[r, :] = da
        return carry[0] + fold8(dn * hat), carry[1] + fold8(dn), carry[2] + fold8(da.astype(F32))
    sums = lax.fori_loop(0, rows // RB, ln1, (zero, zero, zero))
    for row, sv in zip((6, 8, 4), sums):
        put_vec(row, jnp.sum(sv, 0, keepdims=True))
    load("att", att_i, HAT)
    loads["wo"].wait()
    for t in range(3):
        DO[me, :, t * 256:(t + 1) * 256] = nt(DM[...], WO[t * 256:(t + 1) * 256, :]).astype(BF16)

    def d_sib():
        return remote(DO.at[me], DO.at[me], d0s.at[0], d0r.at[0], sib)

    def d_x(j):
        return remote(DO.at[me], DO.at[me], d1s.at[j - 1, 0], d1r.at[j - 1, 0], xps[j - 1])

    def d_f(j):
        w = DO.at[xsrc[j - 1]]
        return remote(w, w, d2s.at[j - 1, 0], d2r.at[j - 1, 0], sib)

    def r_sib():
        return remote(ROWS.at[me], ROWS.at[me], d0s.at[1], d0r.at[1], sib)

    def r_x(j):
        return remote(ROWS.at[me], ROWS.at[me], d1s.at[j - 1, 1], d1r.at[j - 1, 1], xps[j - 1])

    def r_f(j):
        w = ROWS.at[xsrc[j - 1]]
        return remote(w, w, d2s.at[j - 1, 1], d2r.at[j - 1, 1], sib)

    for j in range(1, nx):
        d_x(j).start()
    d_sib().start()
    loads["att"].wait()
    for kk in (1, 0):
        if kk == 1:
            for cp in c1s(4):
                cp.wait_send()

        def wout(ff, kk=kk):
            a = HAT[:, pl.ds(pl.multiple_of(ff * U, U), U)].astype(BF16)
            fill(8, kk, ff, tn(a, DM[:, pl.ds(pl.multiple_of(ccof(kk) * U, U), U)]), 1)
        each_f(wout)
        if kk == 1:
            st1(8)
    head = lax.broadcasted_iota(jnp.int32, (768, 128), 0) // HW
    pick = (head == lax.broadcasted_iota(jnp.int32, (768, 128), 1)).astype(BF16)

    def delta(i, _):
        r = pl.ds(pl.multiple_of(i * 128, 128), 128)
        v = DO[me, r, :].astype(F32) * HAT[r, :]
        hi = v.astype(BF16)
        rest = v - hi.astype(F32)
        mid = rest.astype(BF16)
        low = (rest - mid.astype(F32)).astype(BF16)
        d = mm(hi, pick) + mm(mid, pick) + mm(low, pick)
        COLS[r, 128:256] = d
        ROWS[me, 16:32, r] = jnp.transpose(d)[0:16, :]
        ROWS[me, 0:16, r] = jnp.transpose(COLS[r, 0:128])[0:16, :]
        return 0
    lax.fori_loop(0, rows // 128, delta, 0)
    for j in range(1, nx):
        r_x(j).start()
    r_sib().start()
    st2(6)
    st2(7)
    st2(8)
    tick(0)

    for k in (1, 2, 0):
        for blk in range(nblk):
            loads[("qkv", k, blk)].wait()
    low_half = head_masks(QT)
    lane128 = lax.broadcasted_iota(jnp.int32, (QT, 128), 1)
    kpos = lax.broadcasted_iota(jnp.int32, (QT, QT), 1)
    krow = lax.broadcasted_iota(jnp.int32, (QT, 128), 0)
    nr = seq_rows // QT
    ntile = rows // QT

    def big(k, blk, r0, cols):
        return BIG[pl.ds(pl.multiple_of((k * nblk + blk) * rows + r0, QT), QT), cols]

    def pick_col(v, h):
        return jnp.sum(jnp.where(lane128 == h, v, 0.0), 1, keepdims=True)

    def zero_other(v, h):
        return jnp.where(low_half == (h == 0), v, jnp.zeros_like(v))

    def dq_one(tile, j):
        s0 = tile // nr
        q0 = pl.multiple_of(tile * QT, QT)
        qr = pl.ds(q0, QT)
        cols = pl.ds(pl.multiple_of(j * 128, 128), 128)
        q = big(0, me, q0, cols)
        do = DO[me, qr, cols]
        length = lens[s0]
        res = []
        for h in range(2):
            qh, doh = zero_other(q, h), zero_other(do, h)
            lse = pick_col(COLS[qr, 0:128], 2 * j + h)
            dl = pick_col(COLS[qr, 128:256], 2 * j + h)
            acc = None
            for blk in range(nblk):
                for r in range(nr):
                    k0 = s0 * seq_rows + r * QT
                    kt = big(1, blk, k0, cols)
                    p = jnp.exp(nt(qh, kt) - lse)
                    p = jnp.where(kpos < length - (blk * seq_rows + r * QT), p, 0.0)
                    ds = (p * (nt(doh, big(2, blk, k0, cols)) - dl)).astype(BF16)
                    o = mm(ds, kt)
                    acc = o if acc is None else acc + o
            res.append(acc)
        DQKV[0, qr, cols] = (jnp.where(low_half, res[0], res[1]) * 0.125).astype(BF16)

    def dkv_one(tile, j):
        s0 = tile // nr
        k0 = pl.multiple_of(tile * QT, QT)
        kr = pl.ds(k0, QT)
        cols = pl.ds(pl.multiple_of(j * 128, 128), 128)
        k, v = big(1, me, k0, cols), big(2, me, k0, cols)
        live = krow < lens[s0] - (me * seq_rows + (tile - s0 * nr) * QT)
        resk, resv = [], []
        for h in range(2):
            kh, vh = zero_other(k, h), zero_other(v, h)
            ak = av = None
            for blk in range(nblk):
                for r in range(nr):
                    q0 = pl.multiple_of(s0 * seq_rows + r * QT, QT)
                    qr = pl.ds(q0, QT)
                    qt, dt = big(0, blk, q0, cols), DO[blk, qr, cols]
                    lse = ROWS[blk, pl.ds(2 * j + h, 1), qr]
                    dl = ROWS[blk, pl.ds(16 + 2 * j + h, 1), qr]
                    p = jnp.exp(nt(kh, qt) - lse)
                    ds = (p * (nt(vh, dt) - dl)).astype(BF16)
                    ov_, ok_ = mm(p.astype(BF16), dt), mm(ds, qt)
                    av = ov_ if av is None else av + ov_
                    ak = ok_ if ak is None else ak + ok_
            resk.append(ak)
            resv.append(av)
        DQKV[1, kr, cols] = jnp.where(live, jnp.where(low_half, resk[0], resk[1]), 0.0).astype(BF16)
        DQKV[2, kr, cols] = jnp.where(live, jnp.where(low_half, resv[0], resv[1]), 0.0).astype(BF16)

    def segment(fn, groups, first):
        per = ntile * 6 // groups

        def group(g, _):
            def one(i, _):
                it = g * per + i
                fn(it // 6, lax.rem(it, 6))
                return 0
            lax.fori_loop(0, per, one, 0)
            tick(first + g)
            return 0
        lax.fori_loop(0, groups, group, 0)

    segment(dq_one, 2, 1)
    for j in range(1, nx):
        d_x(j).wait_recv()
        d_f(j).start()
        r_x(j).wait_recv()
        r_f(j).start()
    d_sib().wait_recv()
    r_sib().wait_recv()
    for j in range(1, nx):
        d_f(j).wait_recv()
        r_f(j).wait_recv()
    segment(dkv_one, 3, 3)

    loads["tok"].wait()
    for kk in (1, 0):
        if kk == 1:
            for i in (5, 6, 7):
                for cp in c1s(i):
                    cp.wait_send()
        for i in range(3):
            def wqkv(ff, kk=kk, i=i):
                p = ccof(kk) * 3 + i
                a = NB[:, pl.ds(pl.multiple_of(ff * U, U), U)]
                fill(9 + i, kk, ff, tn(a, DQKV[p // 2, :, pl.ds(pl.multiple_of(lax.rem(p, 2) * U, U), U)]), 1)
            each_f(wqkv)
            if kk == 1:
                st1(9 + i)

    def bias_sum(k):
        def one(i, acc):
            return acc + fold8(DQKV[k, pl.ds(pl.multiple_of(i * RB, RB), RB), :].astype(F32))
        return jnp.sum(lax.fori_loop(0, rows // RB, one, zero), 0, keepdims=True)
    st2(9)
    st2(10)
    st2(11)
    put_vec(0, bias_sum(0))
    put_vec(2, bias_sum(2))
    vst(0)
    tick(6)
    vst(1)
    for b in range(3):
        loads[("wq", b)].wait()
    for t in range(3):
        cs = slice(t * 256, (t + 1) * 256)
        acc = DH[:, cs]
        for b in range(3):
            acc = acc + nt(DQKV[b], WQ[b, cs, :])
        DM[:, cs] = acc.astype(BF16)
    gout = pltpu.make_async_copy(DM, gin_o, s8.at[NCH])
    gout.start()
    vst(2)
    st7(0)
    st7(1)
    tick(7)
    vst(3)
    for c in range(8, NCH + 4):
        tick(c)
        if c == 8:
            vst(4)
    for c in range(NCH):
        c2(c).wait_send()
        c7(c).wait()
        c8(c).wait()
        for j in range(1, nx):
            c3(c, j).wait_send()
            c6(c, j).wait_send()
        for j in range(1, nd):
            c4(c, j).wait_send()
            c5(c, j).wait_send()
    for i in (8, 9, 10, 11):
        for cp in c1s(i):
            cp.wait_send()
    gout.wait()
    v_core().wait_send()
    v_y().wait_send()
    d_sib().wait_send()
    r_sib().wait_send()
    for j in range(1, nx):
        v_x(j).wait_send()
        d_x(j).wait_send()
        d_f(j).wait_send()
        r_x(j).wait_send()
        r_f(j).wait_send()
    for j in range(1, nd):
        v_z(j).wait_send()


def backward_reduce(lens, vec, vg, qkv, att, lse, wq, wo, wu, wd, dh, hat, act, gp, tok, nx, nd, seqs, cid):
    rows, d = att.shape
    nblk = 2 * nx
    CX, PZ = U // nx, U // nx // nd
    N = 12
    anyspec = pl.BlockSpec(memory_space=pl.ANY)
    vspec = pl.BlockSpec(memory_space=pltpu.VMEM)
    sspec = pl.BlockSpec(memory_space=pltpu.SMEM)
    D = pltpu.SemaphoreType.DMA
    V = pltpu.VMEM
    S = jax.ShapeDtypeStruct
    sems = [D((32,)), D((2,)), D((2,))] + [D((nx - 1, 2))] * 4 + [D((N, 2)), D((N, 2)), D((N,)), D((N,)), D((N, nx - 1)), D((N, nx - 1)),
            D((N, nd - 1)), D((N, nd - 1)), D((N, nd - 1)), D((N, nd - 1)), D((N, nx - 1)), D((N, nx - 1)),
            D((N,)), D((N,)), D((N + 1,)), D((nx + nd,)), D((nx + nd,))]
    return pl.pallas_call(
        functools.partial(bwd_kernel, nx, nd, seqs, rows // seqs),
        out_shape=(S((1536, 768), BF16), S((U, 3072), BF16), S((U, 768), BF16), S((U, 2304), BF16), S((12, U), F32), S((rows, d), BF16)),
        in_specs=[sspec, vspec, vspec] + [anyspec] * 12,
        out_specs=(anyspec,) * 4 + (vspec, anyspec),
        scratch_shapes=[V((6144, d), BF16), V((d, d), BF16), V((3, d, d), BF16), V((2, rows, d), F32), V((rows, 3072), BF16),
                        V((rows, d), F32), V((rows, d), BF16), V((rows, d), F32), V((rows, d), BF16), V((nblk, rows, d), BF16),
                        V((nblk, 32, rows), F32), V((rows, 256), F32), V((3, rows, d), BF16),
                        V((N, 2, U, U), BF16), V((4, 2, U, U), BF16), V((N, 2, U, U), BF16), V((N, U, U), BF16),
                        V((N, nx - 1, CX, U), BF16), V((N, nd - 1, PZ, U), BF16), V((N, U, U), BF16),
                        V((24, U), F32), V((3, 24, U), F32), V((nx, 24, U), F32), V((nd, 24, U), F32)] + sems,
        compiler_params=pltpu.CompilerParams(collective_id=cid, has_side_effects=True, vmem_limit_bytes=63 << 20),
        name="backward_reduce",
    )(lens, vec, vg, qkv, att, lse, wq, wo, wu, wd, dh, hat, act, gp, tok)


def fast_body(
    tokens, cotangent, lengths, w_qkv, bias_q, bias_v, w_out, bias_out, gain_one, shift_one,
    w_up, bias_up, w_down, bias_down, gain_two, shift_two,
):
    seqs, seq_rows, width = tokens.shape
    nx, nd = lax.axis_size("ctx") // 2, lax.axis_size("dp")
    small = [bias_q, bias_v, bias_out, gain_one, shift_one, bias_up, bias_down, gain_two, shift_two]
    (qkv, att, lse, wq, wo, wu, wd, vec, out, dh, hat, act, gp, vg) = forward_gather(
        lengths, tokens, cotangent, w_qkv, w_out, w_up, w_down, small, nx, 2
    )
    t_down, t_up, t_out, t_qkv, t_vec, grad_in = backward_reduce(
        lengths, vec, vg, qkv, att, lse, wq, wo, wu, wd, dh, hat, act, gp,
        tokens.reshape(seqs * seq_rows, width), nx, nd, seqs, 3
    )

    def part(first, count):
        return t_vec[first : first + count].reshape(-1)

    return (
        out.reshape(tokens.shape), grad_in.reshape(tokens.shape), t_qkv.astype(F32), part(0, 1), part(1, 1),
        t_out.astype(F32), part(2, 1), part(3, 1), part(4, 1), t_up.astype(F32), part(5, 4),
        t_down.astype(F32), part(9, 1), part(10, 1), part(11, 1),
    )


def solution(mesh):
    return jax.shard_map(
        fast_body if mesh.shape["ctx"] <= 4 else general_body,
        mesh=mesh,
        in_specs=(
            P(("dp", "fsdp"), "ctx", None),
            P(("dp", "fsdp"), "ctx", None),
            P(("dp", "fsdp")),
            P("fsdp", None),
            P("fsdp"),
            P("fsdp"),
            P("fsdp", None),
            P("fsdp"),
            P("fsdp"),
            P("fsdp"),
            P("fsdp", None),
            P("fsdp"),
            P("fsdp", None),
            P("fsdp"),
            P("fsdp"),
            P("fsdp"),
        ),
        out_specs=(
            P(("dp", "fsdp"), "ctx", None),
            P(("dp", "fsdp"), "ctx", None),
            P("fsdp", None),
            P("fsdp"),
            P("fsdp"),
            P("fsdp", None),
            P("fsdp"),
            P("fsdp"),
            P("fsdp"),
            P("fsdp", None),
            P("fsdp"),
            P("fsdp", None),
            P("fsdp"),
            P("fsdp"),
            P("fsdp"),
        ),
        check_vma=False,
    )
```

```python
import functools
import math

import jax
import jax.numpy as jnp
from jax import lax
from jax.experimental import pallas as pl
from jax.experimental.pallas import tpu as pltpu
from jax.sharding import PartitionSpec as P

MESH = pl.DeviceIdType.MESH
F32, BF16 = jnp.float32, jnp.bfloat16
U = 384
VR = 24


def places():
    c = lax.axis_index("ctx")
    return lax.rem(c, 2), c // 2, lax.axis_index("fsdp"), lax.axis_index("dp")


def grad_kernel(nx, nd, grp, wd, wu, wo, wq, vec, od, ou, oo, oq, ov,
                L, R1, R2, R3, R4, AX, AC, ST, V0, VX, VZ,
                s0, s1s, s1r, s2s, s2r, s3s, s3r, s4s, s4r, s5s, s5r, s6s, s6r, s7s, s7r, so, vs, vr):
    core, x, f, z = places()
    nch = 12 // grp
    CH, CX, PZ = U * grp, U * grp // nx, U * grp // nx // nd
    sib = {"ctx": x * 2 + 1 - core}
    yp = {"fsdp": 1 - f}
    xps = [{"ctx": lax.rem(x + j, nx) * 2 + core} for j in range(1, nx)]
    zps = [{"dp": lax.rem(z + j, nd)} for j in range(1, nd)]
    peers = [sib, yp] + xps + zps
    bar = pltpu.get_barrier_semaphore()
    for p in peers:
        pl.semaphore_signal(bar, inc=1, device_id=p, device_id_type=MESH)

    def rect(i, ff, cc):
        if i < 4:
            return wd, ff * 1536 + i * U, cc * U
        if i < 8:
            return wu, ff * U, cc * 1536 + (i - 4) * U
        if i < 9:
            return wo, ff * U, cc * U
        return wq, ff * U, cc * 1152 + (i - 9) * U

    def orect(i, cc):
        if i < 4:
            return od, i * U, cc * U
        if i < 8:
            return ou, 0, cc * 1536 + (i - 4) * U
        if i < 9:
            return oo, 0, cc * U
        return oq, 0, cc * 1152 + (i - 9) * U

    def sl(ref, r, c):
        return ref.at[pl.ds(pl.multiple_of(r, U), U), pl.ds(pl.multiple_of(c, 128), U)]

    def local(i, k):
        ff = (1 - f) if k == 0 else f
        return pltpu.make_async_copy(sl(*rect(i, ff, core)), L.at[i // grp, ff, pl.ds(i % grp * U, U)], s0.at[i, k])

    def remote(src, dst, ss, rs, dev):
        return pltpu.make_async_remote_copy(src_ref=src, dst_ref=dst, send_sem=ss, recv_sem=rs, device_id=dev, device_id_type=MESH)

    def c1(i, k):
        ff = (1 - f) if k == 0 else f
        return remote(sl(*rect(i, ff, 1 - core)), R1.at[i // grp, ff, pl.ds(i % grp * U, U)], s1s.at[i, k], s1r.at[i, k], sib)

    def c2(c):
        return remote(L.at[c, 1 - f], R2.at[c], s2s.at[c], s2r.at[c], yp)

    def c3(c, j):
        xt = lax.rem(x + j, nx)
        return remote(L.at[c, f, pl.ds(pl.multiple_of(xt * CX, CX), CX)], R3.at[c, j - 1], s3s.at[c, j - 1], s3r.at[c, j - 1], xps[j - 1])

    def mine(c, zz):
        return pl.ds(pl.multiple_of(x * CX + zz * PZ, PZ), PZ)

    def c4(c, j):
        zt = lax.rem(z + j, nd)
        return remote(L.at[c, f, mine(c, zt)], R4.at[c, j - 1], s4s.at[c, j - 1], s4r.at[c, j - 1], zps[j - 1])

    def c5(c, j):
        return remote(AX.at[c, mine(c, z)], AX.at[c, mine(c, z)], s5s.at[c, j - 1], s5r.at[c, j - 1], zps[j - 1])

    def c6(c, j):
        rows = pl.ds(pl.multiple_of(x * CX, CX), CX)
        return remote(AX.at[c, rows], AX.at[c, rows], s6s.at[c, j - 1], s6r.at[c, j - 1], xps[j - 1])

    def c7(c):
        return remote(AX.at[c], AC.at[c], s7s.at[c], s7r.at[c], sib)

    B = 48

    def rows_loop(n, fn):
        def bodyf(i, _):
            fn(pl.multiple_of(i * B, B))
            return 0
        lax.fori_loop(0, n // B, bodyf, 0)

    def up(v):
        return v.astype(F32)

    def st2(c):
        for k in range(grp):
            local(c * grp + k, 0).wait()
            c1(c * grp + k, 0).wait_recv()

        def fn(r):
            s = pl.ds(r, B)
            L[c, 1 - f, s, :] = (up(L[c, 1 - f, s, :]) + up(R1[c, 1 - f, s, :])).astype(BF16)
        rows_loop(CH, fn)
        c2(c).start()

    def st3(c):
        for k in range(grp):
            local(c * grp + k, 1).wait()
            c1(c * grp + k, 1).wait_recv()
        c2(c).wait_recv()
        for j in range(1, nx):
            xt = lax.rem(x + j, nx)

            def fn(r):
                s = pl.ds(pl.multiple_of(xt * CX + r, B), B)
                L[c, f, s, :] = (up(L[c, f, s, :]) + up(R1[c, f, s, :]) + up(R2[c, s, :])).astype(BF16)
            rows_loop(CX, fn)
            c3(c, j).start()

    def st4(c):
        for j in range(1, nx):
            c3(c, j).wait_recv()

        def fn(r):
            s = pl.ds(pl.multiple_of(x * CX + r, B), B)
            t = up(L[c, f, s, :]) + up(R1[c, f, s, :]) + up(R2[c, s, :])
            for j in range(1, nx):
                t = t + up(R3[c, j - 1, pl.ds(r, B), :])
            L[c, f, s, :] = t.astype(BF16)
        rows_loop(CX, fn)
        for j in range(1, nd):
            c4(c, j).start()

    def st5(c):
        for j in range(1, nd):
            c4(c, j).wait_recv()
        t = up(L[c, f, mine(c, z), :])
        for j in range(1, nd):
            t = t + up(R4[c, j - 1])
        AX[c, mine(c, z), :] = t.astype(BF16)
        for j in range(1, nd):
            c5(c, j).start()

    def st6(c):
        for j in range(1, nd):
            c5(c, j).wait_recv()
        for j in range(1, nx):
            c6(c, j).start()

    def outc(i, k, slot):
        cc = core if k == 0 else 1 - core
        return pltpu.make_async_copy(ST.at[slot], sl(*orect(i, cc)), so.at[slot])

    def emit(i, k, src):
        slot = emit.n % 4
        if emit.n >= 4:
            outc(*emit.log[emit.n - 4], slot).wait()
        off = i % grp * U

        def fn(r):
            ST[slot, pl.ds(r, B), :] = up(src[i // grp, pl.ds(pl.multiple_of(off + r, B), B), :])
        rows_loop(U, fn)
        outc(i, k, slot).start()
        emit.log.append((i, k))
        emit.n += 1
    emit.n = 0
    emit.log = []

    def st7(c):
        for j in range(1, nx):
            c6(c, j).wait_recv()
        c7(c).start()
        for k in range(grp):
            emit(c * grp + k, 0, AX)

    def st8(c):
        c7(c).wait_recv()
        for k in range(grp):
            emit(c * grp + k, 1, AC)

    def v_core():
        return remote(vec, V0.at[0], vs.at[0], vr.at[0], sib)

    def v_y():
        return remote(V0.at[1], V0.at[2], vs.at[1], vr.at[1], yp)

    def v_x(j):
        return remote(VX.at[x], VX.at[x], vs.at[1 + j], vr.at[1 + j], xps[j - 1])

    def v_z(j):
        return remote(VZ.at[z], VZ.at[z], vs.at[nx + j], vr.at[nx + j], zps[j - 1])

    def vst(k):
        if k == 0:
            v_core().start()
        elif k == 1:
            v_core().wait_recv()
            V0[1] = vec[...] + V0[0]
            v_y().start()
        elif k == 2:
            v_y().wait_recv()
            VX[x] = V0[1] + V0[2]
            for j in range(1, nx):
                v_x(j).start()
        elif k == 3:
            for j in range(1, nx):
                v_x(j).wait_recv()
            t = VX[0]
            for j in range(1, nx):
                t = t + VX[j]
            VZ[z] = t
            for j in range(1, nd):
                v_z(j).start()
        elif k == 4:
            for j in range(1, nd):
                v_z(j).wait_recv()
            t = VZ[0]
            for j in range(1, nd):
                t = t + VZ[j]
            ov[...] = t

    for i in range(12):
        local(i, 0).start()
    pl.semaphore_wait(bar, len(peers))
    for i in range(12):
        c1(i, 0).start()
    vst(0)
    for i in range(12):
        local(i, 1).start()
        c1(i, 1).start()
    stages = [(8, st8), (7, st7), (6, st6), (5, st5), (4, st4), (3, st3)]
    for t in range(nch + 8):
        if t < nch:
            st2(t)
        if 1 <= t <= 4:
            vst(t)
        for k, fn in stages:
            c = t - (k - 1)
            if 0 <= c < nch:
                fn(c)
    n = emit.n
    for q in range(max(0, n - 4), n):
        outc(*emit.log[q], q % 4).wait()
    for i in range(12):
        for k in range(2):
            c1(i, k).wait_send()
    for c in range(nch):
        c2(c).wait_send()
        c7(c).wait_send()
        for j in range(1, nx):
            c3(c, j).wait_send()
            c6(c, j).wait_send()
        for j in range(1, nd):
            c4(c, j).wait_send()
            c5(c, j).wait_send()
    v_core().wait_send()
    v_y().wait_send()
    for j in range(1, nx):
        v_x(j).wait_send()
    for j in range(1, nd):
        v_z(j).wait_send()


def grad_reduce(wd, wu, wo, wq, vec, nx, nd, cid):
    grp = nx * nd // 8
    nch = 12 // grp
    CH, CX, PZ = U * grp, U * grp // nx, U * grp // nx // nd
    anyspec = pl.BlockSpec(memory_space=pl.ANY)
    vspec = pl.BlockSpec(memory_space=pltpu.VMEM)
    D = pltpu.SemaphoreType.DMA
    V = pltpu.VMEM
    sems = [D((12, 2)), D((12, 2)), D((12, 2)), D((nch,)), D((nch,)), D((nch, nx - 1)), D((nch, nx - 1)),
            D((nch, nd - 1)), D((nch, nd - 1)), D((nch, nd - 1)), D((nch, nd - 1)), D((nch, nx - 1)), D((nch, nx - 1)),
            D((nch,)), D((nch,)), D((4,)), D((nx + nd,)), D((nx + nd,))]
    return pl.pallas_call(
        functools.partial(grad_kernel, nx, nd, grp),
        out_shape=(jax.ShapeDtypeStruct((1536, 768), F32), jax.ShapeDtypeStruct((U, 3072), F32),
                   jax.ShapeDtypeStruct((U, 768), F32), jax.ShapeDtypeStruct((U, 2304), F32),
                   jax.ShapeDtypeStruct((VR, U), F32)),
        in_specs=[anyspec] * 4 + [vspec],
        out_specs=(anyspec,) * 4 + (vspec,),
        scratch_shapes=[V((nch, 2, CH, U), BF16), V((nch, 2, CH, U), BF16), V((nch, CH, U), BF16),
                        V((nch, nx - 1, CX, U), BF16), V((nch, nd - 1, PZ, U), BF16),
                        V((nch, CH, U), BF16), V((nch, CH, U), BF16), V((4, U, U), F32),
                        V((3, VR, U), F32), V((nx, VR, U), F32), V((nd, VR, U), F32)] + sems,
        compiler_params=pltpu.CompilerParams(collective_id=cid, has_side_effects=True, vmem_limit_bytes=60 << 20),
        name="grad_reduce",
    )(wd, wu, wo, wq, vec)


HEADS = 12


EPSILON = 1e-12
MASKED = -1e30


def shifted(value, axis, steps):
    count = lax.axis_size(axis)
    pairs = [(source, (source + steps) % count) for source in range(count)]
    return lax.ppermute(value, axis, pairs)


def normalize(values, norm_gain, norm_shift):
    row_mean = jnp.mean(values, -1, keepdims=True)
    centred = values - row_mean
    spread = jnp.mean(centred * centred, -1, keepdims=True)
    return centred * lax.rsqrt(spread + EPSILON) * norm_gain + norm_shift


def gelu_exact(values):
    return jax.nn.gelu(values, approximate=False)


def row_dot(left_op, right_op):
    return jnp.dot(left_op, right_op, preferred_element_type=jnp.float32)


def left_dot(left_op, right_op):
    return lax.dot_general(
        left_op, right_op, (((0,), (0,)), ((), ())), preferred_element_type=jnp.float32
    )


def right_dot(left_op, right_op):
    return lax.dot_general(
        left_op, right_op, (((1,), (1,)), ((), ())), preferred_element_type=jnp.float32
    )


def general_body(
    tokens,
    cotangent,
    lengths,
    w_qkv,
    bias_q,
    bias_v,
    w_out,
    bias_out,
    gain_one,
    shift_one,
    w_up,
    bias_up,
    w_down,
    bias_down,
    gain_two,
    shift_two,
):
    seq_count, block_rows, model_width = tokens.shape
    head_count = HEADS
    head_dim = model_width // head_count
    all_rows = seq_count * block_rows
    score_scale = head_dim ** (-0.5)
    cycle_size = lax.axis_size("ctx")
    cycle_index = lax.axis_index("ctx")
    gathered = (
        lax.all_gather(w_qkv, "fsdp", axis=0, tiled=True),
        lax.all_gather(bias_q, "fsdp", axis=0, tiled=True),
        lax.all_gather(bias_v, "fsdp", axis=0, tiled=True),
        lax.all_gather(w_out, "fsdp", axis=0, tiled=True),
        lax.all_gather(bias_out, "fsdp", axis=0, tiled=True),
        lax.all_gather(gain_one, "fsdp", axis=0, tiled=True),
        lax.all_gather(shift_one, "fsdp", axis=0, tiled=True),
        lax.all_gather(w_up, "fsdp", axis=0, tiled=True),
        lax.all_gather(bias_up, "fsdp", axis=0, tiled=True),
        lax.all_gather(w_down, "fsdp", axis=0, tiled=True),
        lax.all_gather(bias_down, "fsdp", axis=0, tiled=True),
        lax.all_gather(gain_two, "fsdp", axis=0, tiled=True),
        lax.all_gather(shift_two, "fsdp", axis=0, tiled=True),
    )
    full_qkv, full_out, full_up, full_down = (gathered[0], gathered[3], gathered[7], gathered[9])
    add_q, add_v, add_out, scale_one, move_one, add_up, add_down, scale_two, move_two = [
        gathered[place].astype(jnp.float32) for place in (1, 2, 4, 5, 6, 8, 10, 11, 12)
    ]
    flat_tokens = tokens.reshape(all_rows, model_width)
    projected = row_dot(flat_tokens, full_qkv)
    queries = (
        (projected[:, :model_width] + add_q)
        .astype(jnp.bfloat16)
        .reshape(seq_count, block_rows, head_count, head_dim)
    )
    key_rows = (
        projected[:, model_width : 2 * model_width]
        .astype(jnp.bfloat16)
        .reshape(seq_count, block_rows, model_width)
    )
    value_rows = (
        (projected[:, 2 * model_width :] + add_v)
        .astype(jnp.bfloat16)
        .reshape(seq_count, block_rows, model_width)
    )
    start_state = (
        jnp.full((seq_count, block_rows, head_count), MASKED, jnp.float32),
        jnp.zeros((seq_count, block_rows, head_count), jnp.float32),
        jnp.zeros((seq_count, block_rows, head_count, head_dim), jnp.float32),
    )
    key_part = lax.all_gather(key_rows, "ctx", axis=1, tiled=True)
    value_part = lax.all_gather(value_rows, "ctx", axis=1, tiled=True)
    key_count = key_part.shape[1]
    sub_rows = math.gcd(key_count, 512)

    def visit(block_index, carried):
        first_key = block_index * sub_rows
        key_block = lax.dynamic_slice_in_dim(key_part, block_index * sub_rows, sub_rows, 1).reshape(
            seq_count, sub_rows, head_count, head_dim
        )
        value_block = lax.dynamic_slice_in_dim(
            value_part, block_index * sub_rows, sub_rows, 1
        ).reshape(seq_count, sub_rows, head_count, head_dim)
        peak, weight_sum, weighted = carried
        key_live = (
            (first_key + jnp.arange(sub_rows, dtype=jnp.int32))[None, :] < lengths[:, None]
        )[:, None, None, :]
        scores = (
            jnp.einsum("sqhe,skhe->sqhk", queries, key_block, preferred_element_type=jnp.float32)
            * score_scale
        )
        scores = jnp.where(key_live, scores, MASKED)
        new_peak = jnp.maximum(peak, jnp.max(scores, -1))
        factor = jnp.exp(peak - new_peak)
        weights = jnp.where(key_live, jnp.exp(scores - new_peak[..., None]), 0.0)
        mixed_values = jnp.einsum(
            "sqhk,skhe->sqhe",
            weights.astype(jnp.bfloat16),
            value_block,
            preferred_element_type=jnp.float32,
        )
        return (
            new_peak,
            weight_sum * factor + jnp.sum(weights, -1),
            weighted * factor[..., None] + mixed_values,
        )

    peak, weight_sum, weighted = lax.fori_loop(0, key_count // sub_rows, visit, start_state)
    log_total = peak + jnp.log(weight_sum)
    attended = weighted / weight_sum[..., None]
    attended_low = attended.astype(jnp.bfloat16).reshape(all_rows, model_width)
    first_sum = flat_tokens.astype(jnp.float32) + row_dot(attended_low, full_out) + add_out
    normed, norm_pull = jax.vjp(normalize, first_sum, scale_one, move_one)
    normed_low = normed.astype(jnp.bfloat16)
    hidden_pre = row_dot(normed_low, full_up) + add_up
    hidden_act, gelu_pull = jax.vjp(gelu_exact, hidden_pre)
    hidden_low = hidden_act.astype(jnp.bfloat16)
    second_sum = normed + row_dot(hidden_low, full_down) + add_down
    result, result_pull = jax.vjp(normalize, second_sum, scale_two, move_two)
    grad_second, grad_gain_two, grad_shift_two = result_pull(
        cotangent.reshape(all_rows, model_width).astype(jnp.float32)
    )
    down_low = grad_second.astype(jnp.bfloat16)
    grad_w_down = left_dot(hidden_low, down_low)
    grad_bias_down = jnp.sum(down_low.astype(jnp.float32), 0)
    (grad_pre,) = gelu_pull(right_dot(down_low, full_down))
    up_low = grad_pre.astype(jnp.bfloat16)
    grad_w_up = left_dot(normed_low, up_low)
    grad_bias_up = jnp.sum(up_low.astype(jnp.float32), 0)
    grad_first, grad_gain_one, grad_shift_one = norm_pull(grad_second + right_dot(up_low, full_up))
    branch_low = grad_first.astype(jnp.bfloat16)
    grad_w_out = left_dot(attended_low, branch_low)
    grad_bias_out = jnp.sum(branch_low.astype(jnp.float32), 0)
    grad_att = (
        right_dot(branch_low, full_out)
        .astype(jnp.bfloat16)
        .reshape(seq_count, block_rows, head_count, head_dim)
    )
    delta_rows = jnp.sum(grad_att.astype(jnp.float32) * attended, -1)

    def block_grads(query_part, grad_part, lse_part, delta_part, key_block, value_block, first_key):
        key_count = key_block.shape[1]
        key_heads = key_block.reshape(seq_count, key_count, head_count, head_dim)
        value_heads = value_block.reshape(seq_count, key_count, head_count, head_dim)
        key_live = (
            (first_key + jnp.arange(key_count, dtype=jnp.int32))[None, :] < lengths[:, None]
        )[:, None, None, :]
        scores = (
            jnp.einsum("sqhe,skhe->sqhk", query_part, key_heads, preferred_element_type=jnp.float32)
            * score_scale
        )
        chances = jnp.where(key_live, jnp.exp(scores - lse_part[..., None]), 0.0)
        grad_value = jnp.einsum(
            "sqhk,sqhe->skhe",
            chances.astype(jnp.bfloat16),
            grad_part,
            preferred_element_type=jnp.float32,
        )
        grad_chance = jnp.einsum(
            "sqhe,skhe->sqhk", grad_part, value_heads, preferred_element_type=jnp.float32
        )
        grad_score = (chances * (grad_chance - delta_part[..., None])).astype(jnp.bfloat16)
        grad_query = (
            jnp.einsum("sqhk,skhe->sqhe", grad_score, key_heads, preferred_element_type=jnp.float32)
            * score_scale
        )
        grad_key = (
            jnp.einsum(
                "sqhk,sqhe->skhe", grad_score, query_part, preferred_element_type=jnp.float32
            )
            * score_scale
        )
        return (
            grad_query,
            grad_key.reshape(seq_count, key_count, model_width),
            grad_value.reshape(seq_count, key_count, model_width),
        )

    query_start = jnp.zeros((seq_count, block_rows, head_count, head_dim), jnp.float32)

    def key_terms(key_block, value_block, first_key):
        return block_grads(
            queries, grad_att, log_total, delta_rows, key_block, value_block, first_key
        )

    def block_terms(key_block, value_block, first_key):
        return key_terms(key_block, value_block, first_key)

    def turn(step_index, carried):
        key_now, value_now, key_grads, query_acc = carried
        first_key = (cycle_index - step_index) % cycle_size * block_rows
        add_query, add_key, add_value = block_terms(key_now, value_now, first_key)
        key_now, value_now = shifted((key_now, value_now), "ctx", 1)
        key_grads = (
            shifted((key_grads[0] + add_key).astype(jnp.bfloat16), "ctx", 1).astype(jnp.float32),
            shifted((key_grads[1] + add_value).astype(jnp.bfloat16), "ctx", 1).astype(jnp.float32),
        )
        return (key_now, value_now, key_grads, query_acc + add_query)

    grad_start = (
        jnp.zeros((seq_count, block_rows, model_width), jnp.float32),
        jnp.zeros((seq_count, block_rows, model_width), jnp.float32),
    )
    key_final, value_final, key_grads, query_grad = lax.fori_loop(
        0, cycle_size, turn, (key_rows, value_rows, grad_start, query_start)
    )
    grad_key, grad_value = key_grads
    qkv_grad = jnp.concatenate(
        [
            query_grad.astype(jnp.bfloat16).reshape(all_rows, model_width),
            grad_key.astype(jnp.bfloat16).reshape(all_rows, model_width),
            grad_value.astype(jnp.bfloat16).reshape(all_rows, model_width),
        ],
        1,
    )
    grad_w_qkv = left_dot(flat_tokens, qkv_grad)
    grad_bias_q = jnp.sum(qkv_grad[:, :model_width].astype(jnp.float32), 0)
    grad_bias_v = jnp.sum(qkv_grad[:, 2 * model_width :].astype(jnp.float32), 0)
    grad_input = grad_first + right_dot(qkv_grad, full_qkv)
    vectors = (
        grad_bias_q,
        grad_bias_v,
        grad_bias_out,
        grad_gain_one,
        grad_shift_one,
        grad_bias_up,
        grad_bias_down,
        grad_gain_two,
        grad_shift_two,
    )
    packed = jnp.concatenate(vectors).reshape(VR, U)
    t_down, t_up, t_out, t_qkv, t_vec = grad_reduce(
        grad_w_down.astype(BF16),
        grad_w_up.astype(BF16),
        grad_w_out.astype(BF16),
        grad_w_qkv.astype(BF16),
        packed,
        cycle_size // 2,
        lax.axis_size("dp"),
        1,
    )
    flat = t_vec.reshape(-1)
    own = lax.axis_index("fsdp")
    parts, start = [], 0
    for vector in vectors:
        half = vector.shape[0] // 2
        parts.append(lax.dynamic_slice_in_dim(flat, start + own * half, half, 0))
        start += 2 * half
    totals = (
        t_qkv, parts[0], parts[1], t_out, parts[2], parts[3], parts[4],
        t_up, parts[5], t_down, parts[6], parts[7], parts[8],
    )
    output_rows = result.astype(jnp.bfloat16).reshape(seq_count, block_rows, model_width)
    input_rows = grad_input.astype(jnp.bfloat16).reshape(seq_count, block_rows, model_width)
    return (
        output_rows,
        input_rows,
        totals[0],
        totals[1],
        totals[2],
        totals[3],
        totals[4],
        totals[5],
        totals[6],
        totals[7],
        totals[8],
        totals[9],
        totals[10],
        totals[11],
        totals[12],
    )


HW = 64
QT = 256


def remote(src, dst, ss, rs, dev):
    return pltpu.make_async_remote_copy(src_ref=src, dst_ref=dst, send_sem=ss, recv_sem=rs, device_id=dev, device_id_type=MESH)


def nt(a, b):
    return lax.dot_general(a, b, (((1,), (1,)), ((), ())), preferred_element_type=F32)


def mm(a, b):
    return jnp.dot(a, b, preferred_element_type=F32)


def head_masks(rows):
    lane = lax.broadcasted_iota(jnp.int32, (rows, 2 * HW), 1)
    return lane < HW


def normal_parts(v):
    mean = jnp.mean(v, -1, keepdims=True)
    cen = v - mean
    inv = lax.rsqrt(jnp.mean(cen * cen, -1, keepdims=True) + EPSILON)
    return cen * inv, inv


def normal_back(dn, hat, inv, gain):
    d = dn * gain
    return inv * (d - jnp.mean(d, -1, keepdims=True) - hat * jnp.mean(d * hat, -1, keepdims=True))


def gelu_pair(u):
    w = jnp.abs(u)
    t = 1.0 / (1.0 + (0.3275911 * math.sqrt(0.5)) * w)
    e = jnp.exp(-0.5 * u * u)
    poly = t * (0.127414796 + t * (-0.142248368 + t * (0.7107068705 + t * (-0.7265760135 + t * 0.5307027145))))
    tail = poly * e
    phi = jnp.where(u < 0.0, tail, 1.0 - tail)
    return u * phi, phi + u * (e * (1.0 / math.sqrt(2.0 * math.pi)))


def fold8(v):
    return jnp.sum(v.reshape(v.shape[0] // 8, 8, v.shape[1]), 0)


def fwd_kernel(nx, seqs, seq_rows, lens, tok, cot, sq, so_, su, sd, *rest):
    small = rest[:9]
    (qkv_o, att_o, lse_o, wq_o, wo_o, wu_o, wd_o, vec_o, y_o, dh_o, hat_o, act_o, gp_o, vg_o) = rest[9:23]
    (XT, WB, QKV, CT, ATT, LSE, H1, N1, N1B, ACT, GP, YB,
               ls, ys, yr, zs, zr, as_, ar, bs, br, t0s, t0r, t1s, t1r, t2s, t2r, vs, vr, lts, outs) = rest[23:]
    core, x, f, z = places()
    me = x * 2 + core
    nblk = 2 * nx
    rows = seqs * seq_rows
    sib = {"ctx": x * 2 + 1 - core}
    yp = {"fsdp": 1 - f}
    zp = {"dp": z + 1 - 2 * lax.rem(z, 2)}
    zb = lax.rem(z, 2)
    xts = [lax.rem(x + j, nx) for j in range(1, nx)]
    xps = [{"ctx": t * 2 + core} for t in xts]
    xsrc = [lax.rem(x + nx - j, nx) * 2 + core for j in range(1, nx)]
    peers = [sib, yp, zp] + xps
    bar = pltpu.get_barrier_semaphore()
    for p in peers:
        pl.semaphore_signal(bar, inc=1, device_id=p, device_id_type=MESH)
    order = (1, 2, 0)
    PR = U // 4
    piece = pl.multiple_of((zb * 2 + core) * PR, PR)
    zpiece = pl.multiple_of(((1 - zb) * 2 + core) * PR, PR)
    H = rows // 2

    def shard(b, r0, n):
        r = pl.ds(r0, n)
        if b < 3:
            return sq.at[r, pl.ds(b * 768, 768)]
        if b == 3:
            return so_.at[r, :]
        if b < 8:
            return su.at[r, pl.ds((b - 4) * 768, 768)]
        return sd.at[pl.ds((b - 8) * U + r0, n), :]

    def loc(b):
        return pltpu.make_async_copy(shard(b, 0, U), WB.at[b, f], ls.at[b])

    def ycp(b):
        if not isinstance(b, int):
            src = WB.at[b, f, pl.ds(piece, PR)]
        else:
            src = shard(b, piece, PR)
        return remote(src, WB.at[b, f, pl.ds(piece, PR)], ys.at[b], yr.at[b], yp)

    def zcp(b):
        w = WB.at[b, 1 - f, pl.ds(piece, PR)]
        return remote(w, w, zs.at[b], zr.at[b], zp)

    def acp(b):
        w = WB.at[b, 1 - f, pl.ds(piece, PR)]
        return remote(w, w, as_.at[b], ar.at[b], sib)

    def bcp(b):
        w = WB.at[b, 1 - f, pl.ds(zpiece, PR)]
        return remote(w, w, bs.at[b], br.at[b], sib)

    def A(b):
        ycp(b).wait_recv()
        zcp(b).start()
        acp(b).start()

    def B(b):
        zcp(b).wait_recv()
        bcp(b).start()

    def C(b):
        acp(b).wait_recv()
        bcp(b).wait_recv()

    def tsl(h):
        return pl.ds(h * H, H)

    def t_sib(h):
        return remote(tok.at[tsl(h)], XT.at[me, tsl(h)], t0s.at[h], t0r.at[h], sib)

    def t_x(j, h):
        return remote(tok.at[tsl(h)], XT.at[me, tsl(h)], t1s.at[j - 1, h], t1r.at[j - 1, h], xps[j - 1])

    def t_f(j, h):
        w = XT.at[xsrc[j - 1], tsl(h)]
        return remote(w, w, t2s.at[j - 1, h], t2r.at[j - 1, h], sib)

    vcp = remote(vec_o.at[f], vec_o.at[f], vs.at[0], vr.at[0], yp)
    tl = pltpu.make_async_copy(tok, XT.at[me], lts.at[0])
    tl.start()
    for b in order:
        loc(b).start()
    row = 0
    for v in small:
        w = v[...].astype(F32).reshape(1, -1)
        for i in range(v.shape[0] // U):
            vec_o[f, row:row + 1, :] = w[:, i * U:(i + 1) * U]
            row += 1
    tc = pltpu.make_async_copy(cot, CT, lts.at[1])
    pl.semaphore_wait(bar, len(peers))
    vcp.start()
    for b in order:
        ycp(b).start()
    for h in range(2):
        for j in range(1, nx):
            t_x(j, h).start()
        t_sib(h).start()
    for b in range(3, 12):
        ycp(b).start()
    for b in range(3, 12):
        loc(b).start()
    tc.start()
    tl.wait()

    def qkv(b, blk):
        fac = 0.125 if b == 0 else 1.0

        def one(t, _):
            c = pl.ds(pl.multiple_of(t * 256, 256), 256)
            w = WB[b, :, :, c].reshape(768, 256)
            QKV[b, blk, :, c] = mm(XT[blk], w).astype(BF16)
            return 0
        if b == 1:
            lax.fori_loop(0, 3, one, 0)
        else:
            row = 0 if b == 0 else 1
            for t in range(3):
                w = WB[b, :, :, t * 256:(t + 1) * 256].reshape(768, 256)
                if t == 0:
                    bias = vec_o[0, row:row + 1, 0:256]
                elif t == 1:
                    bias = jnp.concatenate([vec_o[0, row:row + 1, 256:384], vec_o[1, row:row + 1, 0:128]], 1)
                else:
                    bias = vec_o[1, row:row + 1, 128:384]
                r = (mm(XT[blk], w) + bias).astype(BF16)
                if b == 0:
                    r = r * jnp.asarray(fac, BF16)
                QKV[b, blk, :, t * 256:(t + 1) * 256] = r

    seq = list(order)
    A(seq[0])
    A(seq[1])
    B(seq[0])
    for h in range(2):
        t_sib(h).wait_recv()
    A(seq[2])
    B(seq[1])
    vcp.wait_recv()
    for n, b in enumerate(seq):
        loc(b).wait()
        C(b)

        def both(i, _):
            qkv(b, x * 2 + i)
            return 0
        lax.fori_loop(0, 2, both, 0)
        if n == 0:
            B(seq[2])
            A(3)
        if n == 1:
            B(3)
            A(4)
    for j in range(1, nx):
        for h in range(2):
            t_x(j, h).wait_recv()
            t_f(j, h).start()
    B(4)
    A(5)
    for j in range(1, nx):
        for h in range(2):
            t_f(j, h).wait_recv()
        base = lax.rem(x + nx - j, nx) * 2

        def pair(i, _):
            for b in seq:
                qkv(b, base + i)
            return 0
        lax.fori_loop(0, 2, pair, 0)
    B(5)
    qo = pltpu.make_async_copy(QKV, qkv_o, outs.at[0])
    qo.start()

    low_half = head_masks(QT)
    lane128 = lax.broadcasted_iota(jnp.int32, (QT, 128), 1)
    kpos = lax.broadcasted_iota(jnp.int32, (QT, QT), 1)
    nr = seq_rows // QT

    def attend(tile, j):
        s0 = tile // nr
        qr = pl.ds(pl.multiple_of(tile * QT, QT), QT)
        cols = pl.ds(pl.multiple_of(j * 128, 128), 128)
        q = QKV[0, me, qr, cols]
        length = lens[s0]
        outs_ = []
        tot = LSE[qr, 0:128]
        for h in range(2):
            qh = jnp.where(low_half == (h == 0), q, jnp.zeros_like(q))
            sc = []
            mx = None
            for blk in range(nblk):
                for r in range(nr):
                    kr = pl.ds(pl.multiple_of(s0 * seq_rows + r * QT, QT), QT)
                    v = nt(qh, QKV[1, blk, kr, cols])
                    v = jnp.where(kpos < length - (blk * seq_rows + r * QT), v, MASKED)
                    sc.append(v)
                    mx = v if mx is None else jnp.maximum(mx, v)
            m = jnp.max(mx, 1, keepdims=True)
            acc = None
            lsum = None
            i = 0
            for blk in range(nblk):
                for r in range(nr):
                    kr = pl.ds(pl.multiple_of(s0 * seq_rows + r * QT, QT), QT)
                    p = jnp.exp(sc[i] - m)
                    i += 1
                    lsum = p if lsum is None else lsum + p
                    o = mm(p.astype(BF16), QKV[2, blk, kr, cols])
                    acc = o if acc is None else acc + o
            den = jnp.sum(lsum, 1, keepdims=True)
            outs_.append(acc / den)
            tot = jnp.where(lane128 == 2 * j + h, m + jnp.log(den), tot)
        ATT[qr, cols] = jnp.where(low_half, outs_[0], outs_[1])
        LSE[qr, 0:128] = tot

    ntile = rows // QT
    per = ntile * 6 // 4

    def group(g, _):
        A(6 + g)

        def one(i, _):
            it = g * per + i
            attend(it // 6, lax.rem(it, 6))
            return 0
        lax.fori_loop(0, per, one, 0)
        B(6 + g)
        return 0
    lax.fori_loop(0, 4, group, 0)
    A(10)
    extra = []

    def send_out(src, dst):
        cp = pltpu.make_async_copy(src, dst, outs.at[25 + len(extra)])
        cp.start()
        extra.append(cp)

    def full(b):
        res = []
        for ff in range(2):
            src = WB.at[b, ff]
            if b < 3:
                dst = wq_o.at[pl.ds(ff * U, U), pl.ds(b * 768, 768)]
            elif b == 3:
                dst = wo_o.at[pl.ds(ff * U, U), :]
            elif b < 8:
                dst = wu_o.at[pl.ds(ff * U, U), pl.ds((b - 4) * 768, 768)]
            else:
                dst = wd_o.at[pl.ds(ff * 1536 + (b - 8) * U, U), :]
            res.append(pltpu.make_async_copy(src, dst, outs.at[1 + 2 * b + ff]))
        return res

    def ready(b):
        loc(b).wait()
        C(b)
        for cp in full(b):
            cp.start()

    def vector(r):
        return jnp.concatenate([vec_o[0, r:r + 1, :], vec_o[1, r:r + 1, :]], 1)

    for b in range(3):
        for cp in full(b):
            cp.start()
    send_out(ATT, att_o)
    ready(3)
    bo = vector(2)
    for t in range(3):
        cs = slice(t * 256, (t + 1) * 256)
        w = WB[3, :, :, cs].reshape(768, 256)
        H1[:, cs] = XT[me, :, cs].astype(F32) + mm(ATT[...].astype(BF16), w) + bo[:, cs]
    g1, s1 = vector(3), vector(4)
    RB = 64

    def ln1(i, _):
        r = pl.ds(pl.multiple_of(i * RB, RB), RB)
        hat, inv = normal_parts(H1[r, :])
        H1[r, :] = hat
        n = hat * g1 + s1
        N1[r, :] = n
        N1B[r, :] = n.astype(BF16)
        LSE[r, 128:256] = jnp.broadcast_to(inv, (RB, 128))
        return 0
    lax.fori_loop(0, rows // RB, ln1, 0)
    send_out(H1, hat_o)
    send_out(LSE, lse_o)
    A(11)
    B(10)
    for b in range(4, 8):
        ready(b)

    def upblock(b, _):
        bias = jnp.concatenate([vec_o[b // 2, pl.ds(5 + lax.rem(b, 2) * 2, 1), :], vec_o[b // 2, pl.ds(6 + lax.rem(b, 2) * 2, 1), :]], 1)
        for t in range(3):
            w = WB[4 + b, :, :, t * 256:(t + 1) * 256].reshape(768, 256)
            cs = pl.ds(pl.multiple_of(b * 768 + t * 256, 256), 256)
            act, gp = gelu_pair(mm(N1B[...], w) + bias[:, t * 256:(t + 1) * 256])
            ACT[:, cs] = act.astype(BF16)
            GP[:, cs] = gp
        return 0
    lax.fori_loop(0, 2, upblock, 0)
    B(11)
    lax.fori_loop(2, 4, upblock, 0)
    send_out(ACT, act_o)
    send_out(GP, gp_o)
    for b in range(8, 12):
        ready(b)
    bd = vector(9)
    for t in range(3):
        cs = slice(t * 256, (t + 1) * 256)
        acc = N1[:, cs] + bd[:, cs]
        for ff in range(2):
            acc = acc + mm(ACT[:, ff * 1536:(ff + 1) * 1536], WB[8:12, ff, :, cs].reshape(1536, 256))
        N1[:, cs] = acc
    g2, s2 = vector(10), vector(11)
    tc.wait()

    def ln2(i, carry):
        r = pl.ds(pl.multiple_of(i * RB, RB), RB)
        hat, inv = normal_parts(N1[r, :])
        YB[r, :] = (hat * g2 + s2).astype(BF16)
        g = CT[r, :].astype(F32)
        N1[r, :] = normal_back(g, hat, inv, g2)
        return carry[0] + fold8(g * hat), carry[1] + fold8(g)
    zero = jnp.zeros((8, 768), F32)
    a0, a1 = lax.fori_loop(0, rows // RB, ln2, (zero, zero))
    send_out(YB, y_o)
    send_out(N1, dh_o)
    vg_o[0:1, :] = jnp.sum(a0, 0, keepdims=True)
    vg_o[1:2, :] = jnp.sum(a1, 0, keepdims=True)
    vcp.wait_send()
    qo.wait()
    for b in range(12):
        ycp(b).wait_send()
        zcp(b).wait_send()
        acp(b).wait_send()
        bcp(b).wait_send()
        for cp in full(b):
            cp.wait()
    for h in range(2):
        t_sib(h).wait_send()
        for j in range(1, nx):
            t_x(j, h).wait_send()
            t_f(j, h).wait_send()
    for cp in extra:
        cp.wait()


def forward_gather(lens, tok, cot, sq, so_, su, sd, small, nx, cid):
    seqs, seq_rows, d = tok.shape
    rows = seqs * seq_rows
    nblk = 2 * nx
    anyspec = pl.BlockSpec(memory_space=pl.ANY)
    vspec = pl.BlockSpec(memory_space=pltpu.VMEM)
    sspec = pl.BlockSpec(memory_space=pltpu.SMEM)
    D = pltpu.SemaphoreType.DMA
    V = pltpu.VMEM
    S = jax.ShapeDtypeStruct
    sems = [D((12,))] * 9 + [D((2,)), D((2,))] + [D((nx - 1, 2))] * 4 + [D((1,)), D((1,)), D((2,)), D((33,))]
    return pl.pallas_call(
        functools.partial(fwd_kernel, nx, seqs, seq_rows),
        out_shape=(S((3, nblk, rows, d), BF16), S((rows, d), F32), S((rows, 256), F32),
                   S((768, 2304), BF16), S((768, 768), BF16), S((768, 3072), BF16), S((3072, 768), BF16),
                   S((2, 12, U), F32), S((rows, d), BF16), S((rows, d), F32), S((rows, d), F32),
                   S((rows, 3072), BF16), S((rows, 3072), F32), S((2, d), F32)),
        in_specs=[sspec] + [anyspec] * 6 + [vspec] * 9,
        out_specs=(anyspec,) * 7 + (vspec,) + (anyspec,) * 5 + (vspec,),
        scratch_shapes=[V((nblk, rows, d), BF16), V((12, 2, U, 768), BF16), V((3, nblk, rows, d), BF16),
                        V((rows, d), BF16), V((rows, d), F32), V((rows, 256), F32), V((rows, d), F32), V((rows, d), F32),
                        V((rows, d), BF16), V((rows, 3072), BF16), V((rows, 3072), F32), V((rows, d), BF16)] + sems,
        compiler_params=pltpu.CompilerParams(collective_id=cid, has_side_effects=True, vmem_limit_bytes=62 << 20),
        name="forward_gather",
    )(lens, tok.reshape(rows, d), cot.reshape(rows, d), sq, so_, su, sd, *small)


def tn(a, b):
    return lax.dot_general(a, b, (((0,), (0,)), ((), ())), preferred_element_type=F32)


def colsum(v):
    return jnp.sum(fold8(v), 0, keepdims=True)


def bwd_kernel(nx, nd, seqs, seq_rows, lens, vec, vg, qkv_i, att_i, lse_i, wq_i, wo_i, wu_i, wd_i, dh_i, hat_i, act_i, gp_i, tok_i,
               od, ou, oo, oq, ov, gin_o,
               BIG, WO, WQ, GP, ACT, DH, DM, HAT, NB, DO, ROWS, COLS, DQKV, L, SB, R1, R2, R3, R4, AX, VV, V0, VX, VZ,
               lds, d0s, d0r, d1s, d1r, d2s, d2r, s1s, s1r, s2s, s2r, s3s, s3r, s4s, s4r, s5s, s5r, s6s, s6r, s7s, s7r, s8, vs, vr):
    core, x, f, z = places()
    me = x * 2 + core
    nblk = 2 * nx
    rows = seqs * seq_rows
    CX, PZ = U // nx, U // nx // nd
    NCH, READY = 12, 8
    sib = {"ctx": x * 2 + 1 - core}
    yp = {"fsdp": 1 - f}
    xps = [{"ctx": lax.rem(x + j, nx) * 2 + core} for j in range(1, nx)]
    xsrc = [lax.rem(x + nx - j, nx) * 2 + core for j in range(1, nx)]
    zps = [{"dp": lax.rem(z + j, nd)} for j in range(1, nd)]
    peers = [sib, yp] + xps + zps
    bar = pltpu.get_barrier_semaphore()
    for p in peers:
        pl.semaphore_signal(bar, inc=1, device_id=p, device_id_type=MESH)

    loads = {}

    def load(name, src, dst):
        cp = pltpu.make_async_copy(src, dst, lds.at[len(loads)])
        cp.start()
        loads[name] = cp

    load("dh", dh_i, DH)
    load("act", act_i, ACT)
    load("wd", wd_i, BIG.at[pl.ds(0, 3072)])
    load("gp0", gp_i.at[:, pl.ds(0, 768)], GP.at[0])
    load("hat", hat_i, HAT)
    load("gp1", gp_i.at[:, pl.ds(768, 768)], GP.at[1])
    for b in range(4):
        load(("wu", b), wu_i.at[:, pl.ds(b * 768, 768)], BIG.at[pl.ds(3072 + b * 768, 768)])
    load("lse", lse_i, COLS.at[:, pl.ds(0, 256)])
    load("wo", wo_i, WO)
    for b in range(3):
        load(("wq", b), wq_i.at[:, pl.ds(b * 768, 768)], WQ.at[b])

    def vector(r):
        return jnp.concatenate([vec[0, r:r + 1, :], vec[1, r:r + 1, :]], 1)

    def c1(i, ff, k):
        return remote(SB.at[i % 4, ff], R1.at[i, ff], s1s.at[i, k], s1r.at[i, k], sib)

    def c1s(i):
        return [c1(i, 1 - f, 0), c1(i, f, 1)]

    def c2(c):
        return remote(L.at[c, 1 - f], R2.at[c], s2s.at[c], s2r.at[c], yp)

    def c3(c, j):
        xt = lax.rem(x + j, nx)
        return remote(L.at[c, f, pl.ds(pl.multiple_of(xt * CX, CX), CX)], R3.at[c, j - 1], s3s.at[c, j - 1], s3r.at[c, j - 1], xps[j - 1])

    def mine(zz):
        return pl.ds(pl.multiple_of(x * CX + zz * PZ, PZ), PZ)

    def c4(c, j):
        zt = lax.rem(z + j, nd)
        return remote(L.at[c, f, mine(zt)], R4.at[c, j - 1], s4s.at[c, j - 1], s4r.at[c, j - 1], zps[j - 1])

    def c5(c, j):
        w = AX.at[c, mine(z)]
        return remote(w, w, s5s.at[c, j - 1], s5r.at[c, j - 1], zps[j - 1])

    def c6(c, j):
        w = AX.at[c, pl.ds(pl.multiple_of(x * CX, CX), CX)]
        return remote(w, w, s6s.at[c, j - 1], s6r.at[c, j - 1], xps[j - 1])

    def orect(i):
        if i < 4:
            return od.at[pl.ds(pl.multiple_of(core * 768 + i // 2 * U, U), U), pl.ds(i % 2 * U, U)]
        if i < 8:
            return ou.at[:, pl.ds(pl.multiple_of(core * 1536 + (i - 4) * U, 128), U)]
        if i < 9:
            return oo.at[:, pl.ds(pl.multiple_of(core * U, 128), U)]
        return oq.at[:, pl.ds(pl.multiple_of(core * 1152 + (i - 9) * U, 128), U)]

    def c7(c):
        return remote(AX.at[c], orect(c), s7s.at[c], s7r.at[c], sib)

    def c8(c):
        return pltpu.make_async_copy(AX.at[c], orect(c), s8.at[c])

    B = 48

    def rows_loop(n, fn):
        def bodyf(i, _):
            fn(pl.multiple_of(i * B, B))
            return 0
        lax.fori_loop(0, n // B, bodyf, 0)

    def up(v):
        return v.astype(F32)

    def st1(i):
        for cp in c1s(i):
            cp.start()

    def st2(c):
        c1(c, 1 - f, 0).wait_recv()

        def fn(r):
            s = pl.ds(r, B)
            L[c, 1 - f, s, :] = (up(L[c, 1 - f, s, :]) + up(R1[c, 1 - f, s, :])).astype(BF16)
        rows_loop(U, fn)
        c2(c).start()

    def st3(c):
        c1(c, f, 1).wait_recv()
        c2(c).wait_recv()
        for j in range(1, nx):
            xt = lax.rem(x + j, nx)

            def fn(r):
                s = pl.ds(pl.multiple_of(xt * CX + r, B), B)
                L[c, f, s, :] = (up(L[c, f, s, :]) + up(R1[c, f, s, :]) + up(R2[c, s, :])).astype(BF16)
            rows_loop(CX, fn)
            c3(c, j).start()

    def st4(c):
        for j in range(1, nx):
            c3(c, j).wait_recv()

        def fn(r):
            s = pl.ds(pl.multiple_of(x * CX + r, B), B)
            t = up(L[c, f, s, :]) + up(R1[c, f, s, :]) + up(R2[c, s, :])
            for j in range(1, nx):
                t = t + up(R3[c, j - 1, pl.ds(r, B), :])
            L[c, f, s, :] = t.astype(BF16)
        rows_loop(CX, fn)
        for j in range(1, nd):
            c4(c, j).start()

    def st5(c):
        for j in range(1, nd):
            c4(c, j).wait_recv()
        t = up(L[c, f, mine(z), :])
        for j in range(1, nd):
            t = t + up(R4[c, j - 1])
        AX[c, mine(z), :] = t.astype(BF16)
        for j in range(1, nd):
            c5(c, j).start()

    def st6(c):
        for j in range(1, nd):
            c5(c, j).wait_recv()
        for j in range(1, nx):
            c6(c, j).start()

    def st7(c):
        for j in range(1, nx):
            c6(c, j).wait_recv()
        c7(c).start()
        c8(c).start()

    def tick(c):
        for lag, fn in ((7, st6), (6, st5), (4, st4), (0, st3)):
            @pl.when(jnp.logical_and(c >= lag, c - lag <= READY))
            def _(lag=lag, fn=fn):
                fn(c - lag)

    def v_core():
        return remote(VV, V0.at[0], vs.at[0], vr.at[0], sib)

    def v_y():
        return remote(V0.at[1], V0.at[2], vs.at[1], vr.at[1], yp)

    def v_x(j):
        return remote(VX.at[x], VX.at[x], vs.at[1 + j], vr.at[1 + j], xps[j - 1])

    def v_z(j):
        return remote(VZ.at[z], VZ.at[z], vs.at[nx + j], vr.at[nx + j], zps[j - 1])

    def vst(k):
        if k == 0:
            v_core().start()
        elif k == 1:
            v_core().wait_recv()
            V0[1] = VV[...] + V0[0]
            v_y().start()
        elif k == 2:
            v_y().wait_recv()
            VX[x] = V0[1] + V0[2]
            for j in range(1, nx):
                v_x(j).start()
        elif k == 3:
            for j in range(1, nx):
                v_x(j).wait_recv()
            t = VX[0]
            for j in range(1, nx):
                t = t + VX[j]
            VZ[z] = t
            for j in range(1, nd):
                v_z(j).start()
        elif k == 4:
            for j in range(1, nd):
                v_z(j).wait_recv()
            t = VZ[0]
            for j in range(1, nd):
                t = t + VZ[j]
            VV2 = t
            for r, n, o in ((0, 1, 0), (2, 1, 1), (4, 1, 2), (6, 1, 3), (8, 1, 4), (10, 4, 5), (18, 1, 9), (20, 1, 10), (22, 1, 11)):
                ov[o:o + n, :] = jnp.where(f == 0, VV2[r:r + n, :], VV2[r + n:r + 2 * n, :])

    def put_vec(r, v):
        VV[r:r + 1, :] = v[:, :U]
        VV[r + 1:r + 2, :] = v[:, U:]

    put_vec(20, vg[0:1, :])
    put_vec(22, vg[1:2, :])

    RB = 64
    loads["dh"].wait()

    def to_dm(i, acc):
        r = pl.ds(pl.multiple_of(i * RB, RB), RB)
        v = DH[r, :].astype(BF16)
        DM[r, :] = v
        return acc + fold8(v.astype(F32))
    zero = jnp.zeros((8, 768), F32)
    put_vec(18, jnp.sum(lax.fori_loop(0, rows // RB, to_dm, zero), 0, keepdims=True))
    loads["act"].wait()

    def fill(i0, kk, ff, val, wide):
        v = val.astype(BF16)
        for t in range(wide):
            if kk == 0:
                L[i0 + t, ff] = v[:, t * U:(t + 1) * U]
            else:
                SB[(i0 + t) % 4, ff] = v[:, t * U:(t + 1) * U]

    def each_f(fn):
        def one(k, _):
            fn(jnp.where(k == 0, 1 - f, f))
            return 0
        lax.fori_loop(0, 2, one, 0)

    def ccof(kk):
        return core if kk == 0 else 1 - core

    for ii in range(2):
        for kk in (1, 0):
            def wdown(ff, kk=kk, ii=ii):
                h = pl.multiple_of(ff * 1536 + ccof(kk) * 768 + ii * U, U)
                fill(2 * ii, kk, ff, tn(ACT[:, pl.ds(h, U)], DM[...]), 2)
            each_f(wdown)
            if kk == 1:
                if ii == 0:
                    pl.semaphore_wait(bar, len(peers))
                st1(2 * ii)
                st1(2 * ii + 1)
    st2(0)
    st2(1)
    loads["wd"].wait()
    for b in range(4):
        loads["gp%d" % b].wait()
        for t in range(3):
            h = b * 768 + t * 256
            du = (nt(DM[...], BIG[h:h + 256, :]) * GP[b % 2, :, t * 256:(t + 1) * 256]).astype(BF16)
            ACT[:, h:h + 256] = du
            s = colsum(du.astype(F32))
            for q in range(2):
                o = h + q * 128
                VV[10 + o // U:11 + o // U, o % U:o % U + 128] = s[:, q * 128:(q + 1) * 128]
        if b < 2:
            load("gp%d" % (b + 2), gp_i.at[:, pl.ds((b + 2) * 768, 768)], GP.at[b % 2])
        if b == 1:
            st2(2)
    st2(3)
    loads["hat"].wait()
    g1, s1 = vector(3), vector(4)

    def to_nb(i, _):
        r = pl.ds(pl.multiple_of(i * RB, RB), RB)
        NB[r, :] = (HAT[r, :] * g1 + s1).astype(BF16)
        return 0
    lax.fori_loop(0, rows // RB, to_nb, 0)
    for ii in range(2):
        for kk in (1, 0):
            if kk == 1:
                for i in (2 * ii, 2 * ii + 1):
                    for cp in c1s(i):
                        cp.wait_send()

            def wup(ff, kk=kk, ii=ii):
                h = pl.multiple_of(ccof(kk) * 1536 + ii * 768, 768)
                fill(4 + 2 * ii, kk, ff, tn(NB[:, pl.ds(pl.multiple_of(ff * U, U), U)], ACT[:, pl.ds(h, 768)]), 2)
            each_f(wup)
            if kk == 1:
                st1(4 + 2 * ii)
                st1(5 + 2 * ii)
    load("tok", tok_i, NB)
    for b in range(4):
        loads[("wu", b)].wait()
    for t in range(3):
        cs = slice(t * 256, (t + 1) * 256)
        acc = DH[:, cs]
        for b in range(4):
            acc = acc + nt(ACT[:, b * 768:(b + 1) * 768], BIG[3072 + b * 768 + t * 256:3072 + b * 768 + (t + 1) * 256, :])
        DH[:, cs] = acc
    for k in (1, 2, 0):
        for blk in range(nblk):
            load(("qkv", k, blk), qkv_i.at[k, blk], BIG.at[pl.ds((k * nblk + blk) * rows, rows)])
    st2(4)
    st2(5)
    loads["lse"].wait()

    def ln1(i, carry):
        r = pl.ds(pl.multiple_of(i * RB, RB), RB)
        dn, hat = DH[r, :], HAT[r, :]
        d = normal_back(dn, hat, COLS[r, 128:129], g1)
        DH[r, :] = d
        da = d.astype(BF16)
        DM[r, :] = da
        return carry[0] + fold8(dn * hat), carry[1] + fold8(dn), carry[2] + fold8(da.astype(F32))
    sums = lax.fori_loop(0, rows // RB, ln1, (zero, zero, zero))
    for row, sv in zip((6, 8, 4), sums):
        put_vec(row, jnp.sum(sv, 0, keepdims=True))
    load("att", att_i, HAT)
    loads["wo"].wait()
    for t in range(3):
        DO[me, :, t * 256:(t + 1) * 256] = nt(DM[...], WO[t * 256:(t + 1) * 256, :]).astype(BF16)

    def d_sib():
        return remote(DO.at[me], DO.at[me], d0s.at[0], d0r.at[0], sib)

    def d_x(j):
        return remote(DO.at[me], DO.at[me], d1s.at[j - 1, 0], d1r.at[j - 1, 0], xps[j - 1])

    def d_f(j):
        w = DO.at[xsrc[j - 1]]
        return remote(w, w, d2s.at[j - 1, 0], d2r.at[j - 1, 0], sib)

    def r_sib():
        return remote(ROWS.at[me], ROWS.at[me], d0s.at[1], d0r.at[1], sib)

    def r_x(j):
        return remote(ROWS.at[me], ROWS.at[me], d1s.at[j - 1, 1], d1r.at[j - 1, 1], xps[j - 1])

    def r_f(j):
        w = ROWS.at[xsrc[j - 1]]
        return remote(w, w, d2s.at[j - 1, 1], d2r.at[j - 1, 1], sib)

    for j in range(1, nx):
        d_x(j).start()
    d_sib().start()
    loads["att"].wait()
    for kk in (1, 0):
        if kk == 1:
            for cp in c1s(4):
                cp.wait_send()

        def wout(ff, kk=kk):
            a = HAT[:, pl.ds(pl.multiple_of(ff * U, U), U)].astype(BF16)
            fill(8, kk, ff, tn(a, DM[:, pl.ds(pl.multiple_of(ccof(kk) * U, U), U)]), 1)
        each_f(wout)
        if kk == 1:
            st1(8)
    head = lax.broadcasted_iota(jnp.int32, (768, 128), 0) // HW
    pick = (head == lax.broadcasted_iota(jnp.int32, (768, 128), 1)).astype(BF16)

    def delta(i, _):
        r = pl.ds(pl.multiple_of(i * 128, 128), 128)
        v = DO[me, r, :].astype(F32) * HAT[r, :]
        hi = v.astype(BF16)
        rest = v - hi.astype(F32)
        mid = rest.astype(BF16)
        low = (rest - mid.astype(F32)).astype(BF16)
        d = mm(hi, pick) + mm(mid, pick) + mm(low, pick)
        COLS[r, 128:256] = d
        ROWS[me, 16:32, r] = jnp.transpose(d)[0:16, :]
        ROWS[me, 0:16, r] = jnp.transpose(COLS[r, 0:128])[0:16, :]
        return 0
    lax.fori_loop(0, rows // 128, delta, 0)
    for j in range(1, nx):
        r_x(j).start()
    r_sib().start()
    st2(6)
    st2(7)
    st2(8)
    st3(0)
    st3(1)

    for k in (1, 2, 0):
        for blk in range(nblk):
            loads[("qkv", k, blk)].wait()
    low_half = head_masks(QT)
    lane128 = lax.broadcasted_iota(jnp.int32, (QT, 128), 1)
    kpos = lax.broadcasted_iota(jnp.int32, (QT, QT), 1)
    krow = lax.broadcasted_iota(jnp.int32, (QT, 128), 0)
    nr = seq_rows // QT
    ntile = rows // QT

    def big(k, blk, r0, cols):
        return BIG[pl.ds(pl.multiple_of((k * nblk + blk) * rows + r0, QT), QT), cols]

    def pick_col(v, h):
        return jnp.sum(jnp.where(lane128 == h, v, 0.0), 1, keepdims=True)

    def zero_other(v, h):
        return jnp.where(low_half == (h == 0), v, jnp.zeros_like(v))

    def dq_one(tile, j):
        s0 = tile // nr
        q0 = pl.multiple_of(tile * QT, QT)
        qr = pl.ds(q0, QT)
        cols = pl.ds(pl.multiple_of(j * 128, 128), 128)
        q = big(0, me, q0, cols)
        do = DO[me, qr, cols]
        length = lens[s0]
        res = []
        for h in range(2):
            qh, doh = zero_other(q, h), zero_other(do, h)
            lse = pick_col(COLS[qr, 0:128], 2 * j + h)
            dl = pick_col(COLS[qr, 128:256], 2 * j + h)
            acc = None
            for blk in range(nblk):
                for r in range(nr):
                    k0 = s0 * seq_rows + r * QT
                    kt = big(1, blk, k0, cols)
                    p = jnp.exp(nt(qh, kt) - lse)
                    p = jnp.where(kpos < length - (blk * seq_rows + r * QT), p, 0.0)
                    ds = (p * (nt(doh, big(2, blk, k0, cols)) - dl)).astype(BF16)
                    o = mm(ds, kt)
                    acc = o if acc is None else acc + o
            res.append(acc)
        DQKV[0, qr, cols] = (jnp.where(low_half, res[0], res[1]) * 0.125).astype(BF16)

    def dkv_one(tile, j):
        s0 = tile // nr
        k0 = pl.multiple_of(tile * QT, QT)
        kr = pl.ds(k0, QT)
        cols = pl.ds(pl.multiple_of(j * 128, 128), 128)
        k, v = big(1, me, k0, cols), big(2, me, k0, cols)
        live = krow < lens[s0] - (me * seq_rows + (tile - s0 * nr) * QT)
        resk, resv = [], []
        for h in range(2):
            kh, vh = zero_other(k, h), zero_other(v, h)
            ak = av = None
            for blk in range(nblk):
                for r in range(nr):
                    q0 = pl.multiple_of(s0 * seq_rows + r * QT, QT)
                    qr = pl.ds(q0, QT)
                    qt, dt = big(0, blk, q0, cols), DO[blk, qr, cols]
                    lse = ROWS[blk, pl.ds(2 * j + h, 1), qr]
                    dl = ROWS[blk, pl.ds(16 + 2 * j + h, 1), qr]
                    p = jnp.exp(nt(kh, qt) - lse)
                    ds = (p * (nt(vh, dt) - dl)).astype(BF16)
                    ov_, ok_ = mm(p.astype(BF16), dt), mm(ds, qt)
                    av = ov_ if av is None else av + ov_
                    ak = ok_ if ak is None else ak + ok_
            resk.append(ak)
            resv.append(av)
        DQKV[1, kr, cols] = jnp.where(live, jnp.where(low_half, resk[0], resk[1]), 0.0).astype(BF16)
        DQKV[2, kr, cols] = jnp.where(live, jnp.where(low_half, resv[0], resv[1]), 0.0).astype(BF16)

    def segment(fn, groups, first, hook):
        per = ntile * 6 // groups

        def group(g, _):
            def one(i, _):
                it = g * per + i
                fn(it // 6, lax.rem(it, 6))
                return 0
            lax.fori_loop(0, per, one, 0)
            tick(first + g)
            if hook is not None:
                @pl.when(g == 2)
                def _():
                    hook()
            return 0
        lax.fori_loop(0, groups, group, 0)

    def relay():
        for j in range(1, nx):
            d_x(j).wait_recv()
            d_f(j).start()
            r_x(j).wait_recv()
            r_f(j).start()

    segment(dq_one, 4, 2, relay)
    d_sib().wait_recv()
    r_sib().wait_recv()
    for j in range(1, nx):
        d_f(j).wait_recv()
        r_f(j).wait_recv()
    segment(dkv_one, 4, 6, None)

    loads["tok"].wait()
    for kk in (1, 0):
        if kk == 1:
            for i in (5, 6, 7):
                for cp in c1s(i):
                    cp.wait_send()
        for i in range(3):
            def wqkv(ff, kk=kk, i=i):
                p = ccof(kk) * 3 + i
                a = NB[:, pl.ds(pl.multiple_of(ff * U, U), U)]
                fill(9 + i, kk, ff, tn(a, DQKV[p // 2, :, pl.ds(pl.multiple_of(lax.rem(p, 2) * U, U), U)]), 1)
            each_f(wqkv)
            if kk == 1:
                st1(9 + i)

    def bias_sum(k):
        def one(i, acc):
            return acc + fold8(DQKV[k, pl.ds(pl.multiple_of(i * RB, RB), RB), :].astype(F32))
        return jnp.sum(lax.fori_loop(0, rows // RB, one, zero), 0, keepdims=True)
    st2(9)
    st2(10)
    st2(11)
    put_vec(0, bias_sum(0))
    put_vec(2, bias_sum(2))
    vst(0)
    for b in range(3):
        loads[("wq", b)].wait()
    for t in range(3):
        cs = slice(t * 256, (t + 1) * 256)
        acc = DH[:, cs]
        for b in range(3):
            acc = acc + nt(DQKV[b], WQ[b, cs, :])
        DM[:, cs] = acc.astype(BF16)
    gout = pltpu.make_async_copy(DM, gin_o, s8.at[NCH])
    gout.start()
    st4(6)
    st5(4)
    st6(3)
    vst(1)
    st4(7)
    st5(5)
    st6(4)
    st7(0)
    st7(1)
    st4(8)
    st5(6)
    st6(5)
    vst(2)
    st7(2)
    st3(9)
    st5(7)
    st6(6)
    vst(3)
    st7(3)
    st5(8)
    st6(7)
    st4(9)
    st3(10)
    st6(8)
    vst(4)
    st7(4)
    st7(5)
    st5(9)
    st4(10)
    st3(11)
    st6(9)
    st7(6)
    st7(7)
    st5(10)
    st4(11)
    st6(10)
    st7(8)
    st5(11)
    st7(9)
    st6(11)
    st7(10)
    st7(11)
    for c in range(NCH):
        c2(c).wait_send()
        c7(c).wait()
        c8(c).wait()
        for j in range(1, nx):
            c3(c, j).wait_send()
            c6(c, j).wait_send()
        for j in range(1, nd):
            c4(c, j).wait_send()
            c5(c, j).wait_send()
    for i in (8, 9, 10, 11):
        for cp in c1s(i):
            cp.wait_send()
    gout.wait()
    v_core().wait_send()
    v_y().wait_send()
    d_sib().wait_send()
    r_sib().wait_send()
    for j in range(1, nx):
        v_x(j).wait_send()
        d_x(j).wait_send()
        d_f(j).wait_send()
        r_x(j).wait_send()
        r_f(j).wait_send()
    for j in range(1, nd):
        v_z(j).wait_send()


def backward_reduce(lens, vec, vg, qkv, att, lse, wq, wo, wu, wd, dh, hat, act, gp, tok, nx, nd, seqs, cid):
    rows, d = att.shape
    nblk = 2 * nx
    CX, PZ = U // nx, U // nx // nd
    N = 12
    anyspec = pl.BlockSpec(memory_space=pl.ANY)
    vspec = pl.BlockSpec(memory_space=pltpu.VMEM)
    sspec = pl.BlockSpec(memory_space=pltpu.SMEM)
    D = pltpu.SemaphoreType.DMA
    V = pltpu.VMEM
    S = jax.ShapeDtypeStruct
    sems = [D((32,)), D((2,)), D((2,))] + [D((nx - 1, 2))] * 4 + [D((N, 2)), D((N, 2)), D((N,)), D((N,)), D((N, nx - 1)), D((N, nx - 1)),
            D((N, nd - 1)), D((N, nd - 1)), D((N, nd - 1)), D((N, nd - 1)), D((N, nx - 1)), D((N, nx - 1)),
            D((N,)), D((N,)), D((N + 1,)), D((nx + nd,)), D((nx + nd,))]
    return pl.pallas_call(
        functools.partial(bwd_kernel, nx, nd, seqs, rows // seqs),
        out_shape=(S((1536, 768), BF16), S((U, 3072), BF16), S((U, 768), BF16), S((U, 2304), BF16), S((12, U), F32), S((rows, d), BF16)),
        in_specs=[sspec, vspec, vspec] + [anyspec] * 12,
        out_specs=(anyspec,) * 4 + (vspec, anyspec),
        scratch_shapes=[V((6144, d), BF16), V((d, d), BF16), V((3, d, d), BF16), V((2, rows, d), F32), V((rows, 3072), BF16),
                        V((rows, d), F32), V((rows, d), BF16), V((rows, d), F32), V((rows, d), BF16), V((nblk, rows, d), BF16),
                        V((nblk, 32, rows), F32), V((rows, 256), F32), V((3, rows, d), BF16),
                        V((N, 2, U, U), BF16), V((4, 2, U, U), BF16), V((N, 2, U, U), BF16), V((N, U, U), BF16),
                        V((N, nx - 1, CX, U), BF16), V((N, nd - 1, PZ, U), BF16), V((N, U, U), BF16),
                        V((24, U), F32), V((3, 24, U), F32), V((nx, 24, U), F32), V((nd, 24, U), F32)] + sems,
        compiler_params=pltpu.CompilerParams(collective_id=cid, has_side_effects=True, vmem_limit_bytes=63 << 20),
        name="backward_reduce",
    )(lens, vec, vg, qkv, att, lse, wq, wo, wu, wd, dh, hat, act, gp, tok)


def fast_body(
    tokens, cotangent, lengths, w_qkv, bias_q, bias_v, w_out, bias_out, gain_one, shift_one,
    w_up, bias_up, w_down, bias_down, gain_two, shift_two,
):
    seqs, seq_rows, width = tokens.shape
    nx, nd = lax.axis_size("ctx") // 2, lax.axis_size("dp")
    small = [bias_q, bias_v, bias_out, gain_one, shift_one, bias_up, bias_down, gain_two, shift_two]
    (qkv, att, lse, wq, wo, wu, wd, vec, out, dh, hat, act, gp, vg) = forward_gather(
        lengths, tokens, cotangent, w_qkv, w_out, w_up, w_down, small, nx, 2
    )
    t_down, t_up, t_out, t_qkv, t_vec, grad_in = backward_reduce(
        lengths, vec, vg, qkv, att, lse, wq, wo, wu, wd, dh, hat, act, gp,
        tokens.reshape(seqs * seq_rows, width), nx, nd, seqs, 3
    )

    def part(first, count):
        return t_vec[first : first + count].reshape(-1)

    return (
        out.reshape(tokens.shape), grad_in.reshape(tokens.shape), t_qkv.astype(F32), part(0, 1), part(1, 1),
        t_out.astype(F32), part(2, 1), part(3, 1), part(4, 1), t_up.astype(F32), part(5, 4),
        t_down.astype(F32), part(9, 1), part(10, 1), part(11, 1),
    )


def solution(mesh):
    return jax.shard_map(
        fast_body if mesh.shape["ctx"] <= 4 else general_body,
        mesh=mesh,
        in_specs=(
            P(("dp", "fsdp"), "ctx", None),
            P(("dp", "fsdp"), "ctx", None),
            P(("dp", "fsdp")),
            P("fsdp", None),
            P("fsdp"),
            P("fsdp"),
            P("fsdp", None),
            P("fsdp"),
            P("fsdp"),
            P("fsdp"),
            P("fsdp", None),
            P("fsdp"),
            P("fsdp", None),
            P("fsdp"),
            P("fsdp"),
            P("fsdp"),
        ),
        out_specs=(
            P(("dp", "fsdp"), "ctx", None),
            P(("dp", "fsdp"), "ctx", None),
            P("fsdp", None),
            P("fsdp"),
            P("fsdp"),
            P("fsdp", None),
            P("fsdp"),
            P("fsdp"),
            P("fsdp"),
            P("fsdp", None),
            P("fsdp"),
            P("fsdp", None),
            P("fsdp"),
            P("fsdp"),
            P("fsdp"),
        ),
        check_vma=False,
    )
```

```python
import functools
import math

import jax
import jax.numpy as jnp
from jax import lax
from jax.experimental import pallas as pl
from jax.experimental.pallas import tpu as pltpu
from jax.sharding import PartitionSpec as P

MESH = pl.DeviceIdType.MESH
F32, BF16 = jnp.float32, jnp.bfloat16
U = 384
VR = 24


def places():
    c = lax.axis_index("ctx")
    return lax.rem(c, 2), c // 2, lax.axis_index("fsdp"), lax.axis_index("dp")


def grad_kernel(nx, nd, grp, wd, wu, wo, wq, vec, od, ou, oo, oq, ov,
                L, R1, R2, R3, R4, AX, AC, ST, V0, VX, VZ,
                s0, s1s, s1r, s2s, s2r, s3s, s3r, s4s, s4r, s5s, s5r, s6s, s6r, s7s, s7r, so, vs, vr):
    core, x, f, z = places()
    nch = 12 // grp
    CH, CX, PZ = U * grp, U * grp // nx, U * grp // nx // nd
    sib = {"ctx": x * 2 + 1 - core}
    yp = {"fsdp": 1 - f}
    xps = [{"ctx": lax.rem(x + j, nx) * 2 + core} for j in range(1, nx)]
    zps = [{"dp": lax.rem(z + j, nd)} for j in range(1, nd)]
    peers = [sib, yp] + xps + zps
    bar = pltpu.get_barrier_semaphore()
    for p in peers:
        pl.semaphore_signal(bar, inc=1, device_id=p, device_id_type=MESH)

    def rect(i, ff, cc):
        if i < 4:
            return wd, ff * 1536 + i * U, cc * U
        if i < 8:
            return wu, ff * U, cc * 1536 + (i - 4) * U
        if i < 9:
            return wo, ff * U, cc * U
        return wq, ff * U, cc * 1152 + (i - 9) * U

    def orect(i, cc):
        if i < 4:
            return od, i * U, cc * U
        if i < 8:
            return ou, 0, cc * 1536 + (i - 4) * U
        if i < 9:
            return oo, 0, cc * U
        return oq, 0, cc * 1152 + (i - 9) * U

    def sl(ref, r, c):
        return ref.at[pl.ds(pl.multiple_of(r, U), U), pl.ds(pl.multiple_of(c, 128), U)]

    def local(i, k):
        ff = (1 - f) if k == 0 else f
        return pltpu.make_async_copy(sl(*rect(i, ff, core)), L.at[i // grp, ff, pl.ds(i % grp * U, U)], s0.at[i, k])

    def remote(src, dst, ss, rs, dev):
        return pltpu.make_async_remote_copy(src_ref=src, dst_ref=dst, send_sem=ss, recv_sem=rs, device_id=dev, device_id_type=MESH)

    def c1(i, k):
        ff = (1 - f) if k == 0 else f
        return remote(sl(*rect(i, ff, 1 - core)), R1.at[i // grp, ff, pl.ds(i % grp * U, U)], s1s.at[i, k], s1r.at[i, k], sib)

    def c2(c):
        return remote(L.at[c, 1 - f], R2.at[c], s2s.at[c], s2r.at[c], yp)

    def c3(c, j):
        xt = lax.rem(x + j, nx)
        return remote(L.at[c, f, pl.ds(pl.multiple_of(xt * CX, CX), CX)], R3.at[c, j - 1], s3s.at[c, j - 1], s3r.at[c, j - 1], xps[j - 1])

    def mine(c, zz):
        return pl.ds(pl.multiple_of(x * CX + zz * PZ, PZ), PZ)

    def c4(c, j):
        zt = lax.rem(z + j, nd)
        return remote(L.at[c, f, mine(c, zt)], R4.at[c, j - 1], s4s.at[c, j - 1], s4r.at[c, j - 1], zps[j - 1])

    def c5(c, j):
        return remote(AX.at[c, mine(c, z)], AX.at[c, mine(c, z)], s5s.at[c, j - 1], s5r.at[c, j - 1], zps[j - 1])

    def c6(c, j):
        rows = pl.ds(pl.multiple_of(x * CX, CX), CX)
        return remote(AX.at[c, rows], AX.at[c, rows], s6s.at[c, j - 1], s6r.at[c, j - 1], xps[j - 1])

    def c7(c):
        return remote(AX.at[c], AC.at[c], s7s.at[c], s7r.at[c], sib)

    B = 48

    def rows_loop(n, fn):
        def bodyf(i, _):
            fn(pl.multiple_of(i * B, B))
            return 0
        lax.fori_loop(0, n // B, bodyf, 0)

    def up(v):
        return v.astype(F32)

    def st2(c):
        for k in range(grp):
            local(c * grp + k, 0).wait()
            c1(c * grp + k, 0).wait_recv()

        def fn(r):
            s = pl.ds(r, B)
            L[c, 1 - f, s, :] = (up(L[c, 1 - f, s, :]) + up(R1[c, 1 - f, s, :])).astype(BF16)
        rows_loop(CH, fn)
        c2(c).start()

    def st3(c):
        for k in range(grp):
            local(c * grp + k, 1).wait()
            c1(c * grp + k, 1).wait_recv()
        c2(c).wait_recv()
        for j in range(1, nx):
            xt = lax.rem(x + j, nx)

            def fn(r):
                s = pl.ds(pl.multiple_of(xt * CX + r, B), B)
                L[c, f, s, :] = (up(L[c, f, s, :]) + up(R1[c, f, s, :]) + up(R2[c, s, :])).astype(BF16)
            rows_loop(CX, fn)
            c3(c, j).start()

    def st4(c):
        for j in range(1, nx):
            c3(c, j).wait_recv()

        def fn(r):
            s = pl.ds(pl.multiple_of(x * CX + r, B), B)
            t = up(L[c, f, s, :]) + up(R1[c, f, s, :]) + up(R2[c, s, :])
            for j in range(1, nx):
                t = t + up(R3[c, j - 1, pl.ds(r, B), :])
            L[c, f, s, :] = t.astype(BF16)
        rows_loop(CX, fn)
        for j in range(1, nd):
            c4(c, j).start()

    def st5(c):
        for j in range(1, nd):
            c4(c, j).wait_recv()
        t = up(L[c, f, mine(c, z), :])
        for j in range(1, nd):
            t = t + up(R4[c, j - 1])
        AX[c, mine(c, z), :] = t.astype(BF16)
        for j in range(1, nd):
            c5(c, j).start()

    def st6(c):
        for j in range(1, nd):
            c5(c, j).wait_recv()
        for j in range(1, nx):
            c6(c, j).start()

    def outc(i, k, slot):
        cc = core if k == 0 else 1 - core
        return pltpu.make_async_copy(ST.at[slot], sl(*orect(i, cc)), so.at[slot])

    def emit(i, k, src):
        slot = emit.n % 4
        if emit.n >= 4:
            outc(*emit.log[emit.n - 4], slot).wait()
        off = i % grp * U

        def fn(r):
            ST[slot, pl.ds(r, B), :] = up(src[i // grp, pl.ds(pl.multiple_of(off + r, B), B), :])
        rows_loop(U, fn)
        outc(i, k, slot).start()
        emit.log.append((i, k))
        emit.n += 1
    emit.n = 0
    emit.log = []

    def st7(c):
        for j in range(1, nx):
            c6(c, j).wait_recv()
        c7(c).start()
        for k in range(grp):
            emit(c * grp + k, 0, AX)

    def st8(c):
        c7(c).wait_recv()
        for k in range(grp):
            emit(c * grp + k, 1, AC)

    def v_core():
        return remote(vec, V0.at[0], vs.at[0], vr.at[0], sib)

    def v_y():
        return remote(V0.at[1], V0.at[2], vs.at[1], vr.at[1], yp)

    def v_x(j):
        return remote(VX.at[x], VX.at[x], vs.at[1 + j], vr.at[1 + j], xps[j - 1])

    def v_z(j):
        return remote(VZ.at[z], VZ.at[z], vs.at[nx + j], vr.at[nx + j], zps[j - 1])

    def vst(k):
        if k == 0:
            v_core().start()
        elif k == 1:
            v_core().wait_recv()
            V0[1] = vec[...] + V0[0]
            v_y().start()
        elif k == 2:
            v_y().wait_recv()
            VX[x] = V0[1] + V0[2]
            for j in range(1, nx):
                v_x(j).start()
        elif k == 3:
            for j in range(1, nx):
                v_x(j).wait_recv()
            t = VX[0]
            for j in range(1, nx):
                t = t + VX[j]
            VZ[z] = t
            for j in range(1, nd):
                v_z(j).start()
        elif k == 4:
            for j in range(1, nd):
                v_z(j).wait_recv()
            t = VZ[0]
            for j in range(1, nd):
                t = t + VZ[j]
            ov[...] = t

    for i in range(12):
        local(i, 0).start()
    pl.semaphore_wait(bar, len(peers))
    for i in range(12):
        c1(i, 0).start()
    vst(0)
    for i in range(12):
        local(i, 1).start()
        c1(i, 1).start()
    stages = [(8, st8), (7, st7), (6, st6), (5, st5), (4, st4), (3, st3)]
    for t in range(nch + 8):
        if t < nch:
            st2(t)
        if 1 <= t <= 4:
            vst(t)
        for k, fn in stages:
            c = t - (k - 1)
            if 0 <= c < nch:
                fn(c)
    n = emit.n
    for q in range(max(0, n - 4), n):
        outc(*emit.log[q], q % 4).wait()
    for i in range(12):
        for k in range(2):
            c1(i, k).wait_send()
    for c in range(nch):
        c2(c).wait_send()
        c7(c).wait_send()
        for j in range(1, nx):
            c3(c, j).wait_send()
            c6(c, j).wait_send()
        for j in range(1, nd):
            c4(c, j).wait_send()
            c5(c, j).wait_send()
    v_core().wait_send()
    v_y().wait_send()
    for j in range(1, nx):
        v_x(j).wait_send()
    for j in range(1, nd):
        v_z(j).wait_send()


def grad_reduce(wd, wu, wo, wq, vec, nx, nd, cid):
    grp = nx * nd // 8
    nch = 12 // grp
    CH, CX, PZ = U * grp, U * grp // nx, U * grp // nx // nd
    anyspec = pl.BlockSpec(memory_space=pl.ANY)
    vspec = pl.BlockSpec(memory_space=pltpu.VMEM)
    D = pltpu.SemaphoreType.DMA
    V = pltpu.VMEM
    sems = [D((12, 2)), D((12, 2)), D((12, 2)), D((nch,)), D((nch,)), D((nch, nx - 1)), D((nch, nx - 1)),
            D((nch, nd - 1)), D((nch, nd - 1)), D((nch, nd - 1)), D((nch, nd - 1)), D((nch, nx - 1)), D((nch, nx - 1)),
            D((nch,)), D((nch,)), D((4,)), D((nx + nd,)), D((nx + nd,))]
    return pl.pallas_call(
        functools.partial(grad_kernel, nx, nd, grp),
        out_shape=(jax.ShapeDtypeStruct((1536, 768), F32), jax.ShapeDtypeStruct((U, 3072), F32),
                   jax.ShapeDtypeStruct((U, 768), F32), jax.ShapeDtypeStruct((U, 2304), F32),
                   jax.ShapeDtypeStruct((VR, U), F32)),
        in_specs=[anyspec] * 4 + [vspec],
        out_specs=(anyspec,) * 4 + (vspec,),
        scratch_shapes=[V((nch, 2, CH, U), BF16), V((nch, 2, CH, U), BF16), V((nch, CH, U), BF16),
                        V((nch, nx - 1, CX, U), BF16), V((nch, nd - 1, PZ, U), BF16),
                        V((nch, CH, U), BF16), V((nch, CH, U), BF16), V((4, U, U), F32),
                        V((3, VR, U), F32), V((nx, VR, U), F32), V((nd, VR, U), F32)] + sems,
        compiler_params=pltpu.CompilerParams(collective_id=cid, has_side_effects=True, vmem_limit_bytes=60 << 20),
        name="grad_reduce",
    )(wd, wu, wo, wq, vec)


HEADS = 12


EPSILON = 1e-12
MASKED = -1e30


def shifted(value, axis, steps):
    count = lax.axis_size(axis)
    pairs = [(source, (source + steps) % count) for source in range(count)]
    return lax.ppermute(value, axis, pairs)


def normalize(values, norm_gain, norm_shift):
    row_mean = jnp.mean(values, -1, keepdims=True)
    centred = values - row_mean
    spread = jnp.mean(centred * centred, -1, keepdims=True)
    return centred * lax.rsqrt(spread + EPSILON) * norm_gain + norm_shift


def gelu_exact(values):
    return jax.nn.gelu(values, approximate=False)


def row_dot(left_op, right_op):
    return jnp.dot(left_op, right_op, preferred_element_type=jnp.float32)


def left_dot(left_op, right_op):
    return lax.dot_general(
        left_op, right_op, (((0,), (0,)), ((), ())), preferred_element_type=jnp.float32
    )


def right_dot(left_op, right_op):
    return lax.dot_general(
        left_op, right_op, (((1,), (1,)), ((), ())), preferred_element_type=jnp.float32
    )


def general_body(
    tokens,
    cotangent,
    lengths,
    w_qkv,
    bias_q,
    bias_v,
    w_out,
    bias_out,
    gain_one,
    shift_one,
    w_up,
    bias_up,
    w_down,
    bias_down,
    gain_two,
    shift_two,
):
    seq_count, block_rows, model_width = tokens.shape
    head_count = HEADS
    head_dim = model_width // head_count
    all_rows = seq_count * block_rows
    score_scale = head_dim ** (-0.5)
    cycle_size = lax.axis_size("ctx")
    cycle_index = lax.axis_index("ctx")
    gathered = (
        lax.all_gather(w_qkv, "fsdp", axis=0, tiled=True),
        lax.all_gather(bias_q, "fsdp", axis=0, tiled=True),
        lax.all_gather(bias_v, "fsdp", axis=0, tiled=True),
        lax.all_gather(w_out, "fsdp", axis=0, tiled=True),
        lax.all_gather(bias_out, "fsdp", axis=0, tiled=True),
        lax.all_gather(gain_one, "fsdp", axis=0, tiled=True),
        lax.all_gather(shift_one, "fsdp", axis=0, tiled=True),
        lax.all_gather(w_up, "fsdp", axis=0, tiled=True),
        lax.all_gather(bias_up, "fsdp", axis=0, tiled=True),
        lax.all_gather(w_down, "fsdp", axis=0, tiled=True),
        lax.all_gather(bias_down, "fsdp", axis=0, tiled=True),
        lax.all_gather(gain_two, "fsdp", axis=0, tiled=True),
        lax.all_gather(shift_two, "fsdp", axis=0, tiled=True),
    )
    full_qkv, full_out, full_up, full_down = (gathered[0], gathered[3], gathered[7], gathered[9])
    add_q, add_v, add_out, scale_one, move_one, add_up, add_down, scale_two, move_two = [
        gathered[place].astype(jnp.float32) for place in (1, 2, 4, 5, 6, 8, 10, 11, 12)
    ]
    flat_tokens = tokens.reshape(all_rows, model_width)
    projected = row_dot(flat_tokens, full_qkv)
    queries = (
        (projected[:, :model_width] + add_q)
        .astype(jnp.bfloat16)
        .reshape(seq_count, block_rows, head_count, head_dim)
    )
    key_rows = (
        projected[:, model_width : 2 * model_width]
        .astype(jnp.bfloat16)
        .reshape(seq_count, block_rows, model_width)
    )
    value_rows = (
        (projected[:, 2 * model_width :] + add_v)
        .astype(jnp.bfloat16)
        .reshape(seq_count, block_rows, model_width)
    )
    start_state = (
        jnp.full((seq_count, block_rows, head_count), MASKED, jnp.float32),
        jnp.zeros((seq_count, block_rows, head_count), jnp.float32),
        jnp.zeros((seq_count, block_rows, head_count, head_dim), jnp.float32),
    )
    key_part = lax.all_gather(key_rows, "ctx", axis=1, tiled=True)
    value_part = lax.all_gather(value_rows, "ctx", axis=1, tiled=True)
    key_count = key_part.shape[1]
    sub_rows = math.gcd(key_count, 512)

    def visit(block_index, carried):
        first_key = block_index * sub_rows
        key_block = lax.dynamic_slice_in_dim(key_part, block_index * sub_rows, sub_rows, 1).reshape(
            seq_count, sub_rows, head_count, head_dim
        )
        value_block = lax.dynamic_slice_in_dim(
            value_part, block_index * sub_rows, sub_rows, 1
        ).reshape(seq_count, sub_rows, head_count, head_dim)
        peak, weight_sum, weighted = carried
        key_live = (
            (first_key + jnp.arange(sub_rows, dtype=jnp.int32))[None, :] < lengths[:, None]
        )[:, None, None, :]
        scores = (
            jnp.einsum("sqhe,skhe->sqhk", queries, key_block, preferred_element_type=jnp.float32)
            * score_scale
        )
        scores = jnp.where(key_live, scores, MASKED)
        new_peak = jnp.maximum(peak, jnp.max(scores, -1))
        factor = jnp.exp(peak - new_peak)
        weights = jnp.where(key_live, jnp.exp(scores - new_peak[..., None]), 0.0)
        mixed_values = jnp.einsum(
            "sqhk,skhe->sqhe",
            weights.astype(jnp.bfloat16),
            value_block,
            preferred_element_type=jnp.float32,
        )
        return (
            new_peak,
            weight_sum * factor + jnp.sum(weights, -1),
            weighted * factor[..., None] + mixed_values,
        )

    peak, weight_sum, weighted = lax.fori_loop(0, key_count // sub_rows, visit, start_state)
    log_total = peak + jnp.log(weight_sum)
    attended = weighted / weight_sum[..., None]
    attended_low = attended.astype(jnp.bfloat16).reshape(all_rows, model_width)
    first_sum = flat_tokens.astype(jnp.float32) + row_dot(attended_low, full_out) + add_out
    normed, norm_pull = jax.vjp(normalize, first_sum, scale_one, move_one)
    normed_low = normed.astype(jnp.bfloat16)
    hidden_pre = row_dot(normed_low, full_up) + add_up
    hidden_act, gelu_pull = jax.vjp(gelu_exact, hidden_pre)
    hidden_low = hidden_act.astype(jnp.bfloat16)
    second_sum = normed + row_dot(hidden_low, full_down) + add_down
    result, result_pull = jax.vjp(normalize, second_sum, scale_two, move_two)
    grad_second, grad_gain_two, grad_shift_two = result_pull(
        cotangent.reshape(all_rows, model_width).astype(jnp.float32)
    )
    down_low = grad_second.astype(jnp.bfloat16)
    grad_w_down = left_dot(hidden_low, down_low)
    grad_bias_down = jnp.sum(down_low.astype(jnp.float32), 0)
    (grad_pre,) = gelu_pull(right_dot(down_low, full_down))
    up_low = grad_pre.astype(jnp.bfloat16)
    grad_w_up = left_dot(normed_low, up_low)
    grad_bias_up = jnp.sum(up_low.astype(jnp.float32), 0)
    grad_first, grad_gain_one, grad_shift_one = norm_pull(grad_second + right_dot(up_low, full_up))
    branch_low = grad_first.astype(jnp.bfloat16)
    grad_w_out = left_dot(attended_low, branch_low)
    grad_bias_out = jnp.sum(branch_low.astype(jnp.float32), 0)
    grad_att = (
        right_dot(branch_low, full_out)
        .astype(jnp.bfloat16)
        .reshape(seq_count, block_rows, head_count, head_dim)
    )
    delta_rows = jnp.sum(grad_att.astype(jnp.float32) * attended, -1)

    def block_grads(query_part, grad_part, lse_part, delta_part, key_block, value_block, first_key):
        key_count = key_block.shape[1]
        key_heads = key_block.reshape(seq_count, key_count, head_count, head_dim)
        value_heads = value_block.reshape(seq_count, key_count, head_count, head_dim)
        key_live = (
            (first_key + jnp.arange(key_count, dtype=jnp.int32))[None, :] < lengths[:, None]
        )[:, None, None, :]
        scores = (
            jnp.einsum("sqhe,skhe->sqhk", query_part, key_heads, preferred_element_type=jnp.float32)
            * score_scale
        )
        chances = jnp.where(key_live, jnp.exp(scores - lse_part[..., None]), 0.0)
        grad_value = jnp.einsum(
            "sqhk,sqhe->skhe",
            chances.astype(jnp.bfloat16),
            grad_part,
            preferred_element_type=jnp.float32,
        )
        grad_chance = jnp.einsum(
            "sqhe,skhe->sqhk", grad_part, value_heads, preferred_element_type=jnp.float32
        )
        grad_score = (chances * (grad_chance - delta_part[..., None])).astype(jnp.bfloat16)
        grad_query = (
            jnp.einsum("sqhk,skhe->sqhe", grad_score, key_heads, preferred_element_type=jnp.float32)
            * score_scale
        )
        grad_key = (
            jnp.einsum(
                "sqhk,sqhe->skhe", grad_score, query_part, preferred_element_type=jnp.float32
            )
            * score_scale
        )
        return (
            grad_query,
            grad_key.reshape(seq_count, key_count, model_width),
            grad_value.reshape(seq_count, key_count, model_width),
        )

    query_start = jnp.zeros((seq_count, block_rows, head_count, head_dim), jnp.float32)

    def key_terms(key_block, value_block, first_key):
        return block_grads(
            queries, grad_att, log_total, delta_rows, key_block, value_block, first_key
        )

    def block_terms(key_block, value_block, first_key):
        return key_terms(key_block, value_block, first_key)

    def turn(step_index, carried):
        key_now, value_now, key_grads, query_acc = carried
        first_key = (cycle_index - step_index) % cycle_size * block_rows
        add_query, add_key, add_value = block_terms(key_now, value_now, first_key)
        key_now, value_now = shifted((key_now, value_now), "ctx", 1)
        key_grads = (
            shifted((key_grads[0] + add_key).astype(jnp.bfloat16), "ctx", 1).astype(jnp.float32),
            shifted((key_grads[1] + add_value).astype(jnp.bfloat16), "ctx", 1).astype(jnp.float32),
        )
        return (key_now, value_now, key_grads, query_acc + add_query)

    grad_start = (
        jnp.zeros((seq_count, block_rows, model_width), jnp.float32),
        jnp.zeros((seq_count, block_rows, model_width), jnp.float32),
    )
    key_final, value_final, key_grads, query_grad = lax.fori_loop(
        0, cycle_size, turn, (key_rows, value_rows, grad_start, query_start)
    )
    grad_key, grad_value = key_grads
    qkv_grad = jnp.concatenate(
        [
            query_grad.astype(jnp.bfloat16).reshape(all_rows, model_width),
            grad_key.astype(jnp.bfloat16).reshape(all_rows, model_width),
            grad_value.astype(jnp.bfloat16).reshape(all_rows, model_width),
        ],
        1,
    )
    grad_w_qkv = left_dot(flat_tokens, qkv_grad)
    grad_bias_q = jnp.sum(qkv_grad[:, :model_width].astype(jnp.float32), 0)
    grad_bias_v = jnp.sum(qkv_grad[:, 2 * model_width :].astype(jnp.float32), 0)
    grad_input = grad_first + right_dot(qkv_grad, full_qkv)
    vectors = (
        grad_bias_q,
        grad_bias_v,
        grad_bias_out,
        grad_gain_one,
        grad_shift_one,
        grad_bias_up,
        grad_bias_down,
        grad_gain_two,
        grad_shift_two,
    )
    packed = jnp.concatenate(vectors).reshape(VR, U)
    t_down, t_up, t_out, t_qkv, t_vec = grad_reduce(
        grad_w_down.astype(BF16),
        grad_w_up.astype(BF16),
        grad_w_out.astype(BF16),
        grad_w_qkv.astype(BF16),
        packed,
        cycle_size // 2,
        lax.axis_size("dp"),
        1,
    )
    flat = t_vec.reshape(-1)
    own = lax.axis_index("fsdp")
    parts, start = [], 0
    for vector in vectors:
        half = vector.shape[0] // 2
        parts.append(lax.dynamic_slice_in_dim(flat, start + own * half, half, 0))
        start += 2 * half
    totals = (
        t_qkv, parts[0], parts[1], t_out, parts[2], parts[3], parts[4],
        t_up, parts[5], t_down, parts[6], parts[7], parts[8],
    )
    output_rows = result.astype(jnp.bfloat16).reshape(seq_count, block_rows, model_width)
    input_rows = grad_input.astype(jnp.bfloat16).reshape(seq_count, block_rows, model_width)
    return (
        output_rows,
        input_rows,
        totals[0],
        totals[1],
        totals[2],
        totals[3],
        totals[4],
        totals[5],
        totals[6],
        totals[7],
        totals[8],
        totals[9],
        totals[10],
        totals[11],
        totals[12],
    )


HW = 64
QT = 256


def remote(src, dst, ss, rs, dev):
    return pltpu.make_async_remote_copy(src_ref=src, dst_ref=dst, send_sem=ss, recv_sem=rs, device_id=dev, device_id_type=MESH)


def nt(a, b):
    return lax.dot_general(a, b, (((1,), (1,)), ((), ())), preferred_element_type=F32)


def mm(a, b):
    return jnp.dot(a, b, preferred_element_type=F32)


def head_masks(rows):
    lane = lax.broadcasted_iota(jnp.int32, (rows, 2 * HW), 1)
    return lane < HW


def normal_parts(v):
    mean = jnp.mean(v, -1, keepdims=True)
    cen = v - mean
    inv = lax.rsqrt(jnp.mean(cen * cen, -1, keepdims=True) + EPSILON)
    return cen * inv, inv


def normal_back(dn, hat, inv, gain):
    d = dn * gain
    return inv * (d - jnp.mean(d, -1, keepdims=True) - hat * jnp.mean(d * hat, -1, keepdims=True))


def gelu_pair(u):
    w = jnp.abs(u)
    t = 1.0 / (1.0 + (0.3275911 * math.sqrt(0.5)) * w)
    e = jnp.exp(-0.5 * u * u)
    poly = t * (0.127414796 + t * (-0.142248368 + t * (0.7107068705 + t * (-0.7265760135 + t * 0.5307027145))))
    tail = poly * e
    phi = jnp.where(u < 0.0, tail, 1.0 - tail)
    return u * phi, phi + u * (e * (1.0 / math.sqrt(2.0 * math.pi)))


def fold8(v):
    return jnp.sum(v.reshape(v.shape[0] // 8, 8, v.shape[1]), 0)


def fwd_kernel(nx, seqs, seq_rows, lens, tok, cot, sq, so_, su, sd, *rest):
    small = rest[:9]
    (qkv_o, att_o, lse_o, wq_o, wo_o, wu_o, wd_o, vec_o, y_o, dh_o, hat_o, act_o, gp_o, vg_o) = rest[9:23]
    (XT, WB, QKV, CT, ATT, LSE, H1, N1, N1B, ACT, GP, YB,
               ls, ys, yr, zs, zr, as_, ar, bs, br, t0s, t0r, t1s, t1r, t2s, t2r, vs, vr, lts, outs) = rest[23:]
    core, x, f, z = places()
    me = x * 2 + core
    nblk = 2 * nx
    rows = seqs * seq_rows
    sib = {"ctx": x * 2 + 1 - core}
    yp = {"fsdp": 1 - f}
    zp = {"dp": z + 1 - 2 * lax.rem(z, 2)}
    zb = lax.rem(z, 2)
    xts = [lax.rem(x + j, nx) for j in range(1, nx)]
    xps = [{"ctx": t * 2 + core} for t in xts]
    xsrc = [lax.rem(x + nx - j, nx) * 2 + core for j in range(1, nx)]
    peers = [sib, yp, zp] + xps
    bar = pltpu.get_barrier_semaphore()
    for p in peers:
        pl.semaphore_signal(bar, inc=1, device_id=p, device_id_type=MESH)
    order = (1, 2, 0)
    PR = U // 4
    piece = pl.multiple_of((zb * 2 + core) * PR, PR)
    zpiece = pl.multiple_of(((1 - zb) * 2 + core) * PR, PR)
    H = rows // 2

    def shard(b, r0, n):
        r = pl.ds(r0, n)
        if b < 3:
            return sq.at[r, pl.ds(b * 768, 768)]
        if b == 3:
            return so_.at[r, :]
        if b < 8:
            return su.at[r, pl.ds((b - 4) * 768, 768)]
        return sd.at[pl.ds((b - 8) * U + r0, n), :]

    def loc(b):
        return pltpu.make_async_copy(shard(b, 0, U), WB.at[b, f], ls.at[b])

    def ycp(b):
        if not isinstance(b, int):
            src = WB.at[b, f, pl.ds(piece, PR)]
        else:
            src = shard(b, piece, PR)
        return remote(src, WB.at[b, f, pl.ds(piece, PR)], ys.at[b], yr.at[b], yp)

    def zcp(b):
        w = WB.at[b, 1 - f, pl.ds(piece, PR)]
        return remote(w, w, zs.at[b], zr.at[b], zp)

    def acp(b):
        w = WB.at[b, 1 - f, pl.ds(piece, PR)]
        return remote(w, w, as_.at[b], ar.at[b], sib)

    def bcp(b):
        w = WB.at[b, 1 - f, pl.ds(zpiece, PR)]
        return remote(w, w, bs.at[b], br.at[b], sib)

    def A(b):
        ycp(b).wait_recv()
        zcp(b).start()
        acp(b).start()

    def B(b):
        zcp(b).wait_recv()
        bcp(b).start()

    def C(b):
        acp(b).wait_recv()
        bcp(b).wait_recv()

    def tsl(h):
        return pl.ds(h * H, H)

    def t_sib(h):
        return remote(tok.at[tsl(h)], XT.at[me, tsl(h)], t0s.at[h], t0r.at[h], sib)

    def t_x(j, h):
        return remote(tok.at[tsl(h)], XT.at[me, tsl(h)], t1s.at[j - 1, h], t1r.at[j - 1, h], xps[j - 1])

    def t_f(j, h):
        w = XT.at[xsrc[j - 1], tsl(h)]
        return remote(w, w, t2s.at[j - 1, h], t2r.at[j - 1, h], sib)

    vcp = remote(vec_o.at[f], vec_o.at[f], vs.at[0], vr.at[0], yp)
    tl = pltpu.make_async_copy(tok, XT.at[me], lts.at[0])
    tl.start()
    for b in order:
        loc(b).start()
    row = 0
    for v in small:
        w = v[...].astype(F32).reshape(1, -1)
        for i in range(v.shape[0] // U):
            vec_o[f, row:row + 1, :] = w[:, i * U:(i + 1) * U]
            row += 1
    tc = pltpu.make_async_copy(cot, CT, lts.at[1])
    pl.semaphore_wait(bar, len(peers))
    vcp.start()
    for b in order:
        ycp(b).start()
    for h in range(2):
        for j in range(1, nx):
            t_x(j, h).start()
        t_sib(h).start()
    for b in range(3, 12):
        ycp(b).start()
    for b in range(3, 12):
        loc(b).start()
    tc.start()
    tl.wait()

    def qkv(b, blk, h):
        hr = pl.ds(pl.multiple_of(h * H, H), H)
        row = 0 if b == 0 else 1
        xr = XT[blk, hr, :]
        for t in range(3):
            w = WB[b, :, :, t * 256:(t + 1) * 256].reshape(768, 256)
            r = mm(xr, w)
            if b != 1:
                if t == 0:
                    bias = vec_o[0, row:row + 1, 0:256]
                elif t == 1:
                    bias = jnp.concatenate([vec_o[0, row:row + 1, 256:384], vec_o[1, row:row + 1, 0:128]], 1)
                else:
                    bias = vec_o[1, row:row + 1, 128:384]
                r = r + bias
            r = r.astype(BF16)
            if b == 0:
                r = r * jnp.asarray(0.125, BF16)
            QKV[b, blk, hr, t * 256:(t + 1) * 256] = r

    def far(h, bs):
        for j in range(1, nx):
            base = lax.rem(x + nx - j, nx) * 2

            def pair(i, _):
                for b in bs:
                    qkv(b, base + i, h)
                return 0
            lax.fori_loop(0, 2, pair, 0)

    def far_wait(h):
        for j in range(1, nx):
            t_f(j, h).wait_recv()

    def relay(h):
        for j in range(1, nx):
            t_x(j, h).wait_recv()
            t_f(j, h).start()

    def near(b):
        def both(i, _):
            qkv(b, x * 2 + i // 2, lax.rem(i, 2))
            return 0
        lax.fori_loop(0, 4, both, 0)

    A(1)
    for h in range(2):
        t_sib(h).wait_recv()
    vcp.wait_recv()
    loc(1).wait()
    B(1)
    A(2)
    C(1)
    near(1)
    B(2)
    A(0)
    relay(0)
    loc(2).wait()
    C(2)
    near(2)
    B(0)
    far_wait(0)
    far(0, (1,))
    A(3)
    loc(0).wait()
    C(0)
    near(0)
    A(4)
    far(0, (2, 0))

    low_half = head_masks(QT)
    lane128 = lax.broadcasted_iota(jnp.int32, (QT, 128), 1)
    kpos = lax.broadcasted_iota(jnp.int32, (QT, QT), 1)
    nr = seq_rows // QT

    def attend(tile, j):
        s0 = tile // nr
        qr = pl.ds(pl.multiple_of(tile * QT, QT), QT)
        cols = pl.ds(pl.multiple_of(j * 128, 128), 128)
        q = QKV[0, me, qr, cols]
        length = lens[s0]
        outs_ = []
        tot = LSE[qr, 0:128]
        for h in range(2):
            qh = jnp.where(low_half == (h == 0), q, jnp.zeros_like(q))
            sc = []
            mx = None
            for blk in range(nblk):
                for r in range(nr):
                    kr = pl.ds(pl.multiple_of(s0 * seq_rows + r * QT, QT), QT)
                    v = nt(qh, QKV[1, blk, kr, cols])
                    v = jnp.where(kpos < length - (blk * seq_rows + r * QT), v, MASKED)
                    sc.append(v)
                    mx = v if mx is None else jnp.maximum(mx, v)
            m = jnp.max(mx, 1, keepdims=True)
            acc = None
            lsum = None
            i = 0
            for blk in range(nblk):
                for r in range(nr):
                    kr = pl.ds(pl.multiple_of(s0 * seq_rows + r * QT, QT), QT)
                    p = jnp.exp(sc[i] - m)
                    i += 1
                    lsum = p if lsum is None else lsum + p
                    o = mm(p.astype(BF16), QKV[2, blk, kr, cols])
                    acc = o if acc is None else acc + o
            den = jnp.sum(lsum, 1, keepdims=True)
            outs_.append(acc / den)
            tot = jnp.where(lane128 == 2 * j + h, m + jnp.log(den), tot)
        ATT[qr, cols] = jnp.where(low_half, outs_[0], outs_[1])
        LSE[qr, 0:128] = tot

    tiles = rows // QT // 2

    def attend_half(h, hooks):
        per = tiles * 6 // len(hooks)

        def group(g, _):
            def one(i, _):
                it = g * per + i
                attend(h * tiles + it // 6, lax.rem(it, 6))
                return 0
            lax.fori_loop(0, per, one, 0)
            for k, hook in enumerate(hooks):
                @pl.when(g == k)
                def _(hook=hook):
                    hook()
            return 0
        lax.fori_loop(0, len(hooks), group, 0)

    def step(a):
        def fn():
            A(a)
            B(a - 2)
        return fn

    def last():
        step(7)()
        relay(1)
    attend_half(0, (step(5), step(6), last))
    far_wait(1)
    far(1, order)
    step(8)()
    qo = pltpu.make_async_copy(QKV, qkv_o, outs.at[0])
    qo.start()
    attend_half(1, (step(9), step(10), step(11)))
    extra = []

    def send_out(src, dst):
        cp = pltpu.make_async_copy(src, dst, outs.at[25 + len(extra)])
        cp.start()
        extra.append(cp)

    def full(b):
        res = []
        for ff in range(2):
            src = WB.at[b, ff]
            if b < 3:
                dst = wq_o.at[pl.ds(ff * U, U), pl.ds(b * 768, 768)]
            elif b == 3:
                dst = wo_o.at[pl.ds(ff * U, U), :]
            elif b < 8:
                dst = wu_o.at[pl.ds(ff * U, U), pl.ds((b - 4) * 768, 768)]
            else:
                dst = wd_o.at[pl.ds(ff * 1536 + (b - 8) * U, U), :]
            res.append(pltpu.make_async_copy(src, dst, outs.at[1 + 2 * b + ff]))
        return res

    def ready(b):
        loc(b).wait()
        C(b)
        for cp in full(b):
            cp.start()

    def vector(r):
        return jnp.concatenate([vec_o[0, r:r + 1, :], vec_o[1, r:r + 1, :]], 1)

    for b in range(3):
        for cp in full(b):
            cp.start()
    send_out(ATT, att_o)
    ready(3)
    bo = vector(2)
    for t in range(3):
        cs = slice(t * 256, (t + 1) * 256)
        w = WB[3, :, :, cs].reshape(768, 256)
        H1[:, cs] = XT[me, :, cs].astype(F32) + mm(ATT[...].astype(BF16), w) + bo[:, cs]
    g1, s1 = vector(3), vector(4)
    RB = 64

    def ln1(i, _):
        r = pl.ds(pl.multiple_of(i * RB, RB), RB)
        hat, inv = normal_parts(H1[r, :])
        H1[r, :] = hat
        n = hat * g1 + s1
        N1[r, :] = n
        N1B[r, :] = n.astype(BF16)
        LSE[r, 128:256] = jnp.broadcast_to(inv, (RB, 128))
        return 0
    lax.fori_loop(0, rows // RB, ln1, 0)
    send_out(H1, hat_o)
    send_out(LSE, lse_o)
    B(10)
    for b in range(4, 8):
        ready(b)

    def upblock(b, _):
        bias = jnp.concatenate([vec_o[b // 2, pl.ds(5 + lax.rem(b, 2) * 2, 1), :], vec_o[b // 2, pl.ds(6 + lax.rem(b, 2) * 2, 1), :]], 1)
        for t in range(3):
            w = WB[4 + b, :, :, t * 256:(t + 1) * 256].reshape(768, 256)
            cs = pl.ds(pl.multiple_of(b * 768 + t * 256, 256), 256)
            act, gp = gelu_pair(mm(N1B[...], w) + bias[:, t * 256:(t + 1) * 256])
            ACT[:, cs] = act.astype(BF16)
            GP[:, cs] = gp
        return 0
    lax.fori_loop(0, 2, upblock, 0)
    B(11)
    ready(8)
    ready(9)
    lax.fori_loop(2, 4, upblock, 0)
    send_out(ACT, act_o)
    send_out(GP, gp_o)
    for b in range(10, 12):
        ready(b)
    bd = vector(9)
    for t in range(3):
        cs = slice(t * 256, (t + 1) * 256)
        acc = N1[:, cs] + bd[:, cs]
        for ff in range(2):
            acc = acc + mm(ACT[:, ff * 1536:(ff + 1) * 1536], WB[8:12, ff, :, cs].reshape(1536, 256))
        N1[:, cs] = acc
    g2, s2 = vector(10), vector(11)
    tc.wait()

    def ln2(i, carry):
        r = pl.ds(pl.multiple_of(i * RB, RB), RB)
        hat, inv = normal_parts(N1[r, :])
        YB[r, :] = (hat * g2 + s2).astype(BF16)
        g = CT[r, :].astype(F32)
        N1[r, :] = normal_back(g, hat, inv, g2)
        return carry[0] + fold8(g * hat), carry[1] + fold8(g)
    zero = jnp.zeros((8, 768), F32)
    a0, a1 = lax.fori_loop(0, rows // RB, ln2, (zero, zero))
    send_out(YB, y_o)
    send_out(N1, dh_o)
    vg_o[0:1, :] = jnp.sum(a0, 0, keepdims=True)
    vg_o[1:2, :] = jnp.sum(a1, 0, keepdims=True)
    vcp.wait_send()
    qo.wait()
    for b in range(12):
        ycp(b).wait_send()
        zcp(b).wait_send()
        acp(b).wait_send()
        bcp(b).wait_send()
        for cp in full(b):
            cp.wait()
    for h in range(2):
        t_sib(h).wait_send()
        for j in range(1, nx):
            t_x(j, h).wait_send()
            t_f(j, h).wait_send()
    for cp in extra:
        cp.wait()


def forward_gather(lens, tok, cot, sq, so_, su, sd, small, nx, cid):
    seqs, seq_rows, d = tok.shape
    rows = seqs * seq_rows
    nblk = 2 * nx
    anyspec = pl.BlockSpec(memory_space=pl.ANY)
    vspec = pl.BlockSpec(memory_space=pltpu.VMEM)
    sspec = pl.BlockSpec(memory_space=pltpu.SMEM)
    D = pltpu.SemaphoreType.DMA
    V = pltpu.VMEM
    S = jax.ShapeDtypeStruct
    sems = [D((12,))] * 9 + [D((2,)), D((2,))] + [D((nx - 1, 2))] * 4 + [D((1,)), D((1,)), D((2,)), D((33,))]
    return pl.pallas_call(
        functools.partial(fwd_kernel, nx, seqs, seq_rows),
        out_shape=(S((3, nblk, rows, d), BF16), S((rows, d), F32), S((rows, 256), F32),
                   S((768, 2304), BF16), S((768, 768), BF16), S((768, 3072), BF16), S((3072, 768), BF16),
                   S((2, 12, U), F32), S((rows, d), BF16), S((rows, d), F32), S((rows, d), F32),
                   S((rows, 3072), BF16), S((rows, 3072), F32), S((2, d), F32)),
        in_specs=[sspec] + [anyspec] * 6 + [vspec] * 9,
        out_specs=(anyspec,) * 7 + (vspec,) + (anyspec,) * 5 + (vspec,),
        scratch_shapes=[V((nblk, rows, d), BF16), V((12, 2, U, 768), BF16), V((3, nblk, rows, d), BF16),
                        V((rows, d), BF16), V((rows, d), F32), V((rows, 256), F32), V((rows, d), F32), V((rows, d), F32),
                        V((rows, d), BF16), V((rows, 3072), BF16), V((rows, 3072), F32), V((rows, d), BF16)] + sems,
        compiler_params=pltpu.CompilerParams(collective_id=cid, has_side_effects=True, vmem_limit_bytes=62 << 20),
        name="forward_gather",
    )(lens, tok.reshape(rows, d), cot.reshape(rows, d), sq, so_, su, sd, *small)


def tn(a, b):
    return lax.dot_general(a, b, (((0,), (0,)), ((), ())), preferred_element_type=F32)


def colsum(v):
    return jnp.sum(fold8(v), 0, keepdims=True)


def bwd_kernel(nx, nd, seqs, seq_rows, lens, vec, vg, qkv_i, att_i, lse_i, wq_i, wo_i, wu_i, wd_i, dh_i, hat_i, act_i, gp_i, tok_i,
               od, ou, oo, oq, ov, gin_o,
               BIG, WO, WQ, GP, ACT, DH, DM, HAT, NB, DO, ROWS, COLS, DQKV, L, SB, R1, R2, R3, R4, AX, VV, V0, VX, VZ,
               lds, d0s, d0r, d1s, d1r, d2s, d2r, s1s, s1r, s2s, s2r, s3s, s3r, s4s, s4r, s5s, s5r, s6s, s6r, s7s, s7r, s8, vs, vr):
    core, x, f, z = places()
    me = x * 2 + core
    nblk = 2 * nx
    rows = seqs * seq_rows
    CX, PZ = U // nx, U // nx // nd
    NCH, READY = 12, 8
    sib = {"ctx": x * 2 + 1 - core}
    yp = {"fsdp": 1 - f}
    xps = [{"ctx": lax.rem(x + j, nx) * 2 + core} for j in range(1, nx)]
    xsrc = [lax.rem(x + nx - j, nx) * 2 + core for j in range(1, nx)]
    zps = [{"dp": lax.rem(z + j, nd)} for j in range(1, nd)]
    peers = [sib, yp] + xps + zps
    bar = pltpu.get_barrier_semaphore()
    for p in peers:
        pl.semaphore_signal(bar, inc=1, device_id=p, device_id_type=MESH)

    loads = {}

    def load(name, src, dst):
        cp = pltpu.make_async_copy(src, dst, lds.at[len(loads)])
        cp.start()
        loads[name] = cp

    load("dh", dh_i, DH)
    load("act", act_i, ACT)
    for b in range(4):
        load(("wd", b), wd_i.at[pl.ds(b * 768, 768)], BIG.at[pl.ds(b * 768, 768)])
        if b < 2:
            load("gp%d" % b, gp_i.at[:, pl.ds(b * 768, 768)], GP.at[b])
    load("hat", hat_i, HAT)
    for b in range(4):
        load(("wu", b), wu_i.at[:, pl.ds(b * 768, 768)], BIG.at[pl.ds(3072 + b * 768, 768)])
    load("lse", lse_i, COLS.at[:, pl.ds(0, 256)])
    load("wo", wo_i, WO)

    def vector(r):
        return jnp.concatenate([vec[0, r:r + 1, :], vec[1, r:r + 1, :]], 1)

    def c1(i, ff, k):
        return remote(SB.at[i % 4, ff], R1.at[i, ff], s1s.at[i, k], s1r.at[i, k], sib)

    def c1s(i):
        return [c1(i, 1 - f, 0), c1(i, f, 1)]

    def c2(c):
        return remote(L.at[c, 1 - f], R2.at[c], s2s.at[c], s2r.at[c], yp)

    def c3(c, j):
        xt = lax.rem(x + j, nx)
        return remote(L.at[c, f, pl.ds(pl.multiple_of(xt * CX, CX), CX)], R3.at[c, j - 1], s3s.at[c, j - 1], s3r.at[c, j - 1], xps[j - 1])

    def mine(zz):
        return pl.ds(pl.multiple_of(x * CX + zz * PZ, PZ), PZ)

    def c4(c, j):
        zt = lax.rem(z + j, nd)
        return remote(L.at[c, f, mine(zt)], R4.at[c, j - 1], s4s.at[c, j - 1], s4r.at[c, j - 1], zps[j - 1])

    def c5(c, j):
        w = AX.at[c, mine(z)]
        return remote(w, w, s5s.at[c, j - 1], s5r.at[c, j - 1], zps[j - 1])

    def c6(c, j):
        w = AX.at[c, pl.ds(pl.multiple_of(x * CX, CX), CX)]
        return remote(w, w, s6s.at[c, j - 1], s6r.at[c, j - 1], xps[j - 1])

    def qpart(i, cc):
        return cc if i == 9 else i - 8 + 2 * cc

    def orect(i):
        if i < 4:
            return od.at[pl.ds(pl.multiple_of(core * 768 + i // 2 * U, U), U), pl.ds(i % 2 * U, U)]
        if i < 8:
            return ou.at[:, pl.ds(pl.multiple_of(core * 1536 + (i - 4) * U, 128), U)]
        if i < 9:
            return oo.at[:, pl.ds(pl.multiple_of(core * U, 128), U)]
        return oq.at[:, pl.ds(pl.multiple_of(qpart(i, core) * U, 128), U)]

    def c7(c):
        return remote(AX.at[c], orect(c), s7s.at[c], s7r.at[c], sib)

    def c8(c):
        return pltpu.make_async_copy(AX.at[c], orect(c), s8.at[c])

    B = 48

    def rows_loop(n, fn):
        def bodyf(i, _):
            fn(pl.multiple_of(i * B, B))
            return 0
        lax.fori_loop(0, n // B, bodyf, 0)

    def up(v):
        return v.astype(F32)

    def st1(i):
        for cp in c1s(i):
            cp.start()

    def st2(c):
        c1(c, 1 - f, 0).wait_recv()

        def fn(r):
            s = pl.ds(r, B)
            L[c, 1 - f, s, :] = (up(L[c, 1 - f, s, :]) + up(R1[c, 1 - f, s, :])).astype(BF16)
        rows_loop(U, fn)
        c2(c).start()

    def st3(c):
        c1(c, f, 1).wait_recv()
        c2(c).wait_recv()
        for j in range(1, nx):
            xt = lax.rem(x + j, nx)

            def fn(r):
                s = pl.ds(pl.multiple_of(xt * CX + r, B), B)
                L[c, f, s, :] = (up(L[c, f, s, :]) + up(R1[c, f, s, :]) + up(R2[c, s, :])).astype(BF16)
            rows_loop(CX, fn)
            c3(c, j).start()

    def st4(c):
        for j in range(1, nx):
            c3(c, j).wait_recv()

        def fn(r):
            s = pl.ds(pl.multiple_of(x * CX + r, B), B)
            t = up(L[c, f, s, :]) + up(R1[c, f, s, :]) + up(R2[c, s, :])
            for j in range(1, nx):
                t = t + up(R3[c, j - 1, pl.ds(r, B), :])
            L[c, f, s, :] = t.astype(BF16)
        rows_loop(CX, fn)
        for j in range(1, nd):
            c4(c, j).start()

    def st5(c):
        for j in range(1, nd):
            c4(c, j).wait_recv()
        t = up(L[c, f, mine(z), :])
        for j in range(1, nd):
            t = t + up(R4[c, j - 1])
        AX[c, mine(z), :] = t.astype(BF16)
        for j in range(1, nd):
            c5(c, j).start()

    def st6(c):
        for j in range(1, nd):
            c5(c, j).wait_recv()
        for j in range(1, nx):
            c6(c, j).start()

    def st7(c):
        for j in range(1, nx):
            c6(c, j).wait_recv()
        c7(c).start()
        c8(c).start()

    def v_core():
        return remote(VV, V0.at[0], vs.at[0], vr.at[0], sib)

    def v_y():
        return remote(V0.at[1], V0.at[2], vs.at[1], vr.at[1], yp)

    def v_x(j):
        return remote(VX.at[x], VX.at[x], vs.at[1 + j], vr.at[1 + j], xps[j - 1])

    def v_z(j):
        return remote(VZ.at[z], VZ.at[z], vs.at[nx + j], vr.at[nx + j], zps[j - 1])

    def vst(k):
        if k == 0:
            v_core().start()
        elif k == 1:
            v_core().wait_recv()
            V0[1] = VV[...] + V0[0]
            v_y().start()
        elif k == 2:
            v_y().wait_recv()
            VX[x] = V0[1] + V0[2]
            for j in range(1, nx):
                v_x(j).start()
        elif k == 3:
            for j in range(1, nx):
                v_x(j).wait_recv()
            t = VX[0]
            for j in range(1, nx):
                t = t + VX[j]
            VZ[z] = t
            for j in range(1, nd):
                v_z(j).start()
        elif k == 4:
            for j in range(1, nd):
                v_z(j).wait_recv()
            t = VZ[0]
            for j in range(1, nd):
                t = t + VZ[j]
            VV2 = t
            for r, n, o in ((0, 1, 0), (2, 1, 1), (4, 1, 2), (6, 1, 3), (8, 1, 4), (10, 4, 5), (18, 1, 9), (20, 1, 10), (22, 1, 11)):
                ov[o:o + n, :] = jnp.where(f == 0, VV2[r:r + n, :], VV2[r + n:r + 2 * n, :])

    def put_vec(r, v):
        VV[r:r + 1, :] = v[:, :U]
        VV[r + 1:r + 2, :] = v[:, U:]

    put_vec(20, vg[0:1, :])
    put_vec(22, vg[1:2, :])

    RB = 64
    loads["dh"].wait()

    def to_dm(i, acc):
        r = pl.ds(pl.multiple_of(i * RB, RB), RB)
        v = DH[r, :].astype(BF16)
        DM[r, :] = v
        return acc + fold8(v.astype(F32))
    zero = jnp.zeros((8, 768), F32)
    put_vec(18, jnp.sum(lax.fori_loop(0, rows // RB, to_dm, zero), 0, keepdims=True))

    def fill(i0, kk, ff, val, wide):
        v = val.astype(BF16)
        for t in range(wide):
            if kk == 0:
                L[i0 + t, ff] = v[:, t * U:(t + 1) * U]
            else:
                SB[(i0 + t) % 4, ff] = v[:, t * U:(t + 1) * U]

    def each_f(fn):
        def one(k, _):
            fn(jnp.where(k == 0, 1 - f, f))
            return 0
        lax.fori_loop(0, 2, one, 0)

    def ccof(kk):
        return core if kk == 0 else 1 - core

    pl.semaphore_wait(bar, len(peers))
    loads["act"].wait()
    for ii in range(2):
        for kk in (1, 0):
            def wdown(ff, kk=kk, ii=ii):
                h = pl.multiple_of(ff * 1536 + ccof(kk) * 768 + ii * U, U)
                fill(2 * ii, kk, ff, tn(ACT[:, pl.ds(h, U)], DM[...]), 2)
            each_f(wdown)
            if kk == 1:
                st1(2 * ii)
                st1(2 * ii + 1)
                if ii == 1:
                    st2(0)
                    st2(1)
    st2(2)
    for b in range(4):
        loads[("wd", b)].wait()
        loads["gp%d" % b].wait()
        for t in range(3):
            h = b * 768 + t * 256
            du = (nt(DM[...], BIG[h:h + 256, :]) * GP[b % 2, :, t * 256:(t + 1) * 256]).astype(BF16)
            WQ[b * rows:(b + 1) * rows, t * 256:(t + 1) * 256] = du
            s = colsum(du.astype(F32))
            for q in range(2):
                o = h + q * 128
                VV[10 + o // U:11 + o // U, o % U:o % U + 128] = s[:, q * 128:(q + 1) * 128]
        if b < 2:
            load("gp%d" % (b + 2), gp_i.at[:, pl.ds((b + 2) * 768, 768)], GP.at[b % 2])
    st2(3)
    loads["hat"].wait()
    g1, s1 = vector(3), vector(4)
    for b in range(4):
        loads[("wu", b)].wait()
    for t in range(3):
        cs = slice(t * 256, (t + 1) * 256)
        acc = DH[:, cs]
        for b in range(4):
            acc = acc + nt(WQ[b * rows:(b + 1) * rows, :], BIG[3072 + b * 768 + t * 256:3072 + b * 768 + (t + 1) * 256, :])
        DH[:, cs] = acc
    for k in (1, 2, 0):
        for blk in range(nblk):
            load(("qkv", k, blk), qkv_i.at[k, blk], BIG.at[pl.ds((k * nblk + blk) * rows, rows)])
    st3(0)
    loads["lse"].wait()

    def ln1(i, carry):
        r = pl.ds(pl.multiple_of(i * RB, RB), RB)
        dn, hat = DH[r, :], HAT[r, :]
        d = normal_back(dn, hat, COLS[r, 128:129], g1)
        DH[r, :] = d
        da = d.astype(BF16)
        DQKV[0, r, :] = da
        NB[r, :] = (hat * g1 + s1).astype(BF16)
        return carry[0] + fold8(dn * hat), carry[1] + fold8(dn), carry[2] + fold8(da.astype(F32))
    sums = lax.fori_loop(0, rows // RB, ln1, (zero, zero, zero))
    for row, sv in zip((6, 8, 4), sums):
        put_vec(row, jnp.sum(sv, 0, keepdims=True))
    load("att", att_i, HAT)
    loads["wo"].wait()
    for t in range(3):
        DO[me, :, t * 256:(t + 1) * 256] = nt(DQKV[0], WO[t * 256:(t + 1) * 256, :]).astype(BF16)

    def d_sib():
        return remote(DO.at[me], DO.at[me], d0s.at[0], d0r.at[0], sib)

    def d_x(j):
        return remote(DO.at[me], DO.at[me], d1s.at[j - 1, 0], d1r.at[j - 1, 0], xps[j - 1])

    def d_f(j):
        w = DO.at[xsrc[j - 1]]
        return remote(w, w, d2s.at[j - 1, 0], d2r.at[j - 1, 0], sib)

    def r_sib():
        return remote(ROWS.at[me], ROWS.at[me], d0s.at[1], d0r.at[1], sib)

    def r_x(j):
        return remote(ROWS.at[me], ROWS.at[me], d1s.at[j - 1, 1], d1r.at[j - 1, 1], xps[j - 1])

    def r_f(j):
        w = ROWS.at[xsrc[j - 1]]
        return remote(w, w, d2s.at[j - 1, 1], d2r.at[j - 1, 1], sib)

    for j in range(1, nx):
        d_x(j).start()
    d_sib().start()
    loads["att"].wait()
    head = lax.broadcasted_iota(jnp.int32, (768, 128), 0) // HW
    pick = (head == lax.broadcasted_iota(jnp.int32, (768, 128), 1)).astype(BF16)

    def delta(i, _):
        r = pl.ds(pl.multiple_of(i * 128, 128), 128)
        v = DO[me, r, :].astype(F32) * HAT[r, :]
        hi = v.astype(BF16)
        rest = v - hi.astype(F32)
        mid = rest.astype(BF16)
        low = (rest - mid.astype(F32)).astype(BF16)
        d = mm(hi, pick) + mm(mid, pick) + mm(low, pick)
        COLS[r, 128:256] = d
        ROWS[me, 16:32, r] = jnp.transpose(d)[0:16, :]
        ROWS[me, 0:16, r] = jnp.transpose(COLS[r, 0:128])[0:16, :]
        return 0
    lax.fori_loop(0, rows // 128, delta, 0)
    for j in range(1, nx):
        r_x(j).start()
    r_sib().start()
    for ii in range(2):
        for kk in (1, 0):
            if kk == 1:
                for i in (2 * ii, 2 * ii + 1):
                    for cp in c1s(i):
                        cp.wait_send()

            def wup(ff, kk=kk, ii=ii):
                h = pl.multiple_of((ccof(kk) * 2 + ii) * rows, rows)
                fill(4 + 2 * ii, kk, ff, tn(NB[:, pl.ds(pl.multiple_of(ff * U, U), U)], WQ[pl.ds(h, rows), :]), 2)
            each_f(wup)
            if kk == 1:
                st1(4 + 2 * ii)
                st1(5 + 2 * ii)
                if ii == 1:
                    st2(4)
                    st2(5)
    load("tok", tok_i, NB)
    for b in range(3):
        load(("wq", b), wq_i.at[:, pl.ds(b * 768, 768)], WQ.at[pl.ds(b * 768, 768)])
    st3(1)
    st2(6)
    for kk in (1, 0):
        if kk == 1:
            for cp in c1s(4):
                cp.wait_send()

        def wout(ff, kk=kk):
            a = HAT[:, pl.ds(pl.multiple_of(ff * U, U), U)].astype(BF16)
            fill(8, kk, ff, tn(a, DQKV[0, :, pl.ds(pl.multiple_of(ccof(kk) * U, U), U)]), 1)
        each_f(wout)
        if kk == 1:
            st1(8)
    st2(7)
    st2(8)
    for k in (1, 2, 0):
        for blk in range(nblk):
            loads[("qkv", k, blk)].wait()
    low_half = head_masks(QT)
    lane128 = lax.broadcasted_iota(jnp.int32, (QT, 128), 1)
    kpos = lax.broadcasted_iota(jnp.int32, (QT, QT), 1)
    krow = lax.broadcasted_iota(jnp.int32, (QT, 128), 0)
    nr = seq_rows // QT
    ntile = rows // QT

    def big(k, blk, r0, cols):
        return BIG[pl.ds(pl.multiple_of((k * nblk + blk) * rows + r0, QT), QT), cols]

    def pick_col(v, h):
        return jnp.sum(jnp.where(lane128 == h, v, 0.0), 1, keepdims=True)

    def zero_other(v, h):
        return jnp.where(low_half == (h == 0), v, jnp.zeros_like(v))

    def dq_one(it):
        tile, j = it // 6, lax.rem(it, 6)
        s0 = tile // nr
        q0 = pl.multiple_of(tile * QT, QT)
        qr = pl.ds(q0, QT)
        cols = pl.ds(pl.multiple_of(j * 128, 128), 128)
        q = big(0, me, q0, cols)
        do = DO[me, qr, cols]
        length = lens[s0]
        res = []
        for h in range(2):
            qh, doh = zero_other(q, h), zero_other(do, h)
            lse = pick_col(COLS[qr, 0:128], 2 * j + h)
            dl = pick_col(COLS[qr, 128:256], 2 * j + h)
            acc = None
            for blk in range(nblk):
                for r in range(nr):
                    k0 = s0 * seq_rows + r * QT
                    kt = big(1, blk, k0, cols)
                    p = jnp.exp(nt(qh, kt) - lse)
                    p = jnp.where(kpos < length - (blk * seq_rows + r * QT), p, 0.0)
                    ds = (p * (nt(doh, big(2, blk, k0, cols)) - dl)).astype(BF16)
                    o = mm(ds, kt)
                    acc = o if acc is None else acc + o
            res.append(acc)
        DQKV[0, qr, cols] = (jnp.where(low_half, res[0], res[1]) * 0.125).astype(BF16)

    def dkv_one(it):
        tile, j = lax.rem(it, ntile), it // ntile
        s0 = tile // nr
        k0 = pl.multiple_of(tile * QT, QT)
        kr = pl.ds(k0, QT)
        cols = pl.ds(pl.multiple_of(j * 128, 128), 128)
        k, v = big(1, me, k0, cols), big(2, me, k0, cols)
        live = krow < lens[s0] - (me * seq_rows + (tile - s0 * nr) * QT)
        resk, resv = [], []
        for h in range(2):
            kh, vh = zero_other(k, h), zero_other(v, h)
            ak = av = None
            for blk in range(nblk):
                for r in range(nr):
                    q0 = pl.multiple_of(s0 * seq_rows + r * QT, QT)
                    qr = pl.ds(q0, QT)
                    qt, dt = big(0, blk, q0, cols), DO[blk, qr, cols]
                    lse = ROWS[blk, pl.ds(2 * j + h, 1), qr]
                    dl = ROWS[blk, pl.ds(16 + 2 * j + h, 1), qr]
                    p = jnp.exp(nt(kh, qt) - lse)
                    ds = (p * (nt(vh, dt) - dl)).astype(BF16)
                    ov_, ok_ = mm(p.astype(BF16), dt), mm(ds, qt)
                    av = ov_ if av is None else av + ov_
                    ak = ok_ if ak is None else ak + ok_
            resk.append(ak)
            resv.append(av)
        DQKV[1, kr, cols] = jnp.where(live, jnp.where(low_half, resk[0], resk[1]), 0.0).astype(BF16)
        DQKV[2, kr, cols] = jnp.where(live, jnp.where(low_half, resv[0], resv[1]), 0.0).astype(BF16)

    def segment(fn, base, count, hooks):
        per = count // len(hooks)

        def group(g, _):
            def one(i, _):
                fn(base + g * per + i)
                return 0
            lax.fori_loop(0, per, one, 0)
            for k, steps in enumerate(hooks):
                @pl.when(g == k)
                def _(steps=steps):
                    for step, arg in steps:
                        step(*arg)
            return 0
        lax.fori_loop(0, len(hooks), group, 0)

    def relay():
        for j in range(1, nx):
            d_x(j).wait_recv()
            d_f(j).start()
            r_x(j).wait_recv()
            r_f(j).start()

    def bias_sum(k):
        def one(i, acc):
            return acc + fold8(DQKV[k, pl.ds(pl.multiple_of(i * RB, RB), RB), :].astype(F32))
        return jnp.sum(lax.fori_loop(0, rows // RB, one, zero), 0, keepdims=True)

    def project(i):
        for cp in c1s(i - 4):
            cp.wait_send()
        for kk in (1, 0):
            def wqkv(ff, kk=kk):
                p = qpart(i, ccof(kk))
                a = NB[:, pl.ds(pl.multiple_of(ff * U, U), U)]
                fill(i, kk, ff, tn(a, DQKV[p // 2, :, pl.ds(pl.multiple_of(lax.rem(p, 2) * U, U), U)]), 1)
            each_f(wqkv)
            if kk == 1:
                st1(i)

    segment(dq_one, 0, ntile * 6, (((st3, (2,)), (st4, (0,)), ),
             ((st3, (3,)), ),
             (),
             ((st5, (0,)), (relay, ()), ),
             ((st3, (4,)), (st4, (1,)), ),
             ((st3, (5,)), (st6, (0,)), (st4, (2,)), ),))
    loads["tok"].wait()
    project(9)
    put_vec(0, bias_sum(0))
    st2(9)
    d_sib().wait_recv()
    r_sib().wait_recv()
    for j in range(1, nx):
        d_f(j).wait_recv()
        r_f(j).wait_recv()
    segment(dkv_one, 0, ntile * 3, (((st4, (3,)), (st5, (1,)), ),
             ((st3, (6,)), (st5, (2,)), (st4, (4,)), ),
             ((st3, (7,)), (st5, (3,)), (st6, (1,)), (st4, (5,)), ),))
    project(10)
    st2(10)
    segment(dkv_one, ntile * 3, ntile * 3, (((st6, (2,)), (st5, (4,)), ),
             ((st3, (8,)), (st5, (5,)), (st4, (6,)), (st6, (3,)), ),
             ((st3, (9,)), (st4, (7,)), (st6, (4,)), ),))
    put_vec(2, bias_sum(2))
    vst(0)
    project(11)
    vst(1)
    st2(11)
    st5(6)
    st6(5)
    for b in range(3):
        loads[("wq", b)].wait()
    for t in range(3):
        cs = slice(t * 256, (t + 1) * 256)
        acc = DH[:, cs]
        for b in range(3):
            acc = acc + nt(DQKV[b], WQ[b * 768 + t * 256:b * 768 + (t + 1) * 256, :])
        DM[:, cs] = acc.astype(BF16)
    gout = pltpu.make_async_copy(DM, gin_o, s8.at[NCH])
    gout.start()
    st4(8)
    st5(7)
    st6(6)
    vst(2)
    st3(10)
    st4(9)
    st7(0)
    st7(1)
    st7(2)
    st5(8)
    st6(7)
    vst(3)
    st7(3)
    st7(4)
    st3(11)
    st4(10)
    st5(9)
    st6(8)
    vst(4)
    st7(5)
    st7(6)
    st4(11)
    st5(10)
    st6(9)
    st7(7)
    st5(11)
    st6(10)
    st7(8)
    st6(11)
    st7(9)
    st7(10)
    st7(11)
    for c in range(NCH):
        c2(c).wait_send()
        c7(c).wait()
        c8(c).wait()
        for j in range(1, nx):
            c3(c, j).wait_send()
            c6(c, j).wait_send()
        for j in range(1, nd):
            c4(c, j).wait_send()
            c5(c, j).wait_send()
    for i in (8, 9, 10, 11):
        for cp in c1s(i):
            cp.wait_send()
    gout.wait()
    v_core().wait_send()
    v_y().wait_send()
    d_sib().wait_send()
    r_sib().wait_send()
    for j in range(1, nx):
        v_x(j).wait_send()
        d_x(j).wait_send()
        d_f(j).wait_send()
        r_x(j).wait_send()
        r_f(j).wait_send()
    for j in range(1, nd):
        v_z(j).wait_send()


def backward_reduce(lens, vec, vg, qkv, att, lse, wq, wo, wu, wd, dh, hat, act, gp, tok, nx, nd, seqs, cid):
    rows, d = att.shape
    nblk = 2 * nx
    CX, PZ = U // nx, U // nx // nd
    N = 12
    anyspec = pl.BlockSpec(memory_space=pl.ANY)
    vspec = pl.BlockSpec(memory_space=pltpu.VMEM)
    sspec = pl.BlockSpec(memory_space=pltpu.SMEM)
    D = pltpu.SemaphoreType.DMA
    V = pltpu.VMEM
    S = jax.ShapeDtypeStruct
    sems = [D((40,)), D((2,)), D((2,))] + [D((nx - 1, 2))] * 4 + [D((N, 2)), D((N, 2)), D((N,)), D((N,)), D((N, nx - 1)), D((N, nx - 1)),
            D((N, nd - 1)), D((N, nd - 1)), D((N, nd - 1)), D((N, nd - 1)), D((N, nx - 1)), D((N, nx - 1)),
            D((N,)), D((N,)), D((N + 1,)), D((nx + nd,)), D((nx + nd,))]
    return pl.pallas_call(
        functools.partial(bwd_kernel, nx, nd, seqs, rows // seqs),
        out_shape=(S((1536, 768), BF16), S((U, 3072), BF16), S((U, 768), BF16), S((U, 2304), BF16), S((12, U), F32), S((rows, d), BF16)),
        in_specs=[sspec, vspec, vspec] + [anyspec] * 12,
        out_specs=(anyspec,) * 4 + (vspec, anyspec),
        scratch_shapes=[V((6144, d), BF16), V((d, d), BF16), V((3 * d, d), BF16), V((2, rows, d), F32), V((rows, 3072), BF16),
                        V((rows, d), F32), V((rows, d), BF16), V((rows, d), F32), V((rows, d), BF16), V((nblk, rows, d), BF16),
                        V((nblk, 32, rows), F32), V((rows, 256), F32), V((3, rows, d), BF16),
                        V((N, 2, U, U), BF16), V((4, 2, U, U), BF16), V((N, 2, U, U), BF16), V((N, U, U), BF16),
                        V((N, nx - 1, CX, U), BF16), V((N, nd - 1, PZ, U), BF16), V((N, U, U), BF16),
                        V((24, U), F32), V((3, 24, U), F32), V((nx, 24, U), F32), V((nd, 24, U), F32)] + sems,
        compiler_params=pltpu.CompilerParams(collective_id=cid, has_side_effects=True, vmem_limit_bytes=63 << 20),
        name="backward_reduce",
    )(lens, vec, vg, qkv, att, lse, wq, wo, wu, wd, dh, hat, act, gp, tok)


def fast_body(
    tokens, cotangent, lengths, w_qkv, bias_q, bias_v, w_out, bias_out, gain_one, shift_one,
    w_up, bias_up, w_down, bias_down, gain_two, shift_two,
):
    seqs, seq_rows, width = tokens.shape
    nx, nd = lax.axis_size("ctx") // 2, lax.axis_size("dp")
    small = [bias_q, bias_v, bias_out, gain_one, shift_one, bias_up, bias_down, gain_two, shift_two]
    (qkv, att, lse, wq, wo, wu, wd, vec, out, dh, hat, act, gp, vg) = forward_gather(
        lengths, tokens, cotangent, w_qkv, w_out, w_up, w_down, small, nx, 2
    )
    t_down, t_up, t_out, t_qkv, t_vec, grad_in = backward_reduce(
        lengths, vec, vg, qkv, att, lse, wq, wo, wu, wd, dh, hat, act, gp,
        tokens.reshape(seqs * seq_rows, width), nx, nd, seqs, 3
    )

    def part(first, count):
        return t_vec[first : first + count].reshape(-1)

    return (
        out.reshape(tokens.shape), grad_in.reshape(tokens.shape), t_qkv.astype(F32), part(0, 1), part(1, 1),
        t_out.astype(F32), part(2, 1), part(3, 1), part(4, 1), t_up.astype(F32), part(5, 4),
        t_down.astype(F32), part(9, 1), part(10, 1), part(11, 1),
    )


def solution(mesh):
    return jax.shard_map(
        fast_body if mesh.shape["ctx"] <= 4 else general_body,
        mesh=mesh,
        in_specs=(
            P(("dp", "fsdp"), "ctx", None),
            P(("dp", "fsdp"), "ctx", None),
            P(("dp", "fsdp")),
            P("fsdp", None),
            P("fsdp"),
            P("fsdp"),
            P("fsdp", None),
            P("fsdp"),
            P("fsdp"),
            P("fsdp"),
            P("fsdp", None),
            P("fsdp"),
            P("fsdp", None),
            P("fsdp"),
            P("fsdp"),
            P("fsdp"),
        ),
        out_specs=(
            P(("dp", "fsdp"), "ctx", None),
            P(("dp", "fsdp"), "ctx", None),
            P("fsdp", None),
            P("fsdp"),
            P("fsdp"),
            P("fsdp", None),
            P("fsdp"),
            P("fsdp"),
            P("fsdp"),
            P("fsdp", None),
            P("fsdp"),
            P("fsdp", None),
            P("fsdp"),
            P("fsdp"),
            P("fsdp"),
        ),
        check_vma=False,
    )
```

```python
import functools
import math

import jax
import jax.numpy as jnp
from jax import lax
from jax.experimental import pallas as pl
from jax.experimental.pallas import tpu as pltpu
from jax.sharding import PartitionSpec as P

MESH = pl.DeviceIdType.MESH
F32, BF16 = jnp.float32, jnp.bfloat16
U = 384
VR = 24


def places():
    c = lax.axis_index("ctx")
    return lax.rem(c, 2), c // 2, lax.axis_index("fsdp"), lax.axis_index("dp")


def grad_kernel(nx, nd, grp, wd, wu, wo, wq, vec, od, ou, oo, oq, ov,
                L, R1, R2, R3, R4, AX, AC, ST, V0, VX, VZ,
                s0, s1s, s1r, s2s, s2r, s3s, s3r, s4s, s4r, s5s, s5r, s6s, s6r, s7s, s7r, so, vs, vr):
    core, x, f, z = places()
    nch = 12 // grp
    CH, CX, PZ = U * grp, U * grp // nx, U * grp // nx // nd
    sib = {"ctx": x * 2 + 1 - core}
    yp = {"fsdp": 1 - f}
    xps = [{"ctx": lax.rem(x + j, nx) * 2 + core} for j in range(1, nx)]
    zps = [{"dp": lax.rem(z + j, nd)} for j in range(1, nd)]
    peers = [sib, yp] + xps + zps
    bar = pltpu.get_barrier_semaphore()
    for p in peers:
        pl.semaphore_signal(bar, inc=1, device_id=p, device_id_type=MESH)

    def rect(i, ff, cc):
        if i < 4:
            return wd, ff * 1536 + i * U, cc * U
        if i < 8:
            return wu, ff * U, cc * 1536 + (i - 4) * U
        if i < 9:
            return wo, ff * U, cc * U
        return wq, ff * U, cc * 1152 + (i - 9) * U

    def orect(i, cc):
        if i < 4:
            return od, i * U, cc * U
        if i < 8:
            return ou, 0, cc * 1536 + (i - 4) * U
        if i < 9:
            return oo, 0, cc * U
        return oq, 0, cc * 1152 + (i - 9) * U

    def sl(ref, r, c):
        return ref.at[pl.ds(pl.multiple_of(r, U), U), pl.ds(pl.multiple_of(c, 128), U)]

    def local(i, k):
        ff = (1 - f) if k == 0 else f
        return pltpu.make_async_copy(sl(*rect(i, ff, core)), L.at[i // grp, ff, pl.ds(i % grp * U, U)], s0.at[i, k])

    def remote(src, dst, ss, rs, dev):
        return pltpu.make_async_remote_copy(src_ref=src, dst_ref=dst, send_sem=ss, recv_sem=rs, device_id=dev, device_id_type=MESH)

    def c1(i, k):
        ff = (1 - f) if k == 0 else f
        return remote(sl(*rect(i, ff, 1 - core)), R1.at[i // grp, ff, pl.ds(i % grp * U, U)], s1s.at[i, k], s1r.at[i, k], sib)

    def c2(c):
        return remote(L.at[c, 1 - f], R2.at[c], s2s.at[c], s2r.at[c], yp)

    def c3(c, j):
        xt = lax.rem(x + j, nx)
        return remote(L.at[c, f, pl.ds(pl.multiple_of(xt * CX, CX), CX)], R3.at[c, j - 1], s3s.at[c, j - 1], s3r.at[c, j - 1], xps[j - 1])

    def mine(c, zz):
        return pl.ds(pl.multiple_of(x * CX + zz * PZ, PZ), PZ)

    def c4(c, j):
        zt = lax.rem(z + j, nd)
        return remote(L.at[c, f, mine(c, zt)], R4.at[c, j - 1], s4s.at[c, j - 1], s4r.at[c, j - 1], zps[j - 1])

    def c5(c, j):
        return remote(AX.at[c, mine(c, z)], AX.at[c, mine(c, z)], s5s.at[c, j - 1], s5r.at[c, j - 1], zps[j - 1])

    def c6(c, j):
        rows = pl.ds(pl.multiple_of(x * CX, CX), CX)
        return remote(AX.at[c, rows], AX.at[c, rows], s6s.at[c, j - 1], s6r.at[c, j - 1], xps[j - 1])

    def c7(c):
        return remote(AX.at[c], AC.at[c], s7s.at[c], s7r.at[c], sib)

    B = 48

    def rows_loop(n, fn):
        def bodyf(i, _):
            fn(pl.multiple_of(i * B, B))
            return 0
        lax.fori_loop(0, n // B, bodyf, 0)

    def up(v):
        return v.astype(F32)

    def st2(c):
        for k in range(grp):
            local(c * grp + k, 0).wait()
            c1(c * grp + k, 0).wait_recv()

        def fn(r):
            s = pl.ds(r, B)
            L[c, 1 - f, s, :] = (up(L[c, 1 - f, s, :]) + up(R1[c, 1 - f, s, :])).astype(BF16)
        rows_loop(CH, fn)
        c2(c).start()

    def st3(c):
        for k in range(grp):
            local(c * grp + k, 1).wait()
            c1(c * grp + k, 1).wait_recv()
        c2(c).wait_recv()
        for j in range(1, nx):
            xt = lax.rem(x + j, nx)

            def fn(r):
                s = pl.ds(pl.multiple_of(xt * CX + r, B), B)
                L[c, f, s, :] = (up(L[c, f, s, :]) + up(R1[c, f, s, :]) + up(R2[c, s, :])).astype(BF16)
            rows_loop(CX, fn)
            c3(c, j).start()

    def st4(c):
        for j in range(1, nx):
            c3(c, j).wait_recv()

        def fn(r):
            s = pl.ds(pl.multiple_of(x * CX + r, B), B)
            t = up(L[c, f, s, :]) + up(R1[c, f, s, :]) + up(R2[c, s, :])
            for j in range(1, nx):
                t = t + up(R3[c, j - 1, pl.ds(r, B), :])
            L[c, f, s, :] = t.astype(BF16)
        rows_loop(CX, fn)
        for j in range(1, nd):
            c4(c, j).start()

    def st5(c):
        for j in range(1, nd):
            c4(c, j).wait_recv()
        t = up(L[c, f, mine(c, z), :])
        for j in range(1, nd):
            t = t + up(R4[c, j - 1])
        AX[c, mine(c, z), :] = t.astype(BF16)
        for j in range(1, nd):
            c5(c, j).start()

    def st6(c):
        for j in range(1, nd):
            c5(c, j).wait_recv()
        for j in range(1, nx):
            c6(c, j).start()

    def outc(i, k, slot):
        cc = core if k == 0 else 1 - core
        return pltpu.make_async_copy(ST.at[slot], sl(*orect(i, cc)), so.at[slot])

    def emit(i, k, src):
        slot = emit.n % 4
        if emit.n >= 4:
            outc(*emit.log[emit.n - 4], slot).wait()
        off = i % grp * U

        def fn(r):
            ST[slot, pl.ds(r, B), :] = up(src[i // grp, pl.ds(pl.multiple_of(off + r, B), B), :])
        rows_loop(U, fn)
        outc(i, k, slot).start()
        emit.log.append((i, k))
        emit.n += 1
    emit.n = 0
    emit.log = []

    def st7(c):
        for j in range(1, nx):
            c6(c, j).wait_recv()
        c7(c).start()
        for k in range(grp):
            emit(c * grp + k, 0, AX)

    def st8(c):
        c7(c).wait_recv()
        for k in range(grp):
            emit(c * grp + k, 1, AC)

    def v_core():
        return remote(vec, V0.at[0], vs.at[0], vr.at[0], sib)

    def v_y():
        return remote(V0.at[1], V0.at[2], vs.at[1], vr.at[1], yp)

    def v_x(j):
        return remote(VX.at[x], VX.at[x], vs.at[1 + j], vr.at[1 + j], xps[j - 1])

    def v_z(j):
        return remote(VZ.at[z], VZ.at[z], vs.at[nx + j], vr.at[nx + j], zps[j - 1])

    def vst(k):
        if k == 0:
            v_core().start()
        elif k == 1:
            v_core().wait_recv()
            V0[1] = vec[...] + V0[0]
            v_y().start()
        elif k == 2:
            v_y().wait_recv()
            VX[x] = V0[1] + V0[2]
            for j in range(1, nx):
                v_x(j).start()
        elif k == 3:
            for j in range(1, nx):
                v_x(j).wait_recv()
            t = VX[0]
            for j in range(1, nx):
                t = t + VX[j]
            VZ[z] = t
            for j in range(1, nd):
                v_z(j).start()
        elif k == 4:
            for j in range(1, nd):
                v_z(j).wait_recv()
            t = VZ[0]
            for j in range(1, nd):
                t = t + VZ[j]
            ov[...] = t

    for i in range(12):
        local(i, 0).start()
    pl.semaphore_wait(bar, len(peers))
    for i in range(12):
        c1(i, 0).start()
    vst(0)
    for i in range(12):
        local(i, 1).start()
        c1(i, 1).start()
    stages = [(8, st8), (7, st7), (6, st6), (5, st5), (4, st4), (3, st3)]
    for t in range(nch + 8):
        if t < nch:
            st2(t)
        if 1 <= t <= 4:
            vst(t)
        for k, fn in stages:
            c = t - (k - 1)
            if 0 <= c < nch:
                fn(c)
    n = emit.n
    for q in range(max(0, n - 4), n):
        outc(*emit.log[q], q % 4).wait()
    for i in range(12):
        for k in range(2):
            c1(i, k).wait_send()
    for c in range(nch):
        c2(c).wait_send()
        c7(c).wait_send()
        for j in range(1, nx):
            c3(c, j).wait_send()
            c6(c, j).wait_send()
        for j in range(1, nd):
            c4(c, j).wait_send()
            c5(c, j).wait_send()
    v_core().wait_send()
    v_y().wait_send()
    for j in range(1, nx):
        v_x(j).wait_send()
    for j in range(1, nd):
        v_z(j).wait_send()


def grad_reduce(wd, wu, wo, wq, vec, nx, nd, cid):
    grp = nx * nd // 8
    nch = 12 // grp
    CH, CX, PZ = U * grp, U * grp // nx, U * grp // nx // nd
    anyspec = pl.BlockSpec(memory_space=pl.ANY)
    vspec = pl.BlockSpec(memory_space=pltpu.VMEM)
    D = pltpu.SemaphoreType.DMA
    V = pltpu.VMEM
    sems = [D((12, 2)), D((12, 2)), D((12, 2)), D((nch,)), D((nch,)), D((nch, nx - 1)), D((nch, nx - 1)),
            D((nch, nd - 1)), D((nch, nd - 1)), D((nch, nd - 1)), D((nch, nd - 1)), D((nch, nx - 1)), D((nch, nx - 1)),
            D((nch,)), D((nch,)), D((4,)), D((nx + nd,)), D((nx + nd,))]
    return pl.pallas_call(
        functools.partial(grad_kernel, nx, nd, grp),
        out_shape=(jax.ShapeDtypeStruct((1536, 768), F32), jax.ShapeDtypeStruct((U, 3072), F32),
                   jax.ShapeDtypeStruct((U, 768), F32), jax.ShapeDtypeStruct((U, 2304), F32),
                   jax.ShapeDtypeStruct((VR, U), F32)),
        in_specs=[anyspec] * 4 + [vspec],
        out_specs=(anyspec,) * 4 + (vspec,),
        scratch_shapes=[V((nch, 2, CH, U), BF16), V((nch, 2, CH, U), BF16), V((nch, CH, U), BF16),
                        V((nch, nx - 1, CX, U), BF16), V((nch, nd - 1, PZ, U), BF16),
                        V((nch, CH, U), BF16), V((nch, CH, U), BF16), V((4, U, U), F32),
                        V((3, VR, U), F32), V((nx, VR, U), F32), V((nd, VR, U), F32)] + sems,
        compiler_params=pltpu.CompilerParams(collective_id=cid, has_side_effects=True, vmem_limit_bytes=60 << 20),
        name="grad_reduce",
    )(wd, wu, wo, wq, vec)


HEADS = 12


EPSILON = 1e-12
MASKED = -1e30


def shifted(value, axis, steps):
    count = lax.axis_size(axis)
    pairs = [(source, (source + steps) % count) for source in range(count)]
    return lax.ppermute(value, axis, pairs)


def normalize(values, norm_gain, norm_shift):
    row_mean = jnp.mean(values, -1, keepdims=True)
    centred = values - row_mean
    spread = jnp.mean(centred * centred, -1, keepdims=True)
    return centred * lax.rsqrt(spread + EPSILON) * norm_gain + norm_shift


def gelu_exact(values):
    return jax.nn.gelu(values, approximate=False)


def row_dot(left_op, right_op):
    return jnp.dot(left_op, right_op, preferred_element_type=jnp.float32)


def left_dot(left_op, right_op):
    return lax.dot_general(
        left_op, right_op, (((0,), (0,)), ((), ())), preferred_element_type=jnp.float32
    )


def right_dot(left_op, right_op):
    return lax.dot_general(
        left_op, right_op, (((1,), (1,)), ((), ())), preferred_element_type=jnp.float32
    )


def general_body(
    tokens,
    cotangent,
    lengths,
    w_qkv,
    bias_q,
    bias_v,
    w_out,
    bias_out,
    gain_one,
    shift_one,
    w_up,
    bias_up,
    w_down,
    bias_down,
    gain_two,
    shift_two,
):
    seq_count, block_rows, model_width = tokens.shape
    head_count = HEADS
    head_dim = model_width // head_count
    all_rows = seq_count * block_rows
    score_scale = head_dim ** (-0.5)
    cycle_size = lax.axis_size("ctx")
    cycle_index = lax.axis_index("ctx")
    gathered = (
        lax.all_gather(w_qkv, "fsdp", axis=0, tiled=True),
        lax.all_gather(bias_q, "fsdp", axis=0, tiled=True),
        lax.all_gather(bias_v, "fsdp", axis=0, tiled=True),
        lax.all_gather(w_out, "fsdp", axis=0, tiled=True),
        lax.all_gather(bias_out, "fsdp", axis=0, tiled=True),
        lax.all_gather(gain_one, "fsdp", axis=0, tiled=True),
        lax.all_gather(shift_one, "fsdp", axis=0, tiled=True),
        lax.all_gather(w_up, "fsdp", axis=0, tiled=True),
        lax.all_gather(bias_up, "fsdp", axis=0, tiled=True),
        lax.all_gather(w_down, "fsdp", axis=0, tiled=True),
        lax.all_gather(bias_down, "fsdp", axis=0, tiled=True),
        lax.all_gather(gain_two, "fsdp", axis=0, tiled=True),
        lax.all_gather(shift_two, "fsdp", axis=0, tiled=True),
    )
    full_qkv, full_out, full_up, full_down = (gathered[0], gathered[3], gathered[7], gathered[9])
    add_q, add_v, add_out, scale_one, move_one, add_up, add_down, scale_two, move_two = [
        gathered[place].astype(jnp.float32) for place in (1, 2, 4, 5, 6, 8, 10, 11, 12)
    ]
    flat_tokens = tokens.reshape(all_rows, model_width)
    projected = row_dot(flat_tokens, full_qkv)
    queries = (
        (projected[:, :model_width] + add_q)
        .astype(jnp.bfloat16)
        .reshape(seq_count, block_rows, head_count, head_dim)
    )
    key_rows = (
        projected[:, model_width : 2 * model_width]
        .astype(jnp.bfloat16)
        .reshape(seq_count, block_rows, model_width)
    )
    value_rows = (
        (projected[:, 2 * model_width :] + add_v)
        .astype(jnp.bfloat16)
        .reshape(seq_count, block_rows, model_width)
    )
    start_state = (
        jnp.full((seq_count, block_rows, head_count), MASKED, jnp.float32),
        jnp.zeros((seq_count, block_rows, head_count), jnp.float32),
        jnp.zeros((seq_count, block_rows, head_count, head_dim), jnp.float32),
    )
    key_part = lax.all_gather(key_rows, "ctx", axis=1, tiled=True)
    value_part = lax.all_gather(value_rows, "ctx", axis=1, tiled=True)
    key_count = key_part.shape[1]
    sub_rows = math.gcd(key_count, 512)

    def visit(block_index, carried):
        first_key = block_index * sub_rows
        key_block = lax.dynamic_slice_in_dim(key_part, block_index * sub_rows, sub_rows, 1).reshape(
            seq_count, sub_rows, head_count, head_dim
        )
        value_block = lax.dynamic_slice_in_dim(
            value_part, block_index * sub_rows, sub_rows, 1
        ).reshape(seq_count, sub_rows, head_count, head_dim)
        peak, weight_sum, weighted = carried
        key_live = (
            (first_key + jnp.arange(sub_rows, dtype=jnp.int32))[None, :] < lengths[:, None]
        )[:, None, None, :]
        scores = (
            jnp.einsum("sqhe,skhe->sqhk", queries, key_block, preferred_element_type=jnp.float32)
            * score_scale
        )
        scores = jnp.where(key_live, scores, MASKED)
        new_peak = jnp.maximum(peak, jnp.max(scores, -1))
        factor = jnp.exp(peak - new_peak)
        weights = jnp.where(key_live, jnp.exp(scores - new_peak[..., None]), 0.0)
        mixed_values = jnp.einsum(
            "sqhk,skhe->sqhe",
            weights.astype(jnp.bfloat16),
            value_block,
            preferred_element_type=jnp.float32,
        )
        return (
            new_peak,
            weight_sum * factor + jnp.sum(weights, -1),
            weighted * factor[..., None] + mixed_values,
        )

    peak, weight_sum, weighted = lax.fori_loop(0, key_count // sub_rows, visit, start_state)
    log_total = peak + jnp.log(weight_sum)
    attended = weighted / weight_sum[..., None]
    attended_low = attended.astype(jnp.bfloat16).reshape(all_rows, model_width)
    first_sum = flat_tokens.astype(jnp.float32) + row_dot(attended_low, full_out) + add_out
    normed, norm_pull = jax.vjp(normalize, first_sum, scale_one, move_one)
    normed_low = normed.astype(jnp.bfloat16)
    hidden_pre = row_dot(normed_low, full_up) + add_up
    hidden_act, gelu_pull = jax.vjp(gelu_exact, hidden_pre)
    hidden_low = hidden_act.astype(jnp.bfloat16)
    second_sum = normed + row_dot(hidden_low, full_down) + add_down
    result, result_pull = jax.vjp(normalize, second_sum, scale_two, move_two)
    grad_second, grad_gain_two, grad_shift_two = result_pull(
        cotangent.reshape(all_rows, model_width).astype(jnp.float32)
    )
    down_low = grad_second.astype(jnp.bfloat16)
    grad_w_down = left_dot(hidden_low, down_low)
    grad_bias_down = jnp.sum(down_low.astype(jnp.float32), 0)
    (grad_pre,) = gelu_pull(right_dot(down_low, full_down))
    up_low = grad_pre.astype(jnp.bfloat16)
    grad_w_up = left_dot(normed_low, up_low)
    grad_bias_up = jnp.sum(up_low.astype(jnp.float32), 0)
    grad_first, grad_gain_one, grad_shift_one = norm_pull(grad_second + right_dot(up_low, full_up))
    branch_low = grad_first.astype(jnp.bfloat16)
    grad_w_out = left_dot(attended_low, branch_low)
    grad_bias_out = jnp.sum(branch_low.astype(jnp.float32), 0)
    grad_att = (
        right_dot(branch_low, full_out)
        .astype(jnp.bfloat16)
        .reshape(seq_count, block_rows, head_count, head_dim)
    )
    delta_rows = jnp.sum(grad_att.astype(jnp.float32) * attended, -1)

    def block_grads(query_part, grad_part, lse_part, delta_part, key_block, value_block, first_key):
        key_count = key_block.shape[1]
        key_heads = key_block.reshape(seq_count, key_count, head_count, head_dim)
        value_heads = value_block.reshape(seq_count, key_count, head_count, head_dim)
        key_live = (
            (first_key + jnp.arange(key_count, dtype=jnp.int32))[None, :] < lengths[:, None]
        )[:, None, None, :]
        scores = (
            jnp.einsum("sqhe,skhe->sqhk", query_part, key_heads, preferred_element_type=jnp.float32)
            * score_scale
        )
        chances = jnp.where(key_live, jnp.exp(scores - lse_part[..., None]), 0.0)
        grad_value = jnp.einsum(
            "sqhk,sqhe->skhe",
            chances.astype(jnp.bfloat16),
            grad_part,
            preferred_element_type=jnp.float32,
        )
        grad_chance = jnp.einsum(
            "sqhe,skhe->sqhk", grad_part, value_heads, preferred_element_type=jnp.float32
        )
        grad_score = (chances * (grad_chance - delta_part[..., None])).astype(jnp.bfloat16)
        grad_query = (
            jnp.einsum("sqhk,skhe->sqhe", grad_score, key_heads, preferred_element_type=jnp.float32)
            * score_scale
        )
        grad_key = (
            jnp.einsum(
                "sqhk,sqhe->skhe", grad_score, query_part, preferred_element_type=jnp.float32
            )
            * score_scale
        )
        return (
            grad_query,
            grad_key.reshape(seq_count, key_count, model_width),
            grad_value.reshape(seq_count, key_count, model_width),
        )

    query_start = jnp.zeros((seq_count, block_rows, head_count, head_dim), jnp.float32)

    def key_terms(key_block, value_block, first_key):
        return block_grads(
            queries, grad_att, log_total, delta_rows, key_block, value_block, first_key
        )

    def block_terms(key_block, value_block, first_key):
        return key_terms(key_block, value_block, first_key)

    def turn(step_index, carried):
        key_now, value_now, key_grads, query_acc = carried
        first_key = (cycle_index - step_index) % cycle_size * block_rows
        add_query, add_key, add_value = block_terms(key_now, value_now, first_key)
        key_now, value_now = shifted((key_now, value_now), "ctx", 1)
        key_grads = (
            shifted((key_grads[0] + add_key).astype(jnp.bfloat16), "ctx", 1).astype(jnp.float32),
            shifted((key_grads[1] + add_value).astype(jnp.bfloat16), "ctx", 1).astype(jnp.float32),
        )
        return (key_now, value_now, key_grads, query_acc + add_query)

    grad_start = (
        jnp.zeros((seq_count, block_rows, model_width), jnp.float32),
        jnp.zeros((seq_count, block_rows, model_width), jnp.float32),
    )
    key_final, value_final, key_grads, query_grad = lax.fori_loop(
        0, cycle_size, turn, (key_rows, value_rows, grad_start, query_start)
    )
    grad_key, grad_value = key_grads
    qkv_grad = jnp.concatenate(
        [
            query_grad.astype(jnp.bfloat16).reshape(all_rows, model_width),
            grad_key.astype(jnp.bfloat16).reshape(all_rows, model_width),
            grad_value.astype(jnp.bfloat16).reshape(all_rows, model_width),
        ],
        1,
    )
    grad_w_qkv = left_dot(flat_tokens, qkv_grad)
    grad_bias_q = jnp.sum(qkv_grad[:, :model_width].astype(jnp.float32), 0)
    grad_bias_v = jnp.sum(qkv_grad[:, 2 * model_width :].astype(jnp.float32), 0)
    grad_input = grad_first + right_dot(qkv_grad, full_qkv)
    vectors = (
        grad_bias_q,
        grad_bias_v,
        grad_bias_out,
        grad_gain_one,
        grad_shift_one,
        grad_bias_up,
        grad_bias_down,
        grad_gain_two,
        grad_shift_two,
    )
    packed = jnp.concatenate(vectors).reshape(VR, U)
    t_down, t_up, t_out, t_qkv, t_vec = grad_reduce(
        grad_w_down.astype(BF16),
        grad_w_up.astype(BF16),
        grad_w_out.astype(BF16),
        grad_w_qkv.astype(BF16),
        packed,
        cycle_size // 2,
        lax.axis_size("dp"),
        1,
    )
    flat = t_vec.reshape(-1)
    own = lax.axis_index("fsdp")
    parts, start = [], 0
    for vector in vectors:
        half = vector.shape[0] // 2
        parts.append(lax.dynamic_slice_in_dim(flat, start + own * half, half, 0))
        start += 2 * half
    totals = (
        t_qkv, parts[0], parts[1], t_out, parts[2], parts[3], parts[4],
        t_up, parts[5], t_down, parts[6], parts[7], parts[8],
    )
    output_rows = result.astype(jnp.bfloat16).reshape(seq_count, block_rows, model_width)
    input_rows = grad_input.astype(jnp.bfloat16).reshape(seq_count, block_rows, model_width)
    return (
        output_rows,
        input_rows,
        totals[0],
        totals[1],
        totals[2],
        totals[3],
        totals[4],
        totals[5],
        totals[6],
        totals[7],
        totals[8],
        totals[9],
        totals[10],
        totals[11],
        totals[12],
    )


HW = 64
QT = 256


def remote(src, dst, ss, rs, dev):
    return pltpu.make_async_remote_copy(src_ref=src, dst_ref=dst, send_sem=ss, recv_sem=rs, device_id=dev, device_id_type=MESH)


def nt(a, b):
    return lax.dot_general(a, b, (((1,), (1,)), ((), ())), preferred_element_type=F32)


def mm(a, b):
    return jnp.dot(a, b, preferred_element_type=F32)


def head_masks(rows):
    lane = lax.broadcasted_iota(jnp.int32, (rows, 2 * HW), 1)
    return lane < HW


def normal_parts(v):
    mean = jnp.mean(v, -1, keepdims=True)
    cen = v - mean
    inv = lax.rsqrt(jnp.mean(cen * cen, -1, keepdims=True) + EPSILON)
    return cen * inv, inv


def normal_back(dn, hat, inv, gain):
    d = dn * gain
    return inv * (d - jnp.mean(d, -1, keepdims=True) - hat * jnp.mean(d * hat, -1, keepdims=True))


def gelu_pair(u):
    w = jnp.abs(u)
    t = 1.0 / (1.0 + (0.3275911 * math.sqrt(0.5)) * w)
    e = jnp.exp(-0.5 * u * u)
    poly = t * (0.127414796 + t * (-0.142248368 + t * (0.7107068705 + t * (-0.7265760135 + t * 0.5307027145))))
    tail = poly * e
    phi = jnp.where(u < 0.0, tail, 1.0 - tail)
    return u * phi, phi + u * (e * (1.0 / math.sqrt(2.0 * math.pi)))


def fold8(v):
    return jnp.sum(v.reshape(v.shape[0] // 8, 8, v.shape[1]), 0)


def fwd_kernel(nx, seqs, seq_rows, lens, tok, cot, sq, so_, su, sd, *rest):
    small = rest[:9]
    (qkv_o, att_o, lse_o, wq_o, wo_o, wu_o, wd_o, vec_o, y_o, dh_o, hat_o, act_o, gp_o, vg_o) = rest[9:23]
    (XT, WB, QKV, CT, ATT, LSE, H1, N1, N1B, ACT, GP, YB,
               ls, ys, yr, zs, zr, as_, ar, bs, br, t0s, t0r, t1s, t1r, t2s, t2r, vs, vr, lts, outs) = rest[23:]
    core, x, f, z = places()
    me = x * 2 + core
    nblk = 2 * nx
    rows = seqs * seq_rows
    sib = {"ctx": x * 2 + 1 - core}
    yp = {"fsdp": 1 - f}
    zp = {"dp": z + 1 - 2 * lax.rem(z, 2)}
    zb = lax.rem(z, 2)
    xts = [lax.rem(x + j, nx) for j in range(1, nx)]
    xps = [{"ctx": t * 2 + core} for t in xts]
    xsrc = [lax.rem(x + nx - j, nx) * 2 + core for j in range(1, nx)]
    peers = [sib, yp, zp] + xps
    bar = pltpu.get_barrier_semaphore()
    for p in peers:
        pl.semaphore_signal(bar, inc=1, device_id=p, device_id_type=MESH)
    order = (1, 2, 0)
    PR = U // 4
    piece = pl.multiple_of((zb * 2 + core) * PR, PR)
    zpiece = pl.multiple_of(((1 - zb) * 2 + core) * PR, PR)
    H = rows // 2

    def shard(b, r0, n):
        r = pl.ds(r0, n)
        if b < 3:
            return sq.at[r, pl.ds(b * 768, 768)]
        if b == 3:
            return so_.at[r, :]
        if b < 8:
            return su.at[r, pl.ds((b - 4) * 768, 768)]
        return sd.at[pl.ds((b - 8) * U + r0, n), :]

    def loc(b):
        return pltpu.make_async_copy(shard(b, 0, U), WB.at[b, f], ls.at[b])

    def ycp(b):
        if not isinstance(b, int):
            src = WB.at[b, f, pl.ds(piece, PR)]
        else:
            src = shard(b, piece, PR)
        return remote(src, WB.at[b, f, pl.ds(piece, PR)], ys.at[b], yr.at[b], yp)

    def zcp(b):
        w = WB.at[b, 1 - f, pl.ds(piece, PR)]
        return remote(w, w, zs.at[b], zr.at[b], zp)

    def acp(b):
        w = WB.at[b, 1 - f, pl.ds(piece, PR)]
        return remote(w, w, as_.at[b], ar.at[b], sib)

    def bcp(b):
        w = WB.at[b, 1 - f, pl.ds(zpiece, PR)]
        return remote(w, w, bs.at[b], br.at[b], sib)

    def A(b):
        ycp(b).wait_recv()
        zcp(b).start()
        acp(b).start()

    def B(b):
        zcp(b).wait_recv()
        bcp(b).start()

    def C(b):
        acp(b).wait_recv()
        bcp(b).wait_recv()

    def tsl(h):
        return pl.ds(h * H, H)

    def t_sib(h):
        return remote(tok.at[tsl(h)], XT.at[me, tsl(h)], t0s.at[h], t0r.at[h], sib)

    def t_x(j, h):
        return remote(tok.at[tsl(h)], XT.at[me, tsl(h)], t1s.at[j - 1, h], t1r.at[j - 1, h], xps[j - 1])

    def t_f(j, h):
        w = XT.at[xsrc[j - 1], tsl(h)]
        return remote(w, w, t2s.at[j - 1, h], t2r.at[j - 1, h], sib)

    vcp = remote(vec_o.at[f], vec_o.at[f], vs.at[0], vr.at[0], yp)
    tl = pltpu.make_async_copy(tok, XT.at[me], lts.at[0])
    tl.start()
    for b in order:
        loc(b).start()
    row = 0
    for v in small:
        w = v[...].astype(F32).reshape(1, -1)
        for i in range(v.shape[0] // U):
            vec_o[f, row:row + 1, :] = w[:, i * U:(i + 1) * U]
            row += 1
    tc = pltpu.make_async_copy(cot, CT, lts.at[1])
    pl.semaphore_wait(bar, len(peers))
    vcp.start()
    for b in order:
        ycp(b).start()
    for h in range(2):
        for j in range(1, nx):
            t_x(j, h).start()
        t_sib(h).start()
    for b in range(3, 12):
        ycp(b).start()
    for b in range(3, 12):
        loc(b).start()
    tc.start()
    tl.wait()

    def qkv(b, blk, h):
        hr = pl.ds(pl.multiple_of(h * H, H), H)
        row = 0 if b == 0 else 1
        xr = XT[blk, hr, :]
        for t in range(3):
            w = WB[b, :, :, t * 256:(t + 1) * 256].reshape(768, 256)
            r = mm(xr, w)
            if b != 1:
                if t == 0:
                    bias = vec_o[0, row:row + 1, 0:256]
                elif t == 1:
                    bias = jnp.concatenate([vec_o[0, row:row + 1, 256:384], vec_o[1, row:row + 1, 0:128]], 1)
                else:
                    bias = vec_o[1, row:row + 1, 128:384]
                r = r + bias
            r = r.astype(BF16)
            if b == 0:
                r = r * jnp.asarray(0.125, BF16)
            QKV[b, blk, hr, t * 256:(t + 1) * 256] = r

    def far(h, bs):
        for j in range(1, nx):
            base = lax.rem(x + nx - j, nx) * 2

            def pair(i, _):
                for b in bs:
                    qkv(b, base + i, h)
                return 0
            lax.fori_loop(0, 2, pair, 0)

    def far_wait(h):
        for j in range(1, nx):
            t_f(j, h).wait_recv()

    def relay(h):
        for j in range(1, nx):
            t_x(j, h).wait_recv()
            t_f(j, h).start()

    def near(b):
        def both(i, _):
            qkv(b, x * 2 + i // 2, lax.rem(i, 2))
            return 0
        lax.fori_loop(0, 4, both, 0)

    A(1)
    for h in range(2):
        t_sib(h).wait_recv()
    vcp.wait_recv()
    loc(1).wait()
    B(1)
    A(2)
    C(1)
    near(1)
    B(2)
    A(0)
    relay(0)
    loc(2).wait()
    C(2)
    near(2)
    B(0)
    far_wait(0)
    far(0, (1,))
    A(3)
    loc(0).wait()
    C(0)
    near(0)
    A(4)
    far(0, (2, 0))

    low_half = head_masks(QT)
    lane128 = lax.broadcasted_iota(jnp.int32, (QT, 128), 1)
    kpos = lax.broadcasted_iota(jnp.int32, (QT, QT), 1)
    nr = seq_rows // QT

    def attend(tile, j):
        s0 = tile // nr
        qr = pl.ds(pl.multiple_of(tile * QT, QT), QT)
        cols = pl.ds(pl.multiple_of(j * 128, 128), 128)
        q = QKV[0, me, qr, cols]
        length = lens[s0]
        outs_ = []
        tot = LSE[qr, 0:128]
        for h in range(2):
            qh = jnp.where(low_half == (h == 0), q, jnp.zeros_like(q))
            sc = []
            mx = None
            for blk in range(nblk):
                for r in range(nr):
                    kr = pl.ds(pl.multiple_of(s0 * seq_rows + r * QT, QT), QT)
                    v = nt(qh, QKV[1, blk, kr, cols])
                    v = jnp.where(kpos < length - (blk * seq_rows + r * QT), v, MASKED)
                    sc.append(v)
                    mx = v if mx is None else jnp.maximum(mx, v)
            m = jnp.max(mx, 1, keepdims=True)
            acc = None
            lsum = None
            i = 0
            for blk in range(nblk):
                for r in range(nr):
                    kr = pl.ds(pl.multiple_of(s0 * seq_rows + r * QT, QT), QT)
                    p = jnp.exp(sc[i] - m)
                    i += 1
                    lsum = p if lsum is None else lsum + p
                    o = mm(p.astype(BF16), QKV[2, blk, kr, cols])
                    acc = o if acc is None else acc + o
            den = jnp.sum(lsum, 1, keepdims=True)
            outs_.append(acc / den)
            tot = jnp.where(lane128 == 2 * j + h, m + jnp.log(den), tot)
        ATT[qr, cols] = jnp.where(low_half, outs_[0], outs_[1])
        LSE[qr, 0:128] = tot

    tiles = rows // QT // 2

    def attend_half(h, hooks):
        per = tiles * 6 // len(hooks)

        def group(g, _):
            def one(i, _):
                it = g * per + i
                attend(h * tiles + it // 6, lax.rem(it, 6))
                return 0
            lax.fori_loop(0, per, one, 0)
            for k, hook in enumerate(hooks):
                @pl.when(g == k)
                def _(hook=hook):
                    hook()
            return 0
        lax.fori_loop(0, len(hooks), group, 0)

    def step(a):
        def fn():
            A(a)
            B(a - 2)
        return fn

    def last():
        step(7)()
        relay(1)
    attend_half(0, (step(5), step(6), last))
    far_wait(1)
    far(1, order)
    step(8)()
    qo = pltpu.make_async_copy(QKV, qkv_o, outs.at[0])
    qo.start()
    attend_half(1, (step(9), step(10), step(11)))
    extra = []

    def send_out(src, dst):
        cp = pltpu.make_async_copy(src, dst, outs.at[25 + len(extra)])
        cp.start()
        extra.append(cp)

    def full(b):
        res = []
        for ff in range(2):
            src = WB.at[b, ff]
            if b < 3:
                dst = wq_o.at[pl.ds(ff * U, U), pl.ds(b * 768, 768)]
            elif b == 3:
                dst = wo_o.at[pl.ds(ff * U, U), :]
            elif b < 8:
                dst = wu_o.at[pl.ds(ff * U, U), pl.ds((b - 4) * 768, 768)]
            else:
                dst = wd_o.at[pl.ds(ff * 1536 + (b - 8) * U, U), :]
            res.append(pltpu.make_async_copy(src, dst, outs.at[1 + 2 * b + ff]))
        return res

    def ready(b):
        loc(b).wait()
        C(b)
        for cp in full(b):
            cp.start()

    def vector(r):
        return jnp.concatenate([vec_o[0, r:r + 1, :], vec_o[1, r:r + 1, :]], 1)

    for b in range(3):
        for cp in full(b):
            cp.start()
    send_out(ATT, att_o)
    ready(3)
    bo = vector(2)
    for t in range(3):
        cs = slice(t * 256, (t + 1) * 256)
        w = WB[3, :, :, cs].reshape(768, 256)
        H1[:, cs] = XT[me, :, cs].astype(F32) + mm(ATT[...].astype(BF16), w) + bo[:, cs]
    g1, s1 = vector(3), vector(4)
    RB = 64

    def ln1(i, _):
        r = pl.ds(pl.multiple_of(i * RB, RB), RB)
        hat, inv = normal_parts(H1[r, :])
        H1[r, :] = hat
        n = hat * g1 + s1
        N1[r, :] = n
        N1B[r, :] = n.astype(BF16)
        LSE[r, 128:256] = jnp.broadcast_to(inv, (RB, 128))
        return 0
    lax.fori_loop(0, rows // RB, ln1, 0)
    send_out(H1, hat_o)
    send_out(LSE, lse_o)
    B(10)
    for b in range(4, 8):
        ready(b)

    def upblock(b, _):
        bias = jnp.concatenate([vec_o[b // 2, pl.ds(5 + lax.rem(b, 2) * 2, 1), :], vec_o[b // 2, pl.ds(6 + lax.rem(b, 2) * 2, 1), :]], 1)
        for t in range(3):
            w = WB[4 + b, :, :, t * 256:(t + 1) * 256].reshape(768, 256)
            cs = pl.ds(pl.multiple_of(b * 768 + t * 256, 256), 256)
            act, gp = gelu_pair(mm(N1B[...], w) + bias[:, t * 256:(t + 1) * 256])
            ACT[:, cs] = act.astype(BF16)
            GP[:, cs] = gp
        return 0
    lax.fori_loop(0, 2, upblock, 0)
    B(11)
    ready(8)
    ready(9)
    lax.fori_loop(2, 4, upblock, 0)
    send_out(ACT, act_o)
    send_out(GP, gp_o)
    for b in range(10, 12):
        ready(b)
    bd = vector(9)
    for t in range(3):
        cs = slice(t * 256, (t + 1) * 256)
        acc = N1[:, cs] + bd[:, cs]
        for ff in range(2):
            acc = acc + mm(ACT[:, ff * 1536:(ff + 1) * 1536], WB[8:12, ff, :, cs].reshape(1536, 256))
        N1[:, cs] = acc
    g2, s2 = vector(10), vector(11)
    tc.wait()

    def ln2(i, carry):
        r = pl.ds(pl.multiple_of(i * RB, RB), RB)
        hat, inv = normal_parts(N1[r, :])
        YB[r, :] = (hat * g2 + s2).astype(BF16)
        g = CT[r, :].astype(F32)
        N1[r, :] = normal_back(g, hat, inv, g2)
        return carry[0] + fold8(g * hat), carry[1] + fold8(g)
    zero = jnp.zeros((8, 768), F32)
    a0, a1 = lax.fori_loop(0, rows // RB, ln2, (zero, zero))
    send_out(YB, y_o)
    send_out(N1, dh_o)
    vg_o[0:1, :] = jnp.sum(a0, 0, keepdims=True)
    vg_o[1:2, :] = jnp.sum(a1, 0, keepdims=True)
    vcp.wait_send()
    qo.wait()
    for b in range(12):
        ycp(b).wait_send()
        zcp(b).wait_send()
        acp(b).wait_send()
        bcp(b).wait_send()
        for cp in full(b):
            cp.wait()
    for h in range(2):
        t_sib(h).wait_send()
        for j in range(1, nx):
            t_x(j, h).wait_send()
            t_f(j, h).wait_send()
    for cp in extra:
        cp.wait()


def forward_gather(lens, tok, cot, sq, so_, su, sd, small, nx, cid):
    seqs, seq_rows, d = tok.shape
    rows = seqs * seq_rows
    nblk = 2 * nx
    anyspec = pl.BlockSpec(memory_space=pl.ANY)
    vspec = pl.BlockSpec(memory_space=pltpu.VMEM)
    sspec = pl.BlockSpec(memory_space=pltpu.SMEM)
    D = pltpu.SemaphoreType.DMA
    V = pltpu.VMEM
    S = jax.ShapeDtypeStruct
    sems = [D((12,))] * 9 + [D((2,)), D((2,))] + [D((nx - 1, 2))] * 4 + [D((1,)), D((1,)), D((2,)), D((33,))]
    return pl.pallas_call(
        functools.partial(fwd_kernel, nx, seqs, seq_rows),
        out_shape=(S((3, nblk, rows, d), BF16), S((rows, d), F32), S((rows, 256), F32),
                   S((768, 2304), BF16), S((768, 768), BF16), S((768, 3072), BF16), S((3072, 768), BF16),
                   S((2, 12, U), F32), S((rows, d), BF16), S((rows, d), F32), S((rows, d), F32),
                   S((rows, 3072), BF16), S((rows, 3072), F32), S((2, d), F32)),
        in_specs=[sspec] + [anyspec] * 6 + [vspec] * 9,
        out_specs=(anyspec,) * 7 + (vspec,) + (anyspec,) * 5 + (vspec,),
        scratch_shapes=[V((nblk, rows, d), BF16), V((12, 2, U, 768), BF16), V((3, nblk, rows, d), BF16),
                        V((rows, d), BF16), V((rows, d), F32), V((rows, 256), F32), V((rows, d), F32), V((rows, d), F32),
                        V((rows, d), BF16), V((rows, 3072), BF16), V((rows, 3072), F32), V((rows, d), BF16)] + sems,
        compiler_params=pltpu.CompilerParams(collective_id=cid, has_side_effects=True, vmem_limit_bytes=62 << 20),
        name="forward_gather",
    )(lens, tok.reshape(rows, d), cot.reshape(rows, d), sq, so_, su, sd, *small)


def tn(a, b):
    return lax.dot_general(a, b, (((0,), (0,)), ((), ())), preferred_element_type=F32)


def colsum(v):
    return jnp.sum(fold8(v), 0, keepdims=True)


def bwd_kernel(nx, nd, seqs, seq_rows, lens, vec, vg, qkv_i, att_i, lse_i, wq_i, wo_i, wu_i, wd_i, dh_i, hat_i, act_i, gp_i, tok_i,
               od, ou, oo, oq, ov, gin_o,
               BIG, WO, WQ, GP, ACT, DH, DM, HAT, NB, DO, ROWS, COLS, DQKV, L, SB, R1, R2, R3, R4, RH, AX, VV, V0, VX, VZ,
               lds, d0s, d0r, d1s, d1r, d2s, d2r, s1s, s1r, s2s, s2r, s3s, s3r, s4s, s4r, s5s, s5r, s6s, s6r, s7s, s7r, s8, vs, vr, hs, hr):
    core, x, f, z = places()
    me = x * 2 + core
    nblk = 2 * nx
    rows = seqs * seq_rows
    CX, PZ = U // nx, U // nx // nd
    NCH, READY, QFIRST = 12, 8, 3
    sib = {"ctx": x * 2 + 1 - core}
    yp = {"fsdp": 1 - f}
    xps = [{"ctx": lax.rem(x + j, nx) * 2 + core} for j in range(1, nx)]
    xsrc = [lax.rem(x + nx - j, nx) * 2 + core for j in range(1, nx)]
    zps = [{"dp": lax.rem(z + j, nd)} for j in range(1, nd)]
    peers = [sib, yp] + xps + zps
    bar = pltpu.get_barrier_semaphore()
    for p in peers:
        pl.semaphore_signal(bar, inc=1, device_id=p, device_id_type=MESH)

    loads = {}

    def load(name, src, dst):
        cp = pltpu.make_async_copy(src, dst, lds.at[len(loads)])
        cp.start()
        loads[name] = cp

    load("dh", dh_i, DH)
    load("act", act_i, ACT)
    for b in range(4):
        load(("wd", b), wd_i.at[pl.ds(b * 768, 768)], BIG.at[pl.ds(b * 768, 768)])
        if b < 2:
            load("gp%d" % b, gp_i.at[:, pl.ds(b * 768, 768)], GP.at[b])
    load("hat", hat_i, HAT)
    for b in range(4):
        load(("wu", b), wu_i.at[:, pl.ds(b * 768, 768)], BIG.at[pl.ds(3072 + b * 768, 768)])
    load("lse", lse_i, COLS.at[:, pl.ds(0, 256)])
    load("wo", wo_i, WO)

    def vector(r):
        return jnp.concatenate([vec[0, r:r + 1, :], vec[1, r:r + 1, :]], 1)

    def c1(i, ff, k):
        return remote(SB.at[i % 4, ff], R1.at[i, ff], s1s.at[i, k], s1r.at[i, k], sib)

    def c1s(i):
        return [c1(i, 1 - f, 0), c1(i, f, 1)]

    def c2(c):
        return remote(L.at[c, 1 - f], R2.at[c], s2s.at[c], s2r.at[c], yp)

    def c3(c, j):
        xt = lax.rem(x + j, nx)
        return remote(L.at[c, f, pl.ds(pl.multiple_of(xt * CX, CX), CX)], R3.at[c - READY - 1, j - 1], s3s.at[c, j - 1], s3r.at[c, j - 1], xps[j - 1])

    def mine(zz):
        return pl.ds(pl.multiple_of(x * CX + (lax.rem(zz, 2) * 2 + zz // 2) * PZ, PZ), PZ)

    zpar = lax.rem(z, 2)
    ways = {"x": (x, xps[0]), "near": (zpar, {"dp": z + 1 - 2 * zpar}), "far": (z // 2, {"dp": lax.rem(z + 2, nd)})}

    def level(c, k):
        dims = ("near", "far", "x") if c < QFIRST else ("x", "near", "far")
        base, n = 0, U
        for d in dims[:k]:
            n = n // 2
            base = base + ways[d][0] * n
        bit, dev = ways[dims[k]]
        half = n // 2
        at = (0, U // 2, 3 * U // 4)[k]
        keep = pl.ds(pl.multiple_of(base + bit * half, half), half)
        give = pl.ds(pl.multiple_of(base + (1 - bit) * half, half), half)
        return keep, give, pl.ds(at, half), half, at, base + bit * half, base + (1 - bit) * half, dev

    def down(c, k):
        _, give, at, _, _, _, _, dev = level(c, k)
        return remote(L.at[c, f, give], RH.at[c, at], hs.at[c, k], hr.at[c, k], dev)

    def upw(c, k):
        keep, _, _, _, _, _, _, dev = level(c, k)
        w = AX.at[c, keep]
        return remote(w, w, hs.at[c, 3 + k], hr.at[c, 3 + k], dev)

    def direct(c):
        return c > READY

    def c4(c, j):
        zt = lax.rem(z + j, nd)
        return remote(L.at[c, f, mine(zt)], R4.at[c - READY - 1, j - 1], s4s.at[c, j - 1], s4r.at[c, j - 1], zps[j - 1])

    def c5(c, j):
        w = AX.at[c, mine(z)]
        return remote(w, w, s5s.at[c, j - 1], s5r.at[c, j - 1], zps[j - 1])

    def c6(c, j):
        w = AX.at[c, pl.ds(pl.multiple_of(x * CX, CX), CX)]
        return remote(w, w, s6s.at[c, j - 1], s6r.at[c, j - 1], xps[j - 1])

    def qpart(i, cc):
        return cc if i == 9 else i - 8 + 2 * cc

    def orect(i):
        if i < 4:
            return od.at[pl.ds(pl.multiple_of(core * 768 + i // 2 * U, U), U), pl.ds(i % 2 * U, U)]
        if i < 8:
            return ou.at[:, pl.ds(pl.multiple_of(core * 1536 + (i - 4) * U, 128), U)]
        if i < 9:
            return oo.at[:, pl.ds(pl.multiple_of(core * U, 128), U)]
        return oq.at[:, pl.ds(pl.multiple_of(qpart(i, core) * U, 128), U)]

    def c7(c):
        return remote(AX.at[c], orect(c), s7s.at[c], s7r.at[c], sib)

    def c8(c):
        return pltpu.make_async_copy(AX.at[c], orect(c), s8.at[c])

    B = 48

    def rows_loop(n, fn):
        def bodyf(i, _):
            fn(pl.multiple_of(i * B, B))
            return 0
        lax.fori_loop(0, n // B, bodyf, 0)

    def up(v):
        return v.astype(F32)

    def st1(i):
        for cp in c1s(i):
            cp.start()

    def st2(c):
        c1(c, 1 - f, 0).wait_recv()

        def fn(r):
            s = pl.ds(r, B)
            L[c, 1 - f, s, :] = (up(L[c, 1 - f, s, :]) + up(R1[c, 1 - f, s, :])).astype(BF16)
        rows_loop(U, fn)
        c2(c).start()

    def st3(c):
        c1(c, f, 1).wait_recv()
        c2(c).wait_recv()
        for j in range(1, nx):
            xt = lax.rem(x + j, nx)

            def fn(r):
                s = pl.ds(pl.multiple_of(xt * CX + r, B), B)
                L[c, f, s, :] = (up(L[c, f, s, :]) + up(R1[c, f, s, :]) + up(R2[c, s, :])).astype(BF16)
            rows_loop(CX, fn)
            c3(c, j).start()

    def st4(c):
        for j in range(1, nx):
            c3(c, j).wait_recv()

        def fn(r):
            s = pl.ds(pl.multiple_of(x * CX + r, B), B)
            t = up(L[c, f, s, :]) + up(R1[c, f, s, :]) + up(R2[c, s, :])
            for j in range(1, nx):
                t = t + up(R3[c - READY - 1, j - 1, pl.ds(r, B), :])
            L[c, f, s, :] = t.astype(BF16)
        rows_loop(CX, fn)
        for j in range(1, nd):
            c4(c, j).start()

    def h0(c):
        c1(c, f, 1).wait_recv()
        c2(c).wait_recv()
        _, _, _, half, _, _, off, _ = level(c, 0)

        def fn(r):
            s = pl.ds(pl.multiple_of(off + r, B), B)
            L[c, f, s, :] = (up(L[c, f, s, :]) + up(R1[c, f, s, :]) + up(R2[c, s, :])).astype(BF16)
        rows_loop(half, fn)
        down(c, 0).start()

    def h1(c):
        down(c, 0).wait_recv()
        _, _, _, half, at, off, _, _ = level(c, 0)

        def fn(r):
            s = pl.ds(pl.multiple_of(off + r, B), B)
            t = up(L[c, f, s, :]) + up(R1[c, f, s, :]) + up(R2[c, s, :]) + up(RH[c, pl.ds(pl.multiple_of(at + r, B), B), :])
            L[c, f, s, :] = t.astype(BF16)
        rows_loop(half, fn)
        down(c, 1).start()

    def h2(c):
        down(c, 1).wait_recv()
        _, _, _, half, at, off, _, _ = level(c, 1)

        def fn(r):
            s = pl.ds(pl.multiple_of(off + r, B), B)
            L[c, f, s, :] = (up(L[c, f, s, :]) + up(RH[c, pl.ds(pl.multiple_of(at + r, B), B), :])).astype(BF16)
        rows_loop(half, fn)
        down(c, 2).start()

    def h3(c):
        down(c, 2).wait_recv()
        keep, _, at, _, _, _, _, _ = level(c, 2)
        AX[c, keep, :] = (up(L[c, f, keep, :]) + up(RH[c, at, :])).astype(BF16)
        upw(c, 2).start()

    def h4(c):
        upw(c, 2).wait_recv()
        upw(c, 1).start()

    def h5(c):
        upw(c, 1).wait_recv()
        upw(c, 0).start()

    def st5(c):
        for j in range(1, nd):
            c4(c, j).wait_recv()
        t = up(L[c, f, mine(z), :])
        for j in range(1, nd):
            t = t + up(R4[c - READY - 1, j - 1])
        AX[c, mine(z), :] = t.astype(BF16)
        for j in range(1, nd):
            c5(c, j).start()

    def st6(c):
        for j in range(1, nd):
            c5(c, j).wait_recv()
        for j in range(1, nx):
            c6(c, j).start()

    def st7(c):
        if direct(c):
            for j in range(1, nx):
                c6(c, j).wait_recv()
        else:
            upw(c, 0).wait_recv()
        c7(c).start()
        c8(c).start()

    def v_core():
        return remote(VV, V0.at[0], vs.at[0], vr.at[0], sib)

    def v_y():
        return remote(V0.at[1], V0.at[2], vs.at[1], vr.at[1], yp)

    def v_x(j):
        return remote(VX.at[x], VX.at[x], vs.at[1 + j], vr.at[1 + j], xps[j - 1])

    def v_z(j):
        return remote(VZ.at[z], VZ.at[z], vs.at[nx + j], vr.at[nx + j], zps[j - 1])

    def vst(k):
        if k == 0:
            v_core().start()
        elif k == 1:
            v_core().wait_recv()
            V0[1] = VV[...] + V0[0]
            v_y().start()
        elif k == 2:
            v_y().wait_recv()
            VX[x] = V0[1] + V0[2]
            for j in range(1, nx):
                v_x(j).start()
        elif k == 3:
            for j in range(1, nx):
                v_x(j).wait_recv()
            t = VX[0]
            for j in range(1, nx):
                t = t + VX[j]
            VZ[z] = t
            for j in range(1, nd):
                v_z(j).start()
        elif k == 4:
            for j in range(1, nd):
                v_z(j).wait_recv()
            t = VZ[0]
            for j in range(1, nd):
                t = t + VZ[j]
            VV2 = t
            for r, n, o in ((0, 1, 0), (2, 1, 1), (4, 1, 2), (6, 1, 3), (8, 1, 4), (10, 4, 5), (18, 1, 9), (20, 1, 10), (22, 1, 11)):
                ov[o:o + n, :] = jnp.where(f == 0, VV2[r:r + n, :], VV2[r + n:r + 2 * n, :])

    def put_vec(r, v):
        VV[r:r + 1, :] = v[:, :U]
        VV[r + 1:r + 2, :] = v[:, U:]

    put_vec(20, vg[0:1, :])
    put_vec(22, vg[1:2, :])

    RB = 64
    loads["dh"].wait()

    def to_dm(i, acc):
        r = pl.ds(pl.multiple_of(i * RB, RB), RB)
        v = DH[r, :].astype(BF16)
        DM[r, :] = v
        return acc + fold8(v.astype(F32))
    zero = jnp.zeros((8, 768), F32)
    put_vec(18, jnp.sum(lax.fori_loop(0, rows // RB, to_dm, zero), 0, keepdims=True))

    def fill(i0, kk, ff, val, wide):
        v = val.astype(BF16)
        for t in range(wide):
            if kk == 0:
                L[i0 + t, ff] = v[:, t * U:(t + 1) * U]
            else:
                SB[(i0 + t) % 4, ff] = v[:, t * U:(t + 1) * U]

    def each_f(fn):
        def one(k, _):
            fn(jnp.where(k == 0, 1 - f, f))
            return 0
        lax.fori_loop(0, 2, one, 0)

    def ccof(kk):
        return core if kk == 0 else 1 - core

    pl.semaphore_wait(bar, len(peers))
    loads["act"].wait()
    for ii in range(2):
        for kk in (1, 0):
            def wdown(ff, kk=kk, ii=ii):
                h = pl.multiple_of(ff * 1536 + ccof(kk) * 768 + ii * U, U)
                fill(2 * ii, kk, ff, tn(ACT[:, pl.ds(h, U)], DM[...]), 2)
            each_f(wdown)
            if kk == 1:
                st1(2 * ii)
                st1(2 * ii + 1)
                if ii == 1:
                    st2(0)
                    st2(1)
    st2(2)
    for b in range(4):
        loads[("wd", b)].wait()
        loads["gp%d" % b].wait()
        for t in range(3):
            h = b * 768 + t * 256
            du = (nt(DM[...], BIG[h:h + 256, :]) * GP[b % 2, :, t * 256:(t + 1) * 256]).astype(BF16)
            WQ[b * rows:(b + 1) * rows, t * 256:(t + 1) * 256] = du
            s = colsum(du.astype(F32))
            for q in range(2):
                o = h + q * 128
                VV[10 + o // U:11 + o // U, o % U:o % U + 128] = s[:, q * 128:(q + 1) * 128]
        if b < 2:
            load("gp%d" % (b + 2), gp_i.at[:, pl.ds((b + 2) * 768, 768)], GP.at[b % 2])
    st2(3)
    loads["hat"].wait()
    g1, s1 = vector(3), vector(4)
    for b in range(4):
        loads[("wu", b)].wait()
    for t in range(3):
        cs = slice(t * 256, (t + 1) * 256)
        acc = DH[:, cs]
        for b in range(4):
            acc = acc + nt(WQ[b * rows:(b + 1) * rows, :], BIG[3072 + b * 768 + t * 256:3072 + b * 768 + (t + 1) * 256, :])
        DH[:, cs] = acc
    for k in (1, 2, 0):
        for blk in range(nblk):
            load(("qkv", k, blk), qkv_i.at[k, blk], BIG.at[pl.ds((k * nblk + blk) * rows, rows)])
    h0(0)
    loads["lse"].wait()

    def ln1(i, carry):
        r = pl.ds(pl.multiple_of(i * RB, RB), RB)
        dn, hat = DH[r, :], HAT[r, :]
        d = normal_back(dn, hat, COLS[r, 128:129], g1)
        DH[r, :] = d
        da = d.astype(BF16)
        DQKV[0, r, :] = da
        NB[r, :] = (hat * g1 + s1).astype(BF16)
        return carry[0] + fold8(dn * hat), carry[1] + fold8(dn), carry[2] + fold8(da.astype(F32))
    sums = lax.fori_loop(0, rows // RB, ln1, (zero, zero, zero))
    for row, sv in zip((6, 8, 4), sums):
        put_vec(row, jnp.sum(sv, 0, keepdims=True))
    load("att", att_i, HAT)
    loads["wo"].wait()
    for t in range(3):
        DO[me, :, t * 256:(t + 1) * 256] = nt(DQKV[0], WO[t * 256:(t + 1) * 256, :]).astype(BF16)

    def d_sib():
        return remote(DO.at[me], DO.at[me], d0s.at[0], d0r.at[0], sib)

    def d_x(j):
        return remote(DO.at[me], DO.at[me], d1s.at[j - 1, 0], d1r.at[j - 1, 0], xps[j - 1])

    def d_f(j):
        w = DO.at[xsrc[j - 1]]
        return remote(w, w, d2s.at[j - 1, 0], d2r.at[j - 1, 0], sib)

    def r_sib():
        return remote(ROWS.at[me], ROWS.at[me], d0s.at[1], d0r.at[1], sib)

    def r_x(j):
        return remote(ROWS.at[me], ROWS.at[me], d1s.at[j - 1, 1], d1r.at[j - 1, 1], xps[j - 1])

    def r_f(j):
        w = ROWS.at[xsrc[j - 1]]
        return remote(w, w, d2s.at[j - 1, 1], d2r.at[j - 1, 1], sib)

    for j in range(1, nx):
        d_x(j).start()
    d_sib().start()
    loads["att"].wait()
    head = lax.broadcasted_iota(jnp.int32, (768, 128), 0) // HW
    pick = (head == lax.broadcasted_iota(jnp.int32, (768, 128), 1)).astype(BF16)

    def delta(i, _):
        r = pl.ds(pl.multiple_of(i * 128, 128), 128)
        v = DO[me, r, :].astype(F32) * HAT[r, :]
        hi = v.astype(BF16)
        rest = v - hi.astype(F32)
        mid = rest.astype(BF16)
        low = (rest - mid.astype(F32)).astype(BF16)
        d = mm(hi, pick) + mm(mid, pick) + mm(low, pick)
        COLS[r, 128:256] = d
        ROWS[me, 16:32, r] = jnp.transpose(d)[0:16, :]
        ROWS[me, 0:16, r] = jnp.transpose(COLS[r, 0:128])[0:16, :]
        return 0
    lax.fori_loop(0, rows // 128, delta, 0)
    for j in range(1, nx):
        r_x(j).start()
    r_sib().start()
    h1(0)
    h0(1)
    for ii in range(2):
        for kk in (1, 0):
            if kk == 1:
                for i in (2 * ii, 2 * ii + 1):
                    for cp in c1s(i):
                        cp.wait_send()

            def wup(ff, kk=kk, ii=ii):
                h = pl.multiple_of((ccof(kk) * 2 + ii) * rows, rows)
                fill(4 + 2 * ii, kk, ff, tn(NB[:, pl.ds(pl.multiple_of(ff * U, U), U)], WQ[pl.ds(h, rows), :]), 2)
            each_f(wup)
            if kk == 1:
                st1(4 + 2 * ii)
                st1(5 + 2 * ii)
                if ii == 1:
                    st2(4)
                    st2(5)
    load("tok", tok_i, NB)
    for b in range(3):
        load(("wq", b), wq_i.at[:, pl.ds(b * 768, 768)], WQ.at[pl.ds(b * 768, 768)])
    h2(0)
    h1(1)
    h0(2)
    st2(6)
    for kk in (1, 0):
        if kk == 1:
            for cp in c1s(4):
                cp.wait_send()

        def wout(ff, kk=kk):
            a = HAT[:, pl.ds(pl.multiple_of(ff * U, U), U)].astype(BF16)
            fill(8, kk, ff, tn(a, DQKV[0, :, pl.ds(pl.multiple_of(ccof(kk) * U, U), U)]), 1)
        each_f(wout)
        if kk == 1:
            st1(8)
    st2(7)
    st2(8)
    for k in (1, 2, 0):
        for blk in range(nblk):
            loads[("qkv", k, blk)].wait()
    low_half = head_masks(QT)
    lane128 = lax.broadcasted_iota(jnp.int32, (QT, 128), 1)
    kpos = lax.broadcasted_iota(jnp.int32, (QT, QT), 1)
    krow = lax.broadcasted_iota(jnp.int32, (QT, 128), 0)
    nr = seq_rows // QT
    ntile = rows // QT

    def big(k, blk, r0, cols):
        return BIG[pl.ds(pl.multiple_of((k * nblk + blk) * rows + r0, QT), QT), cols]

    def pick_col(v, h):
        return jnp.sum(jnp.where(lane128 == h, v, 0.0), 1, keepdims=True)

    def zero_other(v, h):
        return jnp.where(low_half == (h == 0), v, jnp.zeros_like(v))

    def dq_one(it):
        tile, j = it // 6, lax.rem(it, 6)
        s0 = tile // nr
        q0 = pl.multiple_of(tile * QT, QT)
        qr = pl.ds(q0, QT)
        cols = pl.ds(pl.multiple_of(j * 128, 128), 128)
        q = big(0, me, q0, cols)
        do = DO[me, qr, cols]
        length = lens[s0]
        res = []
        for h in range(2):
            qh, doh = zero_other(q, h), zero_other(do, h)
            lse = pick_col(COLS[qr, 0:128], 2 * j + h)
            dl = pick_col(COLS[qr, 128:256], 2 * j + h)
            acc = None
            for blk in range(nblk):
                for r in range(nr):
                    k0 = s0 * seq_rows + r * QT
                    kt = big(1, blk, k0, cols)
                    p = jnp.exp(nt(qh, kt) - lse)
                    p = jnp.where(kpos < length - (blk * seq_rows + r * QT), p, 0.0)
                    ds = (p * (nt(doh, big(2, blk, k0, cols)) - dl)).astype(BF16)
                    o = mm(ds, kt)
                    acc = o if acc is None else acc + o
            res.append(acc)
        DQKV[0, qr, cols] = (jnp.where(low_half, res[0], res[1]) * 0.125).astype(BF16)

    def dkv_one(it):
        tile, j = lax.rem(it, ntile), it // ntile
        s0 = tile // nr
        k0 = pl.multiple_of(tile * QT, QT)
        kr = pl.ds(k0, QT)
        cols = pl.ds(pl.multiple_of(j * 128, 128), 128)
        k, v = big(1, me, k0, cols), big(2, me, k0, cols)
        live = krow < lens[s0] - (me * seq_rows + (tile - s0 * nr) * QT)
        resk, resv = [], []
        for h in range(2):
            kh, vh = zero_other(k, h), zero_other(v, h)
            ak = av = None
            for blk in range(nblk):
                for r in range(nr):
                    q0 = pl.multiple_of(s0 * seq_rows + r * QT, QT)
                    qr = pl.ds(q0, QT)
                    qt, dt = big(0, blk, q0, cols), DO[blk, qr, cols]
                    lse = ROWS[blk, pl.ds(2 * j + h, 1), qr]
                    dl = ROWS[blk, pl.ds(16 + 2 * j + h, 1), qr]
                    p = jnp.exp(nt(kh, qt) - lse)
                    ds = (p * (nt(vh, dt) - dl)).astype(BF16)
                    ov_, ok_ = mm(p.astype(BF16), dt), mm(ds, qt)
                    av = ov_ if av is None else av + ov_
                    ak = ok_ if ak is None else ak + ok_
            resk.append(ak)
            resv.append(av)
        DQKV[1, kr, cols] = jnp.where(live, jnp.where(low_half, resk[0], resk[1]), 0.0).astype(BF16)
        DQKV[2, kr, cols] = jnp.where(live, jnp.where(low_half, resv[0], resv[1]), 0.0).astype(BF16)

    def segment(fn, base, count, hooks):
        per = count // len(hooks)

        def group(g, _):
            def one(i, _):
                fn(base + g * per + i)
                return 0
            lax.fori_loop(0, per, one, 0)
            for k, steps in enumerate(hooks):
                @pl.when(g == k)
                def _(steps=steps):
                    for step, arg in steps:
                        step(*arg)
            return 0
        lax.fori_loop(0, len(hooks), group, 0)

    def relay():
        for j in range(1, nx):
            d_x(j).wait_recv()
            d_f(j).start()
            r_x(j).wait_recv()
            r_f(j).start()

    def bias_sum(k):
        def one(i, acc):
            return acc + fold8(DQKV[k, pl.ds(pl.multiple_of(i * RB, RB), RB), :].astype(F32))
        return jnp.sum(lax.fori_loop(0, rows // RB, one, zero), 0, keepdims=True)

    def project(i):
        for cp in c1s(i - 4):
            cp.wait_send()
        for kk in (1, 0):
            def wqkv(ff, kk=kk):
                p = qpart(i, ccof(kk))
                a = NB[:, pl.ds(pl.multiple_of(ff * U, U), U)]
                fill(i, kk, ff, tn(a, DQKV[p // 2, :, pl.ds(pl.multiple_of(lax.rem(p, 2) * U, U), U)]), 1)
            each_f(wqkv)
            if kk == 1:
                st1(i)

    segment(dq_one, 0, ntile * 6, (((h2, (1,)), (h1, (2,)), ),
             ((h0, (3,)), ),
             ((h2, (2,)), ),
             ((relay, ()), (h0, (4,)), ),
             ((h3, (0,)), (h3, (1,)), (h1, (3,)), ),
             ((h0, (5,)), (h1, (4,)), (h4, (0,)), (h2, (3,)), (h3, (2,)), (h4, (1,)), ),))
    loads["tok"].wait()
    project(9)
    put_vec(0, bias_sum(0))
    d_sib().wait_recv()
    r_sib().wait_recv()
    for j in range(1, nx):
        d_f(j).wait_recv()
        r_f(j).wait_recv()
    segment(dkv_one, 0, ntile * 3, (((st2, (9,)), (h0, (6,)), (h5, (0,)), (h1, (5,)), (h4, (2,)), ),
             ((h5, (1,)), (h2, (4,)), (h3, (3,)), ),
             ((h0, (7,)), (h5, (2,)), (h1, (6,)), (h2, (5,)), ),))
    project(10)
    segment(dkv_one, ntile * 3, ntile * 3, (((st2, (10,)), (h0, (8,)), (h3, (4,)), (h4, (3,)), (h1, (7,)), ),
             ((h2, (6,)), (h3, (5,)), (h4, (4,)), (h5, (3,)), ),
             ((st3, (9,)), (h1, (8,)), (h4, (5,)), (h2, (7,)), ),))
    put_vec(2, bias_sum(2))
    vst(0)
    project(11)
    vst(1)
    st2(11)
    h5(4)
    h3(6)
    h2(8)
    st4(9)
    h5(5)
    h3(7)
    for b in range(3):
        loads[("wq", b)].wait()
    for t in range(3):
        cs = slice(t * 256, (t + 1) * 256)
        acc = DH[:, cs]
        for b in range(3):
            acc = acc + nt(DQKV[b], WQ[b * 768 + t * 256:b * 768 + (t + 1) * 256, :])
        DM[:, cs] = acc.astype(BF16)
    gout = pltpu.make_async_copy(DM, gin_o, s8.at[NCH])
    gout.start()
    st3(10)
    h4(6)
    h4(7)
    h3(8)
    st5(9)
    vst(2)
    st4(10)
    h5(6)
    h5(7)
    h4(8)
    st3(11)
    st6(9)
    vst(3)
    st5(10)
    h5(8)
    st4(11)
    vst(4)
    st7(0)
    st7(1)
    st7(2)
    st7(3)
    st7(4)
    st7(5)
    st6(10)
    st5(11)
    st7(6)
    st7(7)
    st7(8)
    st6(11)
    st7(9)
    st7(10)
    st7(11)
    for c in range(NCH):
        c2(c).wait_send()
        c7(c).wait()
        c8(c).wait()
        if direct(c):
            for j in range(1, nx):
                c3(c, j).wait_send()
                c6(c, j).wait_send()
            for j in range(1, nd):
                c4(c, j).wait_send()
                c5(c, j).wait_send()
        else:
            for k in range(3):
                down(c, k).wait_send()
                upw(c, k).wait_send()
    for i in (8, 9, 10, 11):
        for cp in c1s(i):
            cp.wait_send()
    gout.wait()
    v_core().wait_send()
    v_y().wait_send()
    d_sib().wait_send()
    r_sib().wait_send()
    for j in range(1, nx):
        v_x(j).wait_send()
        d_x(j).wait_send()
        d_f(j).wait_send()
        r_x(j).wait_send()
        r_f(j).wait_send()
    for j in range(1, nd):
        v_z(j).wait_send()


def backward_reduce(lens, vec, vg, qkv, att, lse, wq, wo, wu, wd, dh, hat, act, gp, tok, nx, nd, seqs, cid):
    rows, d = att.shape
    nblk = 2 * nx
    CX, PZ = U // nx, U // nx // nd
    N = 12
    anyspec = pl.BlockSpec(memory_space=pl.ANY)
    vspec = pl.BlockSpec(memory_space=pltpu.VMEM)
    sspec = pl.BlockSpec(memory_space=pltpu.SMEM)
    D = pltpu.SemaphoreType.DMA
    V = pltpu.VMEM
    S = jax.ShapeDtypeStruct
    sems = [D((40,)), D((2,)), D((2,))] + [D((nx - 1, 2))] * 4 + [D((N, 2)), D((N, 2)), D((N,)), D((N,)), D((N, nx - 1)), D((N, nx - 1)),
            D((N, nd - 1)), D((N, nd - 1)), D((N, nd - 1)), D((N, nd - 1)), D((N, nx - 1)), D((N, nx - 1)),
            D((N,)), D((N,)), D((N + 1,)), D((nx + nd,)), D((nx + nd,)), D((9, 6)), D((9, 6))]
    return pl.pallas_call(
        functools.partial(bwd_kernel, nx, nd, seqs, rows // seqs),
        out_shape=(S((1536, 768), BF16), S((U, 3072), BF16), S((U, 768), BF16), S((U, 2304), BF16), S((12, U), F32), S((rows, d), BF16)),
        in_specs=[sspec, vspec, vspec] + [anyspec] * 12,
        out_specs=(anyspec,) * 4 + (vspec, anyspec),
        scratch_shapes=[V((6144, d), BF16), V((d, d), BF16), V((3 * d, d), BF16), V((2, rows, d), F32), V((rows, 3072), BF16),
                        V((rows, d), F32), V((rows, d), BF16), V((rows, d), F32), V((rows, d), BF16), V((nblk, rows, d), BF16),
                        V((nblk, 32, rows), F32), V((rows, 256), F32), V((3, rows, d), BF16),
                        V((N, 2, U, U), BF16), V((4, 2, U, U), BF16), V((N, 2, U, U), BF16), V((N, U, U), BF16),
                        V((3, nx - 1, CX, U), BF16), V((3, nd - 1, PZ, U), BF16), V((9, U - PZ, U), BF16), V((N, U, U), BF16),
                        V((24, U), F32), V((3, 24, U), F32), V((nx, 24, U), F32), V((nd, 24, U), F32)] + sems,
        compiler_params=pltpu.CompilerParams(collective_id=cid, has_side_effects=True, vmem_limit_bytes=63 << 20),
        name="backward_reduce",
    )(lens, vec, vg, qkv, att, lse, wq, wo, wu, wd, dh, hat, act, gp, tok)


FIN = 4


def finish_kernel(td, tu, to, tq, vec, y, gi, *outs):
    fd, fu, fo, fq, fy, fg = outs[:6]
    for src, dst in ((td, fd), (tu, fu), (to, fo), (tq, fq)):
        dst[...] = src[...].astype(F32)
    fy[...] = y[...]
    fg[...] = gi[...]

    @pl.when(pl.program_id(0) == 0)
    def _():
        row = 0
        for dst in outs[6:]:
            for i in range(dst.shape[0] // U):
                dst[i * U:(i + 1) * U] = vec[row:row + 1, :].reshape(U)
                row += 1


def finish(td, tu, to, tq, vec, y, gi):
    def spec(a):
        return pl.BlockSpec((a.shape[0] // FIN, a.shape[1]), lambda i: (i, 0))

    big = [td, tu, to, tq]
    sizes = [U, U, U, U, U, 4 * U, U, U, U]
    S = jax.ShapeDtypeStruct
    return pl.pallas_call(
        finish_kernel,
        grid=(FIN,),
        in_specs=[spec(a) for a in big] + [pl.BlockSpec(vec.shape, lambda i: (0, 0)), spec(y), spec(gi)],
        out_specs=[spec(a) for a in big] + [spec(y), spec(gi)] + [pl.BlockSpec((n,), lambda i: (0,)) for n in sizes],
        out_shape=[S(a.shape, F32) for a in big] + [S(y.shape, y.dtype), S(gi.shape, gi.dtype)] + [S((n,), F32) for n in sizes],
        name="finish",
    )(td, tu, to, tq, vec, y, gi)


def fast_body(
    tokens, cotangent, lengths, w_qkv, bias_q, bias_v, w_out, bias_out, gain_one, shift_one,
    w_up, bias_up, w_down, bias_down, gain_two, shift_two,
):
    seqs, seq_rows, width = tokens.shape
    nx, nd = lax.axis_size("ctx") // 2, lax.axis_size("dp")
    small = [bias_q, bias_v, bias_out, gain_one, shift_one, bias_up, bias_down, gain_two, shift_two]
    (qkv, att, lse, wq, wo, wu, wd, vec, out, dh, hat, act, gp, vg) = forward_gather(
        lengths, tokens, cotangent, w_qkv, w_out, w_up, w_down, small, nx, 2
    )
    t_down, t_up, t_out, t_qkv, t_vec, grad_in = backward_reduce(
        lengths, vec, vg, qkv, att, lse, wq, wo, wu, wd, dh, hat, act, gp,
        tokens.reshape(seqs * seq_rows, width), nx, nd, seqs, 3
    )

    (f_down, f_up, f_out, f_qkv, out, grad_in, bq, bv, bo, g1, s1, bu, bd, g2, s2) = finish(
        t_down, t_up, t_out, t_qkv, t_vec, out, grad_in
    )
    return (
        out.reshape(tokens.shape), grad_in.reshape(tokens.shape), f_qkv, bq, bv,
        f_out, bo, g1, s1, f_up, bu, f_down, bd, g2, s2,
    )


def solution(mesh):
    return jax.shard_map(
        fast_body if mesh.shape["ctx"] == 4 and mesh.shape["dp"] == 4 else general_body,
        mesh=mesh,
        in_specs=(
            P(("dp", "fsdp"), "ctx", None),
            P(("dp", "fsdp"), "ctx", None),
            P(("dp", "fsdp")),
            P("fsdp", None),
            P("fsdp"),
            P("fsdp"),
            P("fsdp", None),
            P("fsdp"),
            P("fsdp"),
            P("fsdp"),
            P("fsdp", None),
            P("fsdp"),
            P("fsdp", None),
            P("fsdp"),
            P("fsdp"),
            P("fsdp"),
        ),
        out_specs=(
            P(("dp", "fsdp"), "ctx", None),
            P(("dp", "fsdp"), "ctx", None),
            P("fsdp", None),
            P("fsdp"),
            P("fsdp"),
            P("fsdp", None),
            P("fsdp"),
            P("fsdp"),
            P("fsdp"),
            P("fsdp", None),
            P("fsdp"),
            P("fsdp", None),
            P("fsdp"),
            P("fsdp"),
            P("fsdp"),
        ),
        check_vma=False,
    )
```
